128 devices in a mesh: dp: 2 (over core), ctx: 64 (over z, y, x).
Axes of the slice: x: 4, y: 4, z: 4, core: 2. Of those that a mesh axis runs over, the one named last changes fastest.
Arguments:
- documents: int32 [32768], P(('dp', 'ctx')), parts along dimension 0, may hold values from 0 to 15, never falling along the last dimension, each value on 1 to 2048 neighbouring positions
- queries: bfloat16 [32768, 4096], P(('dp', 'ctx')), parts along dimension 0, may hold values from -6 to 6
- key_projection_rows: bfloat16 [32768, 512], P(('dp', 'ctx')), parts along dimension 0, may hold values from -6 to 6
- value_projection_rows: bfloat16 [32768, 512], P(('dp', 'ctx')), parts along dimension 0, may hold values from -6 to 6
Outputs:
- attended: bfloat16 [32768, 4096], P(('dp', 'ctx')), parts along dimension 0
The draws below stay inside these ranges and needn't reach their ends.
There are 2 independent parts, one for each index of `dp`. The reference program is written for one: setup_inputs(seed, part) draws one part's arguments, and reference() takes and returns one part's arrays. A program takes and returns all parts, laid end to end along the dimension named above; each array names one. Nothing has to cross between parts.
Inputs may be any that keep to these rules, and one draw needn't show every extreme that they name: `documents`: document numbers never fall along the sequence; every number appears; each document has 1 to 2048 tokens and one has exactly 2048.
All inputs are finite; a program needn't handle non-finite values.
Results may differ from the reference program's by a relative error of at most 0.0074.
Values may be sent and summed in bfloat16 or wider, within the bound.
A program may use at most 192 MiB of HBM per device.

```python
import math
import jax
import jax.numpy as jnp
import numpy as np
from jax import lax

HEAD_WIDTH = 128
QUERY_HEADS = 32
KEY_VALUE_HEADS = 4
DOCS = 16
DEVICE_TOKENS = 256
PACKED_TOKENS = 16384
MOST = 2048


def shared_draw(key):
    base = jax.random.fold_in(key, 7)
    key_q, key_matrix, key_pick, key_polarity = jax.random.split(base, 4)
    key_result = jnp.clip(jax.random.normal(key_matrix, (PACKED_TOKENS, KEY_VALUE_HEADS * HEAD_WIDTH), jnp.float32), -6.0, 6.0)
    query_out = jnp.clip(jax.random.normal(key_q, (PACKED_TOKENS, QUERY_HEADS * HEAD_WIDTH), jnp.float32), -6.0, 6.0)
    return (query_out, key_result)


def draw_queries(key, part):
    return shared_draw(key)[0].astype(jnp.bfloat16)


def draw_key_projection_rows(key, part):
    return shared_draw(key)[1].astype(jnp.bfloat16)


def block_levels(rng, dims, cuts, smallest, high):
    def one(position, blocks):
        steps = jax.random.uniform(jax.random.fold_in(jax.random.fold_in(rng, 6), position), (blocks,), jnp.float32, smallest / len(cuts), high / len(cuts))
        return jnp.repeat(jnp.exp(steps), dims[position] // blocks).reshape((-1,) + (1,) * (len(dims) - position - 1))

    level = one(*cuts[0])
    for cut in cuts[1:]:
        level = level * one(*cut)
    return level


def profile(count, total, limit, skew):
    portions = [(1 << 20) // math.isqrt(rank ** skew) + 1 for rank in range(2, count + 1)]
    surplus, given = total - limit - (count - 1), [1] * (count - 1)
    while surplus > 0:
        free = [i for i in range(count - 1) if given[i] < limit]
        mass, left = sum([portions[i] for i in free]), surplus
        for i in free:
            extra = min(limit - given[i], max(1, left * portions[i] // mass), surplus)
            given[i] = given[i] + extra
            surplus = surplus - extra
    return np.array([limit] + given)


def uneven(rng, number_of, total, bound, skew):
    if number_of == 2:
        one = jax.random.randint(rng, (), max(1, total - bound), min(bound, total - 1) + 1)
        return jnp.stack([one, total - one])
    lengths = jnp.asarray(profile(number_of, total, bound, skew), jnp.int32)
    twos = (number_of - 1) // 2
    giver, taker = lengths[1:1 + 2 * twos:2], lengths[2:2 + 2 * twos:2]
    slack = jnp.minimum(giver - 1, bound - taker)
    shifted = jax.random.randint(jax.random.fold_in(rng, 1), (twos,), 0, 1 << 20) % (slack + 1)
    lengths = lengths.at[1:1 + 2 * twos:2].set(giver - shifted).at[2:2 + 2 * twos:2].set(taker + shifted)
    return lengths[jax.random.permutation(jax.random.fold_in(rng, 2), number_of)]


def noise(stream_key, shape, deviation, most, cuts=(), held_as=jnp.bfloat16):
    loudness = block_levels(stream_key, shape, cuts, -0.22, 0.18) if cuts else 1.0
    values = jax.random.normal(stream_key, shape, jnp.float32) * deviation * loudness
    return jnp.minimum(jnp.maximum(values, -most), most).astype(held_as)


def setup_inputs(seed: int = 0, part: int = 0) -> dict:
    streams_of = jax.random.split(jax.random.key(seed), 5)
    part_keys = jax.random.split(jax.random.fold_in(streams_of[4], part), 5)
    documents = jnp.searchsorted(jnp.cumsum(uneven(part_keys[0], DOCS, PACKED_TOKENS, MOST, 2)), jnp.arange(PACKED_TOKENS), side="right").astype(jnp.int32)
    queries = draw_queries(jax.random.fold_in(jax.random.fold_in(streams_of[4], part), 71), part)
    key_projection_rows = draw_key_projection_rows(jax.random.fold_in(jax.random.fold_in(streams_of[4], part), 71), part)
    value_projection_rows = noise(part_keys[3], (PACKED_TOKENS, KEY_VALUE_HEADS * HEAD_WIDTH), 1.0, 6.0, ((0, 64),))
    return dict(documents=documents, queries=queries, key_projection_rows=key_projection_rows, value_projection_rows=value_projection_rows)


def apply_rotary_rows(matrix, document_position, head_count):
    total_row_count = matrix.shape[0]
    head_size = matrix.shape[1] // head_count
    half_dim = head_size // 2
    widened = matrix.astype(jnp.float32).reshape(total_row_count, head_count, head_size)
    inverse = jnp.power(jnp.float32(1000000.0), -2.0 * jnp.arange(half_dim, dtype=jnp.float32) / head_size)
    angles = document_position.astype(jnp.float32)[:, None] * inverse[None, :]
    cosine = jnp.cos(angles)[:, None, :]
    sine_part = jnp.sin(angles)[:, None, :]
    front = widened[..., :half_dim]
    back = widened[..., half_dim:]
    rotated = jnp.concatenate([front * cosine - back * sine_part, back * cosine + front * sine_part], axis=-1)
    return rotated.reshape(total_row_count, head_count * head_size).astype(jnp.bfloat16)


def reference(documents, queries, key_projection_rows, value_projection_rows):
    token_count = documents.shape[0]
    index_all = jnp.arange(token_count, dtype=jnp.int32)
    doc_start = jnp.searchsorted(documents, documents, side="left").astype(jnp.int32)
    document_position = index_all - doc_start
    rotary_queries = apply_rotary_rows(queries, document_position, QUERY_HEADS)
    rotary_keys = apply_rotary_rows(key_projection_rows, document_position, KEY_VALUE_HEADS)
    query_group_width = QUERY_HEADS // KEY_VALUE_HEADS
    covered_rows = MOST + DEVICE_TOKENS
    scaling = HEAD_WIDTH ** -0.5

    def one_block(block_number):
        query_block_begin = (block_number * DEVICE_TOKENS).astype(jnp.int32)
        key_block_begin = jnp.clip(query_block_begin - MOST, 0, token_count - covered_rows).astype(jnp.int32)
        query_tile_block = lax.dynamic_slice_in_dim(rotary_queries, query_block_begin, DEVICE_TOKENS, 0).astype(jnp.float32).reshape(DEVICE_TOKENS, KEY_VALUE_HEADS, query_group_width, HEAD_WIDTH)
        key_tile_block = lax.dynamic_slice_in_dim(rotary_keys, key_block_begin, covered_rows, 0).astype(jnp.float32).reshape(covered_rows, KEY_VALUE_HEADS, HEAD_WIDTH)
        value_tile_block = lax.dynamic_slice_in_dim(value_projection_rows, key_block_begin, covered_rows, 0).astype(jnp.float32).reshape(covered_rows, KEY_VALUE_HEADS, HEAD_WIDTH)
        query_index = query_block_begin + jnp.arange(DEVICE_TOKENS, dtype=jnp.int32)
        key_index = key_block_begin + jnp.arange(covered_rows, dtype=jnp.int32)
        starts = lax.dynamic_slice_in_dim(doc_start, query_block_begin, DEVICE_TOKENS, 0)
        allowed = (key_index[None, :] <= query_index[:, None]) & (key_index[None, :] >= starts[:, None])
        scores = jnp.einsum("qkgd,nkd->kgqn", query_tile_block, key_tile_block) * scaling
        scores = jnp.where(allowed, scores, jnp.float32(-1e30))
        top_score = jnp.max(scores, axis=-1, keepdims=True)
        weights = jnp.where(allowed, jnp.exp(scores - top_score), jnp.float32(0.0))
        denominator = jnp.sum(weights, axis=-1)
        mixed = jnp.einsum("kgqn,nkd->kgqd", weights.astype(jnp.bfloat16).astype(jnp.float32), value_tile_block)
        mixed = mixed / denominator[..., None]
        return mixed.transpose(2, 0, 1, 3).reshape(DEVICE_TOKENS, QUERY_HEADS * HEAD_WIDTH).astype(jnp.bfloat16)

    result = lax.map(one_block, jnp.arange(token_count // DEVICE_TOKENS, dtype=jnp.int32))
    return result.reshape(token_count, QUERY_HEADS * HEAD_WIDTH)
```

```python
import functools
import math
import jax
import jax.numpy as jnp
import numpy as np
from jax import lax
from jax.experimental import pallas as pl
from jax.experimental.pallas import tpu as pltpu
from jax.sharding import PartitionSpec as P

HEAD = 128
HEADS = 32
KV_HEADS = 4
GROUP = HEADS // KV_HEADS
ROWS = 256
ITEMS = 9
VALUE_ROWS = 144
AT_ONCE = 4
MOST_AT_ONCE = 3
SCALE = math.log2(math.e) / math.sqrt(HEAD)
LOW = 1e-25
HIGH = 1e37
MASKED = -1e30
MESH = pl.DeviceIdType.MESH
VMEM = pltpu.VMEM


def attend(docs, inverse, q_hbm, k_ref, v_ref, ot_hbm, qt_hbm, wk_hbm, wv_hbm, start_out, bad_out,
           q_buf, q_t, wk, wv, bias, acc, probs, o_t, doc_win, cosine, sine,
           rk, rv, sk, sv, doc_send, doc_recv, q_sem, ot_sem, qt_sem, wk_sem, wv_sem):
    count = lax.axis_size("ctx")
    me = lax.axis_index("ctx")
    x = lax.rem(me, 4)
    row = me - x
    right = row + lax.rem(x + 1, 4)
    left = row + lax.rem(x + 3, 4)
    up = lax.rem(me + 4, count)

    barrier = pltpu.get_barrier_semaphore()
    for other in [lax.rem(me + count - d, count) for d in range(1, 9)] + [left, right]:
        pl.semaphore_signal(barrier, inc=1, device_id={"ctx": other}, device_id_type=MESH)
    q_copy = pltpu.make_async_copy(q_hbm, q_buf, q_sem)
    q_copy.start()

    def value_copy(src, dst, c, target):
        return pltpu.make_async_remote_copy(
            wv.at[src, c, pl.ds(0, HEAD)], wv.at[dst, c, pl.ds(0, HEAD)], sv.at[dst, c], rv.at[dst, c],
            device_id={"ctx": target}, device_id_type=MESH)

    def key_copy(src, dst, c, target):
        return pltpu.make_async_remote_copy(
            wk.at[src, c], wk.at[dst, c], sk.at[dst, c], rk.at[dst, c],
            device_id={"ctx": target}, device_id_type=MESH)

    def doc_copy(d):
        return pltpu.make_async_remote_copy(
            docs, doc_win.at[d - 1], doc_send.at[d - 1], doc_recv.at[d - 1],
            device_id={"ctx": lax.rem(me + d, count)}, device_id_type=MESH)

    def when_sent(condition, copy):
        @pl.when(condition)
        def _():
            copy.start()

    wv[:, :, HEAD:, :] = jnp.ones((ITEMS, KV_HEADS, VALUE_ROWS - HEAD, ROWS), jnp.bfloat16)
    for c in range(KV_HEADS):
        wv[0, c, 0:HEAD] = v_ref[:, c * HEAD:(c + 1) * HEAD].T
    pl.semaphore_wait(barrier, 10)
    for d in range(1, 9):
        doc_copy(d).start()
    for c in range(KV_HEADS):
        value_copy(0, 4, c, up).start()
        when_sent(x < 3, value_copy(0, 1, c, right))
        when_sent(x == 0, value_copy(0, 3, c, left))

    doc_row = docs[...].astype(jnp.float32)
    columns = jnp.transpose(jnp.broadcast_to(doc_row, (ROWS, ROWS)))
    local = jnp.sum((columns < doc_row).astype(jnp.float32), axis=0, keepdims=True)
    first = doc_row[:, 0:1]
    for d in range(1, 9):
        doc_copy(d).wait_recv()
    behind = jnp.zeros((1, ROWS), jnp.float32)
    for d in range(1, 9):
        same = (doc_win[d - 1].astype(jnp.float32) == first).astype(jnp.float32)
        behind = behind + same * jnp.where(d <= me, 1.0, 0.0)
    behind = jnp.sum(behind, axis=1, keepdims=True)
    start = jnp.where(doc_row == first, -behind, local)
    start_out[...] = jnp.broadcast_to(start, (8, ROWS))
    tokens = lax.broadcasted_iota(jnp.int32, (1, ROWS), 1).astype(jnp.float32)
    angles = inverse[...] * (tokens - start)
    cosine[...] = jnp.cos(angles)
    sine[...] = jnp.sin(angles)

    def rotated(matrix):
        wide = matrix.astype(jnp.float32)
        a, b = wide[0:HEAD // 2], wide[HEAD // 2:]
        co, si = cosine[...], sine[...]
        return jnp.concatenate([a * co - b * si, b * co + a * si], axis=0)

    for c in range(KV_HEADS):
        wk[0, c] = rotated(k_ref[:, c * HEAD:(c + 1) * HEAD].T).T.astype(jnp.bfloat16)

    query = lax.broadcasted_iota(jnp.int32, (ROWS, ROWS), 1).astype(jnp.float32)
    key = lax.broadcasted_iota(jnp.int32, (ROWS, ROWS), 0).astype(jnp.float32)
    for d in range(ITEMS):
        at = key - float(ROWS * d)
        bias[d] = jnp.where((at >= start) & (at <= query), 0.0, MASKED)

    for c in range(KV_HEADS):
        key_copy(0, 4, c, up).start()
        when_sent(x < 3, key_copy(0, 1, c, right))
        when_sent(x == 0, key_copy(0, 3, c, left))

    def here(values, keys, c):
        for d in values:
            value_copy(d, d, c, up).wait_recv()
        for d in keys:
            key_copy(d, d, c, up).wait_recv()

    q_copy.wait()

    def step_one(c, _):
        here((4,), (), c)
        when_sent(x == 3, value_copy(4, 1, c, right))
        when_sent(x > 0, value_copy(4, 3, c, left))

        def turn(h, _):
            at = pl.multiple_of(h * HEAD, HEAD)
            q_t[h] = rotated(q_buf[:, pl.ds(at, HEAD)].T).astype(jnp.bfloat16)
            return 0

        lax.fori_loop(c * GROUP, c * GROUP + GROUP, turn, 0)
        return 0

    lax.fori_loop(0, KV_HEADS, step_one, 0)
    qt_copy = pltpu.make_async_copy(q_t, qt_hbm, qt_sem)
    qt_copy.start()
    bad_out[...] = jnp.zeros((8, ROWS), jnp.float32)

    def weigh(items, at):
        for u in range(AT_ONCE):
            h = at + u
            for n, d in enumerate(items):
                scores = lax.dot_general(wk[d, h // GROUP], q_t[h], (((1,), (0,)), ((), ())),
                                         preferred_element_type=jnp.float32)
                probs[u, n] = jnp.exp2(scores * SCALE + bias[d]).astype(jnp.bfloat16)

    def gather(items, at, begin, end):
        for u in range(AT_ONCE):
            h = at + u
            kv = jnp.maximum(h, 0) // GROUP
            total = None
            for n, d in enumerate(items):
                part = lax.dot_general(wv[d, kv], probs[u, n], (((1,), (0,)), ((), ())),
                                       preferred_element_type=jnp.float32)
                total = part if total is None else total + part
            if not begin:
                total = acc[h + AT_ONCE] + total
            if end:
                bottom = total[HEAD:HEAD + 1]
                o_t[h + AT_ONCE] = (total[0:HEAD] * (1.0 / bottom)).astype(jnp.bfloat16)
                fine = (bottom >= LOW) & (bottom <= HIGH)
                fine = fine | (h < 0)
                bad_out[0:1] = jnp.maximum(bad_out[0:1], jnp.where(fine, 0.0, 1.0))
            else:
                acc[h + AT_ONCE] = total

    def out_copy(i):
        return pltpu.make_async_copy(o_t.at[pl.ds(AT_ONCE * (i + 1), AT_ONCE)],
                                     ot_hbm.at[pl.ds(AT_ONCE * i, AT_ONCE)], ot_sem.at[i])

    def group(items, event, begin=False, end=False):
        def outer(c, _):
            event(c)

            def inner(j, _):
                i = 2 * c + j
                if end:
                    @pl.when(i >= 2)
                    def _():
                        out_copy(i - 2).start()
                gather(items, AT_ONCE * (i - 1), begin, end)
                weigh(items, AT_ONCE * i)
                return 0

            lax.fori_loop(0, 2, inner, 0)
            return 0

        lax.fori_loop(0, KV_HEADS, outer, 0)
        if end:
            out_copy(6).start()
        gather(items, HEADS - AT_ONCE, begin, end)

    def event_two(c):
        here((), (4,), c)
        value_copy(4, 8, c, up).start()
        when_sent(x < 3, value_copy(4, 5, c, right))
        when_sent(x == 3, key_copy(4, 1, c, right))
        when_sent(x > 0, key_copy(4, 3, c, left))

    def event_three(c):
        here((1, 8), (3,), c)
        key_copy(3, 7, c, up).start()
        when_sent(x < 3, value_copy(1, 2, c, right))
        when_sent(x == 3, value_copy(8, 5, c, right))
        when_sent(x > 0, value_copy(8, 7, c, left))
        when_sent(x == 0, value_copy(4, 7, c, left))

    def event_four(c):
        here((3, 5, 7), (1,), c)
        key_copy(1, 5, c, up).start()
        when_sent(x < 3, key_copy(1, 2, c, right))
        when_sent(x == 3, value_copy(5, 2, c, right))
        when_sent(x > 0, value_copy(7, 6, c, left))
        when_sent(x == 0, value_copy(3, 6, c, left))

    def event_five(c):
        here((), (5, 7), c)
        key_copy(4, 8, c, up).start()
        when_sent(x == 3, key_copy(5, 2, c, right))
        when_sent(x > 0, key_copy(7, 6, c, left))
        when_sent(x == 0, key_copy(3, 6, c, left))

    def event_six(c):
        here((2, 6), (2, 6, 8), c)

    def kept(refs, out, sems, d):
        return pltpu.make_async_copy(refs.at[d], out.at[d], sems.at[d])

    def keep(*items):
        for d in items:
            kept(wk, wk_hbm, wk_sem, d).start()
            kept(wv, wv_hbm, wv_sem, d).start()

    group((0,), event_two, begin=True)
    keep(0, 4)
    group((4,), event_three)
    group((1, 3), event_four)
    keep(1, 3)
    group((5, 7), event_five)
    keep(5, 7)
    group((2, 6, 8), event_six, end=True)
    keep(2, 6, 8)
    out_copy(7).start()

    for d in range(ITEMS):
        kept(wk, wk_hbm, wk_sem, d).wait()
        kept(wv, wv_hbm, wv_sem, d).wait()
    for i in range(HEADS // AT_ONCE):
        out_copy(i).wait()
    qt_copy.wait()
    for d in range(1, 9):
        doc_copy(d).wait_send()

    def drain(c, _):
        for d in range(1, 9):
            value_copy(d, d, c, up).wait_send()
            key_copy(d, d, c, up).wait_send()
        return 0

    lax.fori_loop(0, KV_HEADS, drain, 0)


def finish(o_t, start, bad, qt_hbm, wk_hbm, wv_hbm, out, q_buf, k_buf, v_buf, sems):
    g = pl.program_id(0)
    fine = jnp.max(bad[...]) < 0.5

    @pl.when(fine)
    def _():
        for u in range(GROUP):
            out[:, u * HEAD:(u + 1) * HEAD] = o_t[u].T

    @pl.when(jnp.logical_not(fine))
    def _():
        copies = [
            pltpu.make_async_copy(qt_hbm.at[pl.ds(GROUP * g, GROUP)], q_buf, sems.at[0]),
            pltpu.make_async_copy(wk_hbm.at[:, g], k_buf, sems.at[1]),
            pltpu.make_async_copy(wv_hbm.at[:, g], v_buf, sems.at[2]),
        ]
        for copy in copies:
            copy.start()
        for copy in copies:
            copy.wait()
        query = lax.broadcasted_iota(jnp.int32, (ROWS, ROWS), 1).astype(jnp.float32)
        key = lax.broadcasted_iota(jnp.int32, (ROWS, ROWS), 0).astype(jnp.float32)
        begin = start[0:1]

        for u in range(GROUP):
            def scores(d):
                at = key - (d * ROWS).astype(jnp.float32)
                found = lax.dot_general(k_buf[d], q_buf[u], (((1,), (0,)), ((), ())),
                                        preferred_element_type=jnp.float32)
                return jnp.where((at >= begin) & (at <= query), found * SCALE, MASKED)

            def highest(d, top):
                return jnp.maximum(top, jnp.max(scores(d), axis=0, keepdims=True))

            top = lax.fori_loop(0, ITEMS, highest, jnp.full((1, ROWS), MASKED, jnp.float32))

            def summed(d, carry):
                bottom, total = carry
                weights = jnp.exp2(scores(d) - top)
                bottom = bottom + jnp.sum(weights, axis=0, keepdims=True)
                part = lax.dot_general(v_buf[d, 0:HEAD], weights.astype(jnp.bfloat16), (((1,), (0,)), ((), ())),
                                       preferred_element_type=jnp.float32)
                return bottom, total + part

            bottom, total = lax.fori_loop(
                0, ITEMS, summed, (jnp.zeros((1, ROWS), jnp.float32), jnp.zeros((HEAD, ROWS), jnp.float32)))
            out[:, u * HEAD:(u + 1) * HEAD] = (total / bottom).astype(jnp.bfloat16).T


def shards(documents, queries, key_projection_rows, value_projection_rows):
    bf, f32 = jnp.bfloat16, jnp.float32
    powers = np.float32(1000000.0) ** (-2.0 * np.arange(HEAD // 2, dtype=np.float32) / HEAD)
    inverse = jnp.asarray(np.broadcast_to(powers[:, None], (HEAD // 2, ROWS)), f32)
    vmem, whole = pl.BlockSpec(memory_space=VMEM), pl.BlockSpec(memory_space=pl.ANY)
    dma = pltpu.SemaphoreType.DMA
    flops = 4 * HEADS * ROWS * ITEMS * ROWS * HEAD
    o_t, q_t, wk, wv, start, bad = pl.pallas_call(
        attend,
        out_shape=[
            jax.ShapeDtypeStruct((HEADS, HEAD, ROWS), bf),
            jax.ShapeDtypeStruct((HEADS, HEAD, ROWS), bf),
            jax.ShapeDtypeStruct((ITEMS, KV_HEADS, ROWS, HEAD), bf),
            jax.ShapeDtypeStruct((ITEMS, KV_HEADS, VALUE_ROWS, ROWS), bf),
            jax.ShapeDtypeStruct((8, ROWS), f32),
            jax.ShapeDtypeStruct((8, ROWS), f32),
        ],
        in_specs=[vmem, vmem, whole, vmem, vmem],
        out_specs=[whole] * 4 + [vmem] * 2,
        scratch_shapes=[
            VMEM((ROWS, HEADS * HEAD), bf),
            VMEM((HEADS, HEAD, ROWS), bf),
            VMEM((ITEMS, KV_HEADS, ROWS, HEAD), bf),
            VMEM((ITEMS, KV_HEADS, VALUE_ROWS, ROWS), bf),
            VMEM((ITEMS, ROWS, ROWS), f32),
            VMEM((HEADS + AT_ONCE, VALUE_ROWS, ROWS), f32),
            VMEM((AT_ONCE, MOST_AT_ONCE, ROWS, ROWS), bf),
            VMEM((HEADS + AT_ONCE, HEAD, ROWS), bf),
            VMEM((8, 1, ROWS), jnp.int32),
            VMEM((HEAD // 2, ROWS), f32),
            VMEM((HEAD // 2, ROWS), f32),
            dma((ITEMS, KV_HEADS)), dma((ITEMS, KV_HEADS)), dma((ITEMS, KV_HEADS)), dma((ITEMS, KV_HEADS)),
            dma((8,)), dma((8,)), dma, dma((HEADS // AT_ONCE,)), dma, dma((ITEMS,)), dma((ITEMS,)),
        ],
        compiler_params=pltpu.CompilerParams(collective_id=0, has_side_effects=True, vmem_limit_bytes=56 * 2**20),
        cost_estimate=pl.CostEstimate(flops=flops, bytes_accessed=12 * 2**20, transcendentals=HEADS * ROWS * ITEMS * ROWS),
        name="attend",
    )(documents.reshape(1, ROWS), inverse, queries, key_projection_rows, value_projection_rows)
    return pl.pallas_call(
        finish,
        grid=(KV_HEADS,),
        out_shape=jax.ShapeDtypeStruct((ROWS, HEADS * HEAD), bf),
        in_specs=[
            pl.BlockSpec((GROUP, HEAD, ROWS), lambda g: (g, 0, 0)),
            pl.BlockSpec((8, ROWS), lambda g: (0, 0)),
            pl.BlockSpec((8, ROWS), lambda g: (0, 0)),
            whole, whole, whole,
        ],
        out_specs=pl.BlockSpec((ROWS, GROUP * HEAD), lambda g: (0, g)),
        scratch_shapes=[
            VMEM((GROUP, HEAD, ROWS), bf),
            VMEM((ITEMS, ROWS, HEAD), bf),
            VMEM((ITEMS, VALUE_ROWS, ROWS), bf),
            dma((3,)),
        ],
        compiler_params=pltpu.CompilerParams(vmem_limit_bytes=40 * 2**20),
        cost_estimate=pl.CostEstimate(flops=2**20, bytes_accessed=4 * 2**20, transcendentals=0),
        name="finish",
    )(o_t, start, bad, q_t, wk, wv)


def solution(mesh):
    in_specs = (
        P(("dp", "ctx")),
        P(("dp", "ctx"), None),
        P(("dp", "ctx"), None),
        P(("dp", "ctx"), None),
    )
    out_specs = P(("dp", "ctx"), None)
    return jax.shard_map(shards, mesh=mesh, in_specs=in_specs, out_specs=out_specs, check_vma=False)
```

```python
import functools
import math
import jax
import jax.numpy as jnp
import numpy as np
from jax import lax
from jax.experimental import pallas as pl
from jax.experimental.pallas import tpu as pltpu
from jax.sharding import PartitionSpec as P

HEAD = 128
HEADS = 32
KV_HEADS = 4
GROUP = HEADS // KV_HEADS
ROWS = 256
ITEMS = 9
VALUE_ROWS = 144
AT_ONCE = 4
MOST_AT_ONCE = 3
SCALE = math.log2(math.e) / math.sqrt(HEAD)
LOW = 1e-25
HIGH = 1e37
MASKED = -1e30
MESH = pl.DeviceIdType.MESH
VMEM = pltpu.VMEM


def attend(doc_hbm, inverse, q_hbm, k_hbm, v_hbm, out_hbm, qt_hbm, wk_hbm, wv_hbm, start_out, bad_out,
           docs, k_buf, v_buf, q_buf, q_t, wk, wv, bias, acc, probs, doc_win, cosine, sine,
           rk, rv, sk, sv, doc_send, doc_recv, in_sem, out_sem, qt_sem, wk_sem, wv_sem):
    count = lax.axis_size("ctx")
    me = lax.axis_index("ctx")
    x = lax.rem(me, 4)
    row = me - x
    right = row + lax.rem(x + 1, 4)
    left = row + lax.rem(x + 3, 4)
    up = lax.rem(me + 4, count)

    barrier = pltpu.get_barrier_semaphore()

    def greet(other):
        pl.semaphore_signal(barrier, inc=1, device_id={"ctx": other}, device_id_type=MESH)

    for d in range(1, 9):
        @pl.when(d <= me)
        def _():
            greet(lax.rem(me + count - d, count))
    greet(left)
    greet(right)
    loads = [pltpu.make_async_copy(a, b, in_sem.at[n])
             for n, (a, b) in enumerate([(v_hbm, v_buf), (doc_hbm, docs), (k_hbm, k_buf), (q_hbm, q_buf)])]
    for load in loads:
        load.start()

    def value_copy(src, dst, c, target):
        return pltpu.make_async_remote_copy(
            wv.at[src, c, pl.ds(0, HEAD)], wv.at[dst, c, pl.ds(0, HEAD)], sv.at[dst, c], rv.at[dst, c],
            device_id={"ctx": target}, device_id_type=MESH)

    def key_copy(src, dst, c, target):
        return pltpu.make_async_remote_copy(
            wk.at[src, c], wk.at[dst, c], sk.at[dst, c], rk.at[dst, c],
            device_id={"ctx": target}, device_id_type=MESH)

    def doc_copy(d):
        return pltpu.make_async_remote_copy(
            docs, doc_win.at[d - 1], doc_send.at[d - 1], doc_recv.at[d - 1],
            device_id={"ctx": lax.rem(me + d, count)}, device_id_type=MESH)

    def when_sent(condition, copy):
        @pl.when(condition)
        def _():
            copy.start()

    def send_up(copy, src, dst, c):
        when_sent((me + 4 < count) & (src <= me), copy(src, dst, c, up))

    def send_right(copy, src, dst, c, there):
        when_sent(there & (src <= me), copy(src, dst, c, right))

    def send_left(copy, src, dst, c, there):
        when_sent(there & (src <= me), copy(src, dst, c, left))

    wv[:, :, HEAD:, :] = jnp.ones((ITEMS, KV_HEADS, VALUE_ROWS - HEAD, ROWS), jnp.bfloat16)
    loads[0].wait()
    for c in range(KV_HEADS):
        wv[0, c, 0:HEAD] = v_buf[:, c * HEAD:(c + 1) * HEAD].T
    loads[1].wait()
    pl.semaphore_wait(barrier, 2 + jnp.minimum(8, count - 1 - me))
    for d in range(1, 9):
        when_sent(me + d < count, doc_copy(d))
    for c in range(KV_HEADS):
        send_up(value_copy, 0, 4, c)
        send_right(value_copy, 0, 1, c, x < 3)
        send_left(value_copy, 0, 3, c, x == 0)
    loads[3].wait()

    def turn(n, _):
        for u in range(4):
            at = pl.multiple_of((4 * n + u) * HEAD, HEAD)
            q_t[4 * n + u] = q_buf[:, pl.ds(at, HEAD)].T
        return 0

    lax.fori_loop(0, HEADS // 4, turn, 0)
    for d in range(1, 9):
        @pl.when(d > me)
        def _():
            wk[d] = jnp.zeros((KV_HEADS, ROWS, HEAD), jnp.bfloat16)
            wv[d, :, 0:HEAD] = jnp.zeros((KV_HEADS, HEAD, ROWS), jnp.bfloat16)

    doc_row = docs[...].astype(jnp.float32)
    columns = jnp.transpose(jnp.broadcast_to(doc_row, (ROWS, ROWS)))
    local = jnp.sum((columns < doc_row).astype(jnp.float32), axis=0, keepdims=True)
    first = doc_row[:, 0:1]
    powers = jnp.transpose(jnp.broadcast_to(inverse[...], (HEAD, HEAD)))[0:HEAD // 2]
    powers = jnp.concatenate([powers, powers], axis=1)
    tokens = lax.broadcasted_iota(jnp.int32, (1, ROWS), 1).astype(jnp.float32)
    loads[2].wait()
    for d in range(1, 9):
        @pl.when(d <= me)
        def _():
            doc_copy(d).wait_recv()
    behind = jnp.zeros((1, ROWS), jnp.float32)
    for d in range(1, 9):
        same = (doc_win[d - 1].astype(jnp.float32) == first) & (d <= me)
        behind = behind + jnp.where(same, 1.0, 0.0)
    behind = jnp.sum(behind, axis=1, keepdims=True)
    start = jnp.where(doc_row == first, -behind, local)
    start_out[...] = jnp.broadcast_to(start, (8, ROWS))
    angles = powers * (tokens - start)
    cosine[...] = jnp.cos(angles)
    sine[...] = jnp.sin(angles)

    def rotated(matrix):
        wide = matrix.astype(jnp.float32)
        a, b = wide[0:HEAD // 2], wide[HEAD // 2:]
        co, si = cosine[...], sine[...]
        return jnp.concatenate([a * co - b * si, b * co + a * si], axis=0)

    for c in range(KV_HEADS):
        wk[0, c] = rotated(k_buf[:, c * HEAD:(c + 1) * HEAD].T).T.astype(jnp.bfloat16)
    query = lax.broadcasted_iota(jnp.int32, (ROWS, ROWS), 1).astype(jnp.float32)
    key = lax.broadcasted_iota(jnp.int32, (ROWS, ROWS), 0).astype(jnp.float32)
    bias[0] = jnp.where((key >= start) & (key <= query), 0.0, MASKED)
    for c in range(KV_HEADS):
        send_up(key_copy, 0, 4, c)
        send_right(key_copy, 0, 1, c, x < 3)
        send_left(key_copy, 0, 3, c, x == 0)
    for d in range(1, ITEMS):
        at = key - float(ROWS * d)
        bias[d] = jnp.where((at >= start) & (at <= query), 0.0, MASKED)

    def here(values, keys, c):
        for d in values:
            @pl.when(d <= me)
            def _():
                value_copy(d, d, c, up).wait_recv()
        for d in keys:
            @pl.when(d <= me)
            def _():
                key_copy(d, d, c, up).wait_recv()

    def step_one(c, _):
        here((4,), (), c)
        send_right(value_copy, 4, 1, c, x == 3)
        send_left(value_copy, 4, 3, c, x > 0)

        def turned(n, _):
            for u in range(4):
                h = c * GROUP + 4 * n + u
                q_t[h] = rotated(q_t[h]).astype(jnp.bfloat16)
            return 0

        lax.fori_loop(0, GROUP // 4, turned, 0)
        return 0

    lax.fori_loop(0, KV_HEADS, step_one, 0)
    qt_copy = pltpu.make_async_copy(q_t, qt_hbm, qt_sem)
    qt_copy.start()
    bad_out[...] = jnp.zeros((8, ROWS), jnp.float32)

    def weigh(items, at, size):
        for u in range(size):
            h = at + u
            for n, d in enumerate(items):
                scores = lax.dot_general(wk[d, h // GROUP], q_t[h], (((1,), (0,)), ((), ())),
                                         preferred_element_type=jnp.float32)
                probs[u * len(items) + n] = jnp.exp2(scores * SCALE + bias[d]).astype(jnp.bfloat16)

    def gather(items, at, size, begin, end):
        for u in range(size):
            h = at + u
            total = None
            for n, d in enumerate(items):
                part = lax.dot_general(wv[d, h // GROUP], probs[u * len(items) + n], (((1,), (0,)), ((), ())),
                                       preferred_element_type=jnp.float32)
                total = part if total is None else total + part
            if not begin:
                total = acc[h] + total
            if end:
                bottom = total[HEAD:HEAD + 1]
                lane = h * HEAD if isinstance(h, int) else pl.multiple_of(h * HEAD, HEAD)
                q_buf[:, pl.ds(lane, HEAD)] = (total[0:HEAD] * (1.0 / bottom)).astype(jnp.bfloat16).T
                fine = (bottom >= LOW) & (bottom <= HIGH)
                bad_out[0:1] = jnp.maximum(bad_out[0:1], jnp.where(fine, 0.0, 1.0))
            else:
                acc[h] = total

    def out_copy(i):
        wide = AT_ONCE * HEAD
        lanes = pl.ds(i * wide if isinstance(i, int) else pl.multiple_of(i * wide, wide), wide)
        return pltpu.make_async_copy(q_buf.at[:, lanes], out_hbm.at[:, lanes], out_sem.at[i])

    def group(items, size, event, before):
        begin, end = before is None, event is event_six
        per = GROUP // size
        event(0)
        if before is not None:
            gather(before[0], HEADS - before[1], before[1], before[2], False)
        weigh(items, 0, size)

        def inner(i):
            if end:
                @pl.when(i >= 2)
                def _():
                    out_copy(i - 2).start()
            gather(items, size * (i - 1), size, begin, end)
            weigh(items, size * i, size)

        for j in range(1, per):
            inner(j)

        def outer(c, _):
            event(c)
            lax.fori_loop(0, per, lambda j, _: (inner(per * c + j), 0)[1], 0)
            return 0

        lax.fori_loop(1, KV_HEADS, outer, 0)
        return items, size, begin

    def event_two(c):
        here((), (4,), c)
        send_up(value_copy, 4, 8, c)
        send_right(value_copy, 4, 5, c, x < 3)
        send_right(key_copy, 4, 1, c, x == 3)
        send_left(key_copy, 4, 3, c, x > 0)

    def event_three(c):
        here((1, 8), (3,), c)
        send_up(key_copy, 3, 7, c)
        send_right(value_copy, 1, 2, c, x < 3)
        send_right(value_copy, 8, 5, c, x == 3)
        send_left(value_copy, 8, 7, c, x > 0)
        send_left(value_copy, 4, 7, c, x == 0)

    def event_four(c):
        here((3, 5, 7), (1,), c)
        send_up(key_copy, 1, 5, c)
        send_right(key_copy, 1, 2, c, x < 3)
        send_right(value_copy, 5, 2, c, x == 3)
        send_left(value_copy, 7, 6, c, x > 0)
        send_left(value_copy, 3, 6, c, x == 0)

    def event_five(c):
        here((), (5, 7), c)
        send_up(key_copy, 4, 8, c)
        send_right(key_copy, 5, 2, c, x == 3)
        send_left(key_copy, 7, 6, c, x > 0)
        send_left(key_copy, 3, 6, c, x == 0)

    def kept(refs, out, sems, d):
        return pltpu.make_async_copy(refs.at[d], out.at[d], sems.at[d])

    def keep(*items):
        for d in items:
            kept(wk, wk_hbm, wk_sem, d).start()
            kept(wv, wv_hbm, wv_sem, d).start()

    def event_six(c):
        here((2, 6), (2, 6, 8), c)

    before = group((0,), GROUP, event_two, None)
    keep(0)
    before = group((4,), GROUP, event_three, before)
    keep(4)
    before = group((1, 3), AT_ONCE, event_four, before)
    keep(1, 3)
    before = group((5, 7), AT_ONCE, event_five, before)
    keep(5, 7)
    group((2, 6, 8), AT_ONCE, event_six, before)
    keep(2, 6, 8)
    out_copy(6).start()
    gather((2, 6, 8), HEADS - AT_ONCE, AT_ONCE, False, True)
    out_copy(7).start()

    for d in range(1, 9):
        @pl.when(me + d < count)
        def _():
            doc_copy(d).wait_send()

    def drain(c, _):
        for d in range(1, 9):
            if d in (4, 8):
                sent = (me + 4 < count) & (d - 4 <= me)
                sent_key = sent
            elif d in (1, 2):
                sent = jnp.where(x < 3, d - 1, d + 3) <= me
                sent_key = sent
            elif d in (3, 6):
                sent = jnp.where(x > 0, d + 1, d - 3) <= me
                sent_key = sent
            elif d == 5:
                sent = jnp.where(x < 3, d - 1, d + 3) <= me
                sent_key = (me + 4 < count) & (d - 4 <= me)
            else:
                sent = jnp.where(x > 0, d + 1, d - 3) <= me
                sent_key = (me + 4 < count) & (d - 4 <= me)

            @pl.when(sent)
            def _():
                value_copy(d, d, c, up).wait_send()

            @pl.when(sent_key)
            def _():
                key_copy(d, d, c, up).wait_send()
        return 0

    lax.fori_loop(0, KV_HEADS, drain, 0)
    for d in range(ITEMS):
        kept(wk, wk_hbm, wk_sem, d).wait()
        kept(wv, wv_hbm, wv_sem, d).wait()
    qt_copy.wait()
    for i in range(HEADS // AT_ONCE):
        out_copy(i).wait()


def finish(found, start, bad, qt_hbm, wk_hbm, wv_hbm, out, q_buf, k_buf, v_buf, o_buf, sems):
    del found

    @pl.when(jnp.logical_not(jnp.max(bad[...]) < 0.5))
    def _():
        query = lax.broadcasted_iota(jnp.int32, (ROWS, ROWS), 1).astype(jnp.float32)
        key = lax.broadcasted_iota(jnp.int32, (ROWS, ROWS), 0).astype(jnp.float32)
        begin = start[0:1]

        def of_head(h, _):
            copies = [
                pltpu.make_async_copy(qt_hbm.at[h], q_buf, sems.at[0]),
                pltpu.make_async_copy(wk_hbm.at[:, h // GROUP], k_buf, sems.at[1]),
                pltpu.make_async_copy(wv_hbm.at[:, h // GROUP], v_buf, sems.at[2]),
            ]
            for copy in copies:
                copy.start()
            for copy in copies:
                copy.wait()

            def scores(d):
                at = key - (d * ROWS).astype(jnp.float32)
                product = lax.dot_general(k_buf[d], q_buf[...], (((1,), (0,)), ((), ())),
                                          preferred_element_type=jnp.float32)
                return jnp.where((at >= begin) & (at <= query), product * SCALE, MASKED)

            def highest(d, top):
                return jnp.maximum(top, jnp.max(scores(d), axis=0, keepdims=True))

            top = lax.fori_loop(0, ITEMS, highest, jnp.full((1, ROWS), MASKED, jnp.float32))

            def summed(d, carry):
                bottom, total = carry
                weights = jnp.exp2(scores(d) - top)
                bottom = bottom + jnp.sum(weights, axis=0, keepdims=True)
                part = lax.dot_general(v_buf[d, 0:HEAD], weights.astype(jnp.bfloat16), (((1,), (0,)), ((), ())),
                                       preferred_element_type=jnp.float32)
                return bottom, total + part

            bottom, total = lax.fori_loop(
                0, ITEMS, summed, (jnp.zeros((1, ROWS), jnp.float32), jnp.zeros((HEAD, ROWS), jnp.float32)))
            o_buf[...] = (total / bottom).astype(jnp.bfloat16).T
            put = pltpu.make_async_copy(o_buf, out.at[:, pl.ds(pl.multiple_of(h * HEAD, HEAD), HEAD)], sems.at[3])
            put.start()
            put.wait()
            return 0

        lax.fori_loop(0, HEADS, of_head, 0)


def shards(documents, queries, key_projection_rows, value_projection_rows):
    bf, f32 = jnp.bfloat16, jnp.float32
    powers = np.float32(1000000.0) ** (-2.0 * np.arange(HEAD // 2, dtype=np.float32) / HEAD)
    inverse = jnp.asarray(np.tile(powers, 2)[None, :], f32)
    vmem, whole = pl.BlockSpec(memory_space=VMEM), pl.BlockSpec(memory_space=pl.ANY)
    dma = pltpu.SemaphoreType.DMA
    flops = 4 * HEADS * ROWS * ITEMS * ROWS * HEAD
    per_item = (ITEMS, KV_HEADS)
    found, q_t, wk, wv, start, bad = pl.pallas_call(
        attend,
        out_shape=[
            jax.ShapeDtypeStruct((ROWS, HEADS * HEAD), bf),
            jax.ShapeDtypeStruct((HEADS, HEAD, ROWS), bf),
            jax.ShapeDtypeStruct((ITEMS, KV_HEADS, ROWS, HEAD), bf),
            jax.ShapeDtypeStruct((ITEMS, KV_HEADS, VALUE_ROWS, ROWS), bf),
            jax.ShapeDtypeStruct((8, ROWS), f32),
            jax.ShapeDtypeStruct((8, ROWS), f32),
        ],
        in_specs=[whole, vmem, whole, whole, whole],
        out_specs=[whole] * 4 + [vmem] * 2,
        scratch_shapes=[
            VMEM((1, ROWS), jnp.int32),
            VMEM((ROWS, KV_HEADS * HEAD), bf),
            VMEM((ROWS, KV_HEADS * HEAD), bf),
            VMEM((ROWS, HEADS * HEAD), bf),
            VMEM((HEADS, HEAD, ROWS), bf),
            VMEM((ITEMS, KV_HEADS, ROWS, HEAD), bf),
            VMEM((ITEMS, KV_HEADS, VALUE_ROWS, ROWS), bf),
            VMEM((ITEMS, ROWS, ROWS), f32),
            VMEM((HEADS, VALUE_ROWS, ROWS), f32),
            VMEM((AT_ONCE * MOST_AT_ONCE, ROWS, ROWS), bf),
            VMEM((8, 1, ROWS), jnp.int32),
            VMEM((HEAD // 2, ROWS), f32),
            VMEM((HEAD // 2, ROWS), f32),
            dma(per_item), dma(per_item), dma(per_item), dma(per_item),
            dma((8,)), dma((8,)), dma((4,)), dma((HEADS // AT_ONCE,)), dma, dma((ITEMS,)), dma((ITEMS,)),
        ],
        compiler_params=pltpu.CompilerParams(collective_id=0, has_side_effects=True, vmem_limit_bytes=67043328),
        cost_estimate=pl.CostEstimate(flops=flops, bytes_accessed=12 * 2**20, transcendentals=HEADS * ROWS * ITEMS * ROWS),
        name="attend",
    )(documents.reshape(1, ROWS), inverse, queries, key_projection_rows, value_projection_rows)
    return pl.pallas_call(
        finish,
        out_shape=jax.ShapeDtypeStruct((ROWS, HEADS * HEAD), bf),
        in_specs=[whole, vmem, vmem, whole, whole, whole],
        out_specs=whole,
        input_output_aliases={0: 0},
        scratch_shapes=[
            VMEM((HEAD, ROWS), bf),
            VMEM((ITEMS, ROWS, HEAD), bf),
            VMEM((ITEMS, VALUE_ROWS, ROWS), bf),
            VMEM((ROWS, HEAD), bf),
            dma((4,)),
        ],
        compiler_params=pltpu.CompilerParams(vmem_limit_bytes=67043328),
        cost_estimate=pl.CostEstimate(flops=2**20, bytes_accessed=2**14, transcendentals=0),
        name="finish",
    )(found, start, bad, q_t, wk, wv)


def solution(mesh):
    in_specs = (
        P(("dp", "ctx")),
        P(("dp", "ctx"), None),
        P(("dp", "ctx"), None),
        P(("dp", "ctx"), None),
    )
    out_specs = P(("dp", "ctx"), None)
    return jax.shard_map(shards, mesh=mesh, in_specs=in_specs, out_specs=out_specs, check_vma=False)
```

```python
import functools
import math
import jax
import jax.numpy as jnp
import numpy as np
from jax import lax
from jax.experimental import pallas as pl
from jax.experimental.pallas import tpu as pltpu
from jax.sharding import PartitionSpec as P

HEAD = 128
HEADS = 32
KV_HEADS = 4
GROUP = HEADS // KV_HEADS
ROWS = 256
ITEMS = 9
VALUE_ROWS = 144
AT_ONCE = 4
MOST_AT_ONCE = 3
SCALE = math.log2(math.e) / math.sqrt(HEAD)
LOW = 1e-25
HIGH = 1e37
MASKED = -1e30
MESH = pl.DeviceIdType.MESH
UP, RIGHT, LEFT, RELAY = range(4)
V, K = range(2)
SOURCES = {(UP, 4): (0, 0), (UP, 5): (1, 1), (UP, 6): (2, 2), (UP, 7): (3, 3), (UP, 8): (4, 4), (RIGHT, 1): (0, 4),
           (RIGHT, 2): (1, 5), (RIGHT, 5): (4, 8), (LEFT, 3): (4, 0), (LEFT, 6): (7, 3), (LEFT, 7): (8, 4)}
ROUTE = {(1, K): RIGHT, (1, V): RIGHT, (2, K): RIGHT, (2, V): RIGHT, (3, K): LEFT, (3, V): LEFT, (4, K): UP, (4, V): UP, (5, K): UP, (5, V): RIGHT, (6, K): LEFT, (6, V): UP, (7, K): LEFT, (7, V): UP, (8, K): RELAY, (8, V): RELAY}
ARRIVE = {(1, K): (2, 4), (1, V): (1, 9), (2, K): (5, 3), (2, V): (4, 6), (3, K): (3, 2), (3, V): (1, 11), (4, K): (1, 7), (4, V): (0, 14), (5, K): (4, 12), (5, V): (3, 13), (6, K): (5, 15), (6, V): (5, 8), (7, K): (4, 5), (7, V): (3, 0), (8, K): (2, 1), (8, V): (2, 10)}
LEAVE = {(1, K, 1): 1, (1, V, 1): 0, (2, K, 0): 3, (2, K, 1): 4, (2, V, 0): 2, (2, V, 1): 3, (3, K, 0): 1, (3, V, 0): 0, (5, K, 0): 2, (5, V, 0): 1, (5, V, 1): 2, (6, K, 0): 4, (6, K, 1): 3, (6, V, 0): 4, (7, K, 0): 2, (7, K, 1): 1, (7, V, 0): 1}
RELAYED = {V: (0, 0), K: (1, 0)}
RELAY_KEYS_AT = 0
GROUPS = ((0,), (1, 4), (8,), (5, 3, 7), (2, 6))
SIZES = (8, 4, 8, 4, 4)
VMEM = pltpu.VMEM


def attend(doc_hbm, inverse, q_hbm, k_hbm, v_hbm, out_hbm, qt_hbm, wk_hbm, wv_hbm, start_out, bad_out,
           docs, k_buf, v_buf, q_buf, q_t, wk, wv, bias, acc, probs, doc_win, cosine, sine,
           rk, rv, sk, sv, relay_v, relay_k, relay_sems, doc_send, doc_recv, in_sem, out_sem, qt_sem, wk_sem, wv_sem):
    count = lax.axis_size("ctx")
    me = lax.axis_index("ctx")
    x = lax.rem(me, 4)
    row = me - x
    right = row + lax.rem(x + 1, 4)
    left = row + lax.rem(x + 3, 4)
    up = lax.rem(me + 4, count)

    plane = me - lax.rem(me, 16)
    y = lax.rem(me // 4, 4)
    down = plane + 4 * lax.rem(y + 3, 4) + x
    above = plane + 4 * lax.rem(y + 1, 4) + x
    behind_8 = me + count - 8
    far = lax.rem(behind_8, count)
    relay = far - lax.rem(far, 16) + 4 * lax.rem(lax.rem(far // 4, 4) + 3, 4) + x

    barrier = pltpu.get_barrier_semaphore()

    def greet(other):
        pl.semaphore_signal(barrier, inc=1, device_id={"ctx": other}, device_id_type=MESH)

    for d in range(1, 9):
        @pl.when(d <= me)
        def _():
            greet(lax.rem(me + count - d, count))
    greet(left)
    greet(right)

    @pl.when(above + 8 < count)
    def _():
        greet(above)

    @pl.when(me >= 8)
    def _():
        greet(relay)

    loads = [pltpu.make_async_copy(a, b, in_sem.at[n])
             for n, (a, b) in enumerate([(v_hbm, v_buf), (doc_hbm, docs), (k_hbm, k_buf), (q_hbm, q_buf)])]
    for load in loads:
        load.start()

    def value_copy(src, dst, c, target):
        return pltpu.make_async_remote_copy(
            wv.at[src, c, pl.ds(0, HEAD)], wv.at[dst, c, pl.ds(0, HEAD)], sv.at[dst, c], rv.at[dst, c],
            device_id={"ctx": target}, device_id_type=MESH)

    def key_copy(src, dst, c, target):
        return pltpu.make_async_remote_copy(
            wk.at[src, c], wk.at[dst, c], sk.at[dst, c], rk.at[dst, c],
            device_id={"ctx": target}, device_id_type=MESH)

    def doc_copy(d):
        return pltpu.make_async_remote_copy(
            docs, doc_win.at[d - 1], doc_send.at[d - 1], doc_recv.at[d - 1],
            device_id={"ctx": lax.rem(me + d, count)}, device_id_type=MESH)

    def when_sent(condition, copy):
        @pl.when(condition)
        def _():
            copy.start()

    def relay_copy(kind, c):
        buf = relay_v if kind == V else relay_k
        mine = wv.at[0, c, pl.ds(0, HEAD)] if kind == V else wk.at[0, c]
        return pltpu.make_async_remote_copy(
            mine, buf.at[c], relay_sems.at[kind, 0, c], relay_sems.at[kind, 1, c],
            device_id={"ctx": down}, device_id_type=MESH)

    def relayed_copy(kind, c):
        if kind == V:
            return pltpu.make_async_remote_copy(
                relay_v.at[c], wv.at[8, c, pl.ds(0, HEAD)], relay_sems.at[kind, 2, c], rv.at[8, c],
                device_id={"ctx": lax.rem(above + 8, count)}, device_id_type=MESH)
        return pltpu.make_async_remote_copy(
            relay_k.at[c], wk.at[8, c], relay_sems.at[kind, 2, c], rk.at[8, c],
            device_id={"ctx": lax.rem(above + 8, count)}, device_id_type=MESH)

    def relay_own(kind, c):
        if kind in RELAYED:
            when_sent(me + 8 < count, relay_copy(kind, c))

    def relay_keys(stage):
        if K in RELAYED and stage == RELAY_KEYS_AT:
            for c in range(KV_HEADS):
                relay_own(K, c)

    def relay_event(stage, late, c):
        for kind in RELAYED:
            if RELAYED[kind] == (stage, late):
                @pl.when(above + 8 < count)
                def _():
                    relay_copy(kind, c).wait_recv()
                    relayed_copy(kind, c).start()

    def drain_relays(c):
        for kind in RELAYED:
            @pl.when(me + 8 < count)
            def _():
                relay_copy(kind, c).wait_send()

            @pl.when(above + 8 < count)
            def _():
                relayed_copy(kind, c).wait_send()

    def copy_of(kind):
        return value_copy if kind == V else key_copy

    def ways(d, kind):
        link = ROUTE[d, kind]
        if link == RELAY:
            return []
        plain, edge = SOURCES[link, d]
        if link == UP:
            return [(0, plain, up, me + 4 < count)]
        special = x == 3 if link == RIGHT else x == 0
        target = right if link == RIGHT else left
        return [(0, plain, target, jnp.logical_not(special)), (1, edge, target, special)]

    def send(way, d, kind, c):
        _, src, target, there = way
        when_sent(there & (src <= me), copy_of(kind)(src, d, c, target))

    def send_own(kind, c):
        for d in (4, 1, 3):
            for way in ways(d, kind):
                if way[1] == 0:
                    send(way, d, kind, c)

    def stage_event(stage, c):
        first, after = [], {}
        for (d, kind) in ROUTE:
            for way in ways(d, kind):
                if way[1] != 0 and LEAVE[d, kind, way[0]] == stage:
                    if ARRIVE[way[1], kind][0] < stage:
                        first.append((way, d, kind))
                    else:
                        after.setdefault((way[1], kind), []).append((way, d, kind))
        for entry in first:
            send(*entry, c)
        relay_event(stage, 0, c)
        for d, kind in sorted((e for e in ARRIVE if ARRIVE[e][0] == stage), key=lambda e: ARRIVE[e][1]):
            @pl.when(d <= me)
            def _():
                copy_of(kind)(d, d, c, up).wait_recv()
            for entry in after.get((d, kind), []):
                send(*entry, c)
        relay_event(stage, 1, c)

    wv[:, :, HEAD:, :] = jnp.ones((ITEMS, KV_HEADS, VALUE_ROWS - HEAD, ROWS), jnp.bfloat16)
    loads[0].wait()
    for c in range(KV_HEADS):
        wv[0, c, 0:HEAD] = v_buf[:, c * HEAD:(c + 1) * HEAD].T
    loads[1].wait()
    pl.semaphore_wait(barrier, 2 + jnp.minimum(8, count - 1 - me) + jnp.where(me + 8 < count, 1, 0)
                      + jnp.where(above + 8 < count, 1, 0))
    for d in range(1, 9):
        when_sent(me + d < count, doc_copy(d))
    for c in range(KV_HEADS):
        send_own(V, c)
        relay_own(V, c)
    loads[3].wait()

    def turn(n, _):
        for u in range(4):
            at = pl.multiple_of((4 * n + u) * HEAD, HEAD)
            q_t[4 * n + u] = q_buf[:, pl.ds(at, HEAD)].T
        return 0

    lax.fori_loop(0, HEADS // 4, turn, 0)
    for d in range(1, 9):
        @pl.when(d > me)
        def _():
            wk[d] = jnp.zeros((KV_HEADS, ROWS, HEAD), jnp.bfloat16)
            wv[d, :, 0:HEAD] = jnp.zeros((KV_HEADS, HEAD, ROWS), jnp.bfloat16)

    doc_row = docs[...].astype(jnp.float32)
    columns = jnp.transpose(jnp.broadcast_to(doc_row, (ROWS, ROWS)))
    local = jnp.sum((columns < doc_row).astype(jnp.float32), axis=0, keepdims=True)
    first = doc_row[:, 0:1]
    powers = jnp.transpose(jnp.broadcast_to(inverse[...], (HEAD, HEAD)))[0:HEAD // 2]
    powers = jnp.concatenate([powers, powers], axis=1)
    tokens = lax.broadcasted_iota(jnp.int32, (1, ROWS), 1).astype(jnp.float32)
    loads[2].wait()
    for d in range(1, 9):
        @pl.when(d <= me)
        def _():
            doc_copy(d).wait_recv()
    behind = jnp.zeros((1, ROWS), jnp.float32)
    for d in range(1, 9):
        same = (doc_win[d - 1].astype(jnp.float32) == first) & (d <= me)
        behind = behind + jnp.where(same, 1.0, 0.0)
    behind = jnp.sum(behind, axis=1, keepdims=True)
    start = jnp.where(doc_row == first, -behind, local)
    start_out[...] = jnp.broadcast_to(start, (8, ROWS))
    angles = powers * (tokens - start)
    cosine[...] = jnp.cos(angles)
    sine[...] = jnp.sin(angles)

    def rotated(matrix):
        wide = matrix.astype(jnp.float32)
        a, b = wide[0:HEAD // 2], wide[HEAD // 2:]
        co, si = cosine[...], sine[...]
        return jnp.concatenate([a * co - b * si, b * co + a * si], axis=0)

    for c in range(KV_HEADS):
        wk[0, c] = rotated(k_buf[:, c * HEAD:(c + 1) * HEAD].T).T.astype(jnp.bfloat16)
    query = lax.broadcasted_iota(jnp.int32, (ROWS, ROWS), 1).astype(jnp.float32)
    key = lax.broadcasted_iota(jnp.int32, (ROWS, ROWS), 0).astype(jnp.float32)
    bias[0] = jnp.where((key >= start) & (key <= query), 0.0, MASKED)
    for c in range(KV_HEADS):
        send_own(K, c)
    for d in range(1, ITEMS):
        at = key - float(ROWS * d)
        bias[d] = jnp.where((at >= start) & (at <= query), 0.0, MASKED)

    def step_one(c, _):
        stage_event(0, c)

        def turned(n, _):
            for u in range(4):
                h = c * GROUP + 4 * n + u
                q_t[h] = rotated(q_t[h]).astype(jnp.bfloat16)
            return 0

        lax.fori_loop(0, GROUP // 4, turned, 0)
        return 0

    relay_keys(0)
    lax.fori_loop(0, KV_HEADS, step_one, 0)
    qt_copy = pltpu.make_async_copy(q_t, qt_hbm, qt_sem)
    qt_copy.start()
    bad_out[...] = jnp.zeros((8, ROWS), jnp.float32)

    def weigh(items, at, size):
        for u in range(size):
            h = at + u
            for n, d in enumerate(items):
                scores = lax.dot_general(wk[d, h // GROUP], q_t[h], (((1,), (0,)), ((), ())),
                                         preferred_element_type=jnp.float32)
                probs[u * len(items) + n] = jnp.exp2(scores * SCALE + bias[d]).astype(jnp.bfloat16)

    def gather(items, at, size, begin, end):
        for u in range(size):
            h = at + u
            total = None
            for n, d in enumerate(items):
                part = lax.dot_general(wv[d, h // GROUP], probs[u * len(items) + n], (((1,), (0,)), ((), ())),
                                       preferred_element_type=jnp.float32)
                total = part if total is None else total + part
            if not begin:
                total = acc[h] + total
            if end:
                bottom = total[HEAD:HEAD + 1]
                lane = h * HEAD if isinstance(h, int) else pl.multiple_of(h * HEAD, HEAD)
                q_buf[:, pl.ds(lane, HEAD)] = (total[0:HEAD] * (1.0 / bottom)).astype(jnp.bfloat16).T
                fine = (bottom >= LOW) & (bottom <= HIGH)
                bad_out[0:1] = jnp.maximum(bad_out[0:1], jnp.where(fine, 0.0, 1.0))
            else:
                acc[h] = total

    def out_copy(i):
        wide = AT_ONCE * HEAD
        lanes = pl.ds(i * wide if isinstance(i, int) else pl.multiple_of(i * wide, wide), wide)
        return pltpu.make_async_copy(q_buf.at[:, lanes], out_hbm.at[:, lanes], out_sem.at[i])

    def group(items, size, stage, before):
        begin, end = before is None, stage == len(GROUPS)
        per = GROUP // size
        stage_event(stage, 0)
        if before is not None:
            gather(before[0], HEADS - before[1], before[1], before[2], False)
        weigh(items, 0, size)

        def inner(i):
            if end:
                @pl.when(i >= 2)
                def _():
                    out_copy(i - 2).start()
            gather(items, size * (i - 1), size, begin, end)
            weigh(items, size * i, size)

        for j in range(1, per):
            inner(j)

        def outer(c, _):
            stage_event(stage, c)
            lax.fori_loop(0, per, lambda j, _: (inner(per * c + j), 0)[1], 0)
            return 0

        lax.fori_loop(1, KV_HEADS, outer, 0)
        return items, size, begin

    def kept(refs, out, sems, d):
        return pltpu.make_async_copy(refs.at[d], out.at[d], sems.at[d])

    def keep(*items):
        for d in items:
            kept(wk, wk_hbm, wk_sem, d).start()
            kept(wv, wv_hbm, wv_sem, d).start()

    before = None
    for n, items in enumerate(GROUPS):
        relay_keys(n + 1)
        before = group(items, SIZES[n], n + 1, before)
        keep(*items)
    out_copy(6).start()
    gather(GROUPS[-1], HEADS - AT_ONCE, AT_ONCE, False, True)
    out_copy(7).start()

    for d in range(1, 9):
        @pl.when(me + d < count)
        def _():
            doc_copy(d).wait_send()

    def drain(c, _):
        for (d, kind) in ROUTE:
            for way in ways(d, kind):
                @pl.when(way[3] & (way[1] <= me))
                def _():
                    copy_of(kind)(d, d, c, up).wait_send()
        drain_relays(c)
        return 0

    lax.fori_loop(0, KV_HEADS, drain, 0)
    for d in range(ITEMS):
        kept(wk, wk_hbm, wk_sem, d).wait()
        kept(wv, wv_hbm, wv_sem, d).wait()
    qt_copy.wait()
    for i in range(HEADS // AT_ONCE):
        out_copy(i).wait()


def finish(found, start, bad, qt_hbm, wk_hbm, wv_hbm, out, o_buf, q_buf, k_buf, v_buf, sems, in_sems, out_sems):
    pieces = 8
    tall = ROWS // pieces

    def taken(i):
        return pltpu.make_async_copy(found.at[pl.ds(i * tall, tall)], o_buf.at[pl.ds(i * tall, tall)], in_sems.at[i])

    def given(i):
        return pltpu.make_async_copy(o_buf.at[pl.ds(i * tall, tall)], out.at[pl.ds(i * tall, tall)], out_sems.at[i])

    for i in range(pieces):
        taken(i).start()
    fine = jnp.max(bad[...]) < 0.5

    @pl.when(fine)
    def _():
        for i in range(pieces):
            taken(i).wait()
            given(i).start()

    @pl.when(jnp.logical_not(fine))
    def _():
        for i in range(pieces):
            taken(i).wait()
        query = lax.broadcasted_iota(jnp.int32, (ROWS, ROWS), 1).astype(jnp.float32)
        key = lax.broadcasted_iota(jnp.int32, (ROWS, ROWS), 0).astype(jnp.float32)
        begin = start[0:1]

        def of_head(h, _):
            copies = [
                pltpu.make_async_copy(qt_hbm.at[h], q_buf, sems.at[0]),
                pltpu.make_async_copy(wk_hbm.at[:, h // GROUP], k_buf, sems.at[1]),
                pltpu.make_async_copy(wv_hbm.at[:, h // GROUP], v_buf, sems.at[2]),
            ]
            for copy in copies:
                copy.start()
            for copy in copies:
                copy.wait()

            def scores(d):
                at = key - (d * ROWS).astype(jnp.float32)
                product = lax.dot_general(k_buf[d], q_buf[...], (((1,), (0,)), ((), ())),
                                          preferred_element_type=jnp.float32)
                return jnp.where((at >= begin) & (at <= query), product * SCALE, MASKED)

            def highest(d, top):
                return jnp.maximum(top, jnp.max(scores(d), axis=0, keepdims=True))

            top = lax.fori_loop(0, ITEMS, highest, jnp.full((1, ROWS), MASKED, jnp.float32))

            def summed(d, carry):
                bottom, total = carry
                weights = jnp.exp2(scores(d) - top)
                bottom = bottom + jnp.sum(weights, axis=0, keepdims=True)
                part = lax.dot_general(v_buf[d, 0:HEAD], weights.astype(jnp.bfloat16), (((1,), (0,)), ((), ())),
                                       preferred_element_type=jnp.float32)
                return bottom, total + part

            bottom, total = lax.fori_loop(
                0, ITEMS, summed, (jnp.zeros((1, ROWS), jnp.float32), jnp.zeros((HEAD, ROWS), jnp.float32)))
            o_buf[:, pl.ds(pl.multiple_of(h * HEAD, HEAD), HEAD)] = (total / bottom).astype(jnp.bfloat16).T
            return 0

        lax.fori_loop(0, HEADS, of_head, 0)
        for i in range(pieces):
            given(i).start()

    for i in range(pieces):
        given(i).wait()


def shards(documents, queries, key_projection_rows, value_projection_rows):
    bf, f32 = jnp.bfloat16, jnp.float32
    powers = np.float32(1000000.0) ** (-2.0 * np.arange(HEAD // 2, dtype=np.float32) / HEAD)
    inverse = jnp.asarray(np.tile(powers, 2)[None, :], f32)
    vmem, whole = pl.BlockSpec(memory_space=VMEM), pl.BlockSpec(memory_space=pl.ANY)
    dma = pltpu.SemaphoreType.DMA
    flops = 4 * HEADS * ROWS * ITEMS * ROWS * HEAD
    per_item = (ITEMS, KV_HEADS)
    found, q_t, wk, wv, start, bad = pl.pallas_call(
        attend,
        out_shape=[
            jax.ShapeDtypeStruct((ROWS, HEADS * HEAD), bf),
            jax.ShapeDtypeStruct((HEADS, HEAD, ROWS), bf),
            jax.ShapeDtypeStruct((ITEMS, KV_HEADS, ROWS, HEAD), bf),
            jax.ShapeDtypeStruct((ITEMS, KV_HEADS, VALUE_ROWS, ROWS), bf),
            jax.ShapeDtypeStruct((8, ROWS), f32),
            jax.ShapeDtypeStruct((8, ROWS), f32),
        ],
        in_specs=[whole, vmem, whole, whole, whole],
        out_specs=[whole] * 4 + [vmem] * 2,
        scratch_shapes=[
            VMEM((1, ROWS), jnp.int32),
            VMEM((ROWS, KV_HEADS * HEAD), bf),
            VMEM((ROWS, KV_HEADS * HEAD), bf),
            VMEM((ROWS, HEADS * HEAD), bf),
            VMEM((HEADS, HEAD, ROWS), bf),
            VMEM((ITEMS, KV_HEADS, ROWS, HEAD), bf),
            VMEM((ITEMS, KV_HEADS, VALUE_ROWS, ROWS), bf),
            VMEM((ITEMS, ROWS, ROWS), f32),
            VMEM((HEADS, VALUE_ROWS, ROWS), f32),
            VMEM((AT_ONCE * MOST_AT_ONCE, ROWS, ROWS), bf),
            VMEM((8, 1, ROWS), jnp.int32),
            VMEM((HEAD // 2, ROWS), f32),
            VMEM((HEAD // 2, ROWS), f32),
            dma(per_item), dma(per_item), dma(per_item), dma(per_item),
            VMEM((KV_HEADS, HEAD, ROWS), bf), VMEM((KV_HEADS, ROWS, HEAD), bf), dma((2, 3, KV_HEADS)),
            dma((8,)), dma((8,)), dma((4,)), dma((HEADS // AT_ONCE,)), dma, dma((ITEMS,)), dma((ITEMS,)),
        ],
        compiler_params=pltpu.CompilerParams(collective_id=0, has_side_effects=True, vmem_limit_bytes=67043328),
        cost_estimate=pl.CostEstimate(flops=flops, bytes_accessed=12 * 2**20, transcendentals=HEADS * ROWS * ITEMS * ROWS),
        name="attend",
    )(documents.reshape(1, ROWS), inverse, queries, key_projection_rows, value_projection_rows)
    return pl.pallas_call(
        finish,
        out_shape=jax.ShapeDtypeStruct((ROWS, HEADS * HEAD), bf),
        in_specs=[whole, vmem, vmem, whole, whole, whole],
        out_specs=whole,
        scratch_shapes=[
            VMEM((ROWS, HEADS * HEAD), bf),
            VMEM((HEAD, ROWS), bf),
            VMEM((ITEMS, ROWS, HEAD), bf),
            VMEM((ITEMS, VALUE_ROWS, ROWS), bf),
            dma((3,)), dma((8,)), dma((8,)),
        ],
        compiler_params=pltpu.CompilerParams(vmem_limit_bytes=67043328),
        cost_estimate=pl.CostEstimate(flops=2**20, bytes_accessed=2**14, transcendentals=0),
        name="finish",
    )(found, start, bad, q_t, wk, wv)


def solution(mesh):
    in_specs = (
        P(("dp", "ctx")),
        P(("dp", "ctx"), None),
        P(("dp", "ctx"), None),
        P(("dp", "ctx"), None),
    )
    out_specs = P(("dp", "ctx"), None)
    return jax.shard_map(shards, mesh=mesh, in_specs=in_specs, out_specs=out_specs, check_vma=False)
```

```python
import functools
import math
import jax
import jax.numpy as jnp
import numpy as np
from jax import lax
from jax.experimental import pallas as pl
from jax.experimental.pallas import tpu as pltpu
from jax.sharding import PartitionSpec as P

HEAD = 128
HEADS = 32
KV_HEADS = 4
GROUP = HEADS // KV_HEADS
ROWS = 256
ITEMS = 9
VALUE_ROWS = 144
AT_ONCE = 4
MOST_AT_ONCE = 3
SCALE = math.log2(math.e) / math.sqrt(HEAD)
LOW = 1e-25
HIGH = 1e37
MASKED = -1e30
MESH = pl.DeviceIdType.MESH
UP, RIGHT, LEFT, RELAY = range(4)
V, K = range(2)
SOURCES = {(UP, 4): (0, 0), (UP, 5): (1, 1), (UP, 6): (2, 2), (UP, 7): (3, 3), (UP, 8): (4, 4), (RIGHT, 1): (0, 4),
           (RIGHT, 2): (1, 5), (RIGHT, 5): (4, 8), (LEFT, 3): (4, 0), (LEFT, 6): (7, 3), (LEFT, 7): (8, 4)}
ROUTE = {(1, K): RIGHT, (1, V): RIGHT, (2, K): RIGHT, (2, V): RIGHT, (3, K): LEFT, (3, V): LEFT, (4, K): UP, (4, V): UP, (5, K): UP, (5, V): RIGHT, (6, K): LEFT, (6, V): UP, (7, K): LEFT, (7, V): UP, (8, K): RELAY, (8, V): RELAY}
ARRIVE = {(1, K): (2, 4), (1, V): (1, 9), (2, K): (5, 3), (2, V): (4, 6), (3, K): (3, 2), (3, V): (1, 11), (4, K): (1, 7), (4, V): (0, 14), (5, K): (4, 12), (5, V): (3, 13), (6, K): (5, 15), (6, V): (5, 8), (7, K): (4, 5), (7, V): (3, 0), (8, K): (2, 1), (8, V): (2, 10)}
LEAVE = {(1, K, 1): 1, (1, V, 1): 0, (2, K, 0): 3, (2, K, 1): 4, (2, V, 0): 2, (2, V, 1): 3, (3, K, 0): 1, (3, V, 0): 0, (5, K, 0): 2, (5, V, 0): 1, (5, V, 1): 2, (6, K, 0): 4, (6, K, 1): 3, (6, V, 0): 4, (7, K, 0): 2, (7, K, 1): 1, (7, V, 0): 1}
RELAYED = {V: (0, 0), K: (1, 0)}
RELAY_KEYS_AT = 0
GROUPS = ((0,), (1, 4), (8,), (5, 3, 7), (2, 6))
SIZES = (8, 4, 8, 4, 4)
VMEM = pltpu.VMEM


def attend(doc_hbm, inverse, q_hbm, k_hbm, v_hbm, out_hbm, qt_hbm, wk_hbm, wv_hbm, start_out, bad_out,
           docs, k_buf, v_buf, q_buf, q_t, wk, wv, bias, acc, probs, doc_win, cosine, sine,
           rk, rv, sk, sv, relay_v, relay_k, relay_sems, doc_send, doc_recv, in_sem, out_sem, qt_sem, wk_sem, wv_sem):
    count = lax.axis_size("ctx")
    me = lax.axis_index("ctx")
    x = lax.rem(me, 4)
    row = me - x
    right = row + lax.rem(x + 1, 4)
    left = row + lax.rem(x + 3, 4)
    up = lax.rem(me + 4, count)

    plane = me - lax.rem(me, 16)
    y = lax.rem(me // 4, 4)
    down = plane + 4 * lax.rem(y + 3, 4) + x
    above = plane + 4 * lax.rem(y + 1, 4) + x
    ahead = lax.rem(me + 8, count)
    relay = ahead - lax.rem(ahead, 16) + 4 * lax.rem(lax.rem(ahead // 4, 4) + 1, 4) + x

    barrier = pltpu.get_barrier_semaphore()

    def greet(other):
        pl.semaphore_signal(barrier, inc=1, device_id={"ctx": other}, device_id_type=MESH)

    for d in range(1, 9):
        @pl.when(d <= me)
        def _():
            greet(lax.rem(me + count - d, count))
    greet(left)
    greet(right)

    @pl.when(down >= 8)
    def _():
        greet(lax.rem(down + count - 8, count))

    @pl.when(me >= 8)
    def _():
        greet(above)

    loads = [pltpu.make_async_copy(a, b, in_sem.at[n])
             for n, (a, b) in enumerate([(v_hbm, v_buf), (doc_hbm, docs), (k_hbm, k_buf), (q_hbm, q_buf)])]
    for load in loads:
        load.start()

    def value_copy(src, dst, c, target):
        return pltpu.make_async_remote_copy(
            wv.at[src, c, pl.ds(0, HEAD)], wv.at[dst, c, pl.ds(0, HEAD)], sv.at[dst, c], rv.at[dst, c],
            device_id={"ctx": target}, device_id_type=MESH)

    def key_copy(src, dst, c, target):
        return pltpu.make_async_remote_copy(
            wk.at[src, c], wk.at[dst, c], sk.at[dst, c], rk.at[dst, c],
            device_id={"ctx": target}, device_id_type=MESH)

    def doc_copy(d):
        return pltpu.make_async_remote_copy(
            docs, doc_win.at[d - 1], doc_send.at[d - 1], doc_recv.at[d - 1],
            device_id={"ctx": lax.rem(me + d, count)}, device_id_type=MESH)

    def when_sent(condition, copy):
        @pl.when(condition)
        def _():
            copy.start()

    def relay_copy(kind, c):
        buf = relay_v if kind == V else relay_k
        mine = wv.at[0, c, pl.ds(0, HEAD)] if kind == V else wk.at[0, c]
        return pltpu.make_async_remote_copy(
            mine, buf.at[c], relay_sems.at[kind, 0, c], relay_sems.at[kind, 1, c],
            device_id={"ctx": relay}, device_id_type=MESH)

    def relayed_copy(kind, c):
        if kind == V:
            return pltpu.make_async_remote_copy(
                relay_v.at[c], wv.at[8, c, pl.ds(0, HEAD)], relay_sems.at[kind, 2, c], rv.at[8, c],
                device_id={"ctx": down}, device_id_type=MESH)
        return pltpu.make_async_remote_copy(
            relay_k.at[c], wk.at[8, c], relay_sems.at[kind, 2, c], rk.at[8, c],
            device_id={"ctx": down}, device_id_type=MESH)

    def relay_own(kind, c):
        if kind in RELAYED:
            when_sent(me + 8 < count, relay_copy(kind, c))

    def relay_keys(stage):
        if K in RELAYED and stage == RELAY_KEYS_AT:
            for c in range(KV_HEADS):
                relay_own(K, c)

    def relay_event(stage, late, c):
        for kind in RELAYED:
            if RELAYED[kind] == (stage, late):
                @pl.when(down >= 8)
                def _():
                    relay_copy(kind, c).wait_recv()
                    relayed_copy(kind, c).start()

    def drain_relays(c):
        for kind in RELAYED:
            @pl.when(me + 8 < count)
            def _():
                relay_copy(kind, c).wait_send()

            @pl.when(down >= 8)
            def _():
                relayed_copy(kind, c).wait_send()

    def copy_of(kind):
        return value_copy if kind == V else key_copy

    def ways(d, kind):
        link = ROUTE[d, kind]
        if link == RELAY:
            return []
        plain, edge = SOURCES[link, d]
        if link == UP:
            return [(0, plain, up, me + 4 < count)]
        special = x == 3 if link == RIGHT else x == 0
        target = right if link == RIGHT else left
        return [(0, plain, target, jnp.logical_not(special)), (1, edge, target, special)]

    def send(way, d, kind, c):
        _, src, target, there = way
        when_sent(there & (src <= me), copy_of(kind)(src, d, c, target))

    def send_own(kind, c):
        for d in (4, 1, 3):
            for way in ways(d, kind):
                if way[1] == 0:
                    send(way, d, kind, c)

    def stage_event(stage, c):
        first, after = [], {}
        for (d, kind) in ROUTE:
            for way in ways(d, kind):
                if way[1] != 0 and LEAVE[d, kind, way[0]] == stage:
                    if ARRIVE[way[1], kind][0] < stage:
                        first.append((way, d, kind))
                    else:
                        after.setdefault((way[1], kind), []).append((way, d, kind))
        for entry in first:
            send(*entry, c)
        relay_event(stage, 0, c)
        for d, kind in sorted((e for e in ARRIVE if ARRIVE[e][0] == stage), key=lambda e: ARRIVE[e][1]):
            @pl.when(d <= me)
            def _():
                copy_of(kind)(d, d, c, up).wait_recv()
            for entry in after.get((d, kind), []):
                send(*entry, c)
        relay_event(stage, 1, c)

    wv[:, :, HEAD:, :] = jnp.ones((ITEMS, KV_HEADS, VALUE_ROWS - HEAD, ROWS), jnp.bfloat16)
    loads[0].wait()
    for c in range(KV_HEADS):
        wv[0, c, 0:HEAD] = v_buf[:, c * HEAD:(c + 1) * HEAD].T
    loads[1].wait()
    pl.semaphore_wait(barrier, 2 + jnp.minimum(8, count - 1 - me) + jnp.where(me + 8 < count, 1, 0)
                      + jnp.where(down >= 8, 1, 0))
    for d in range(1, 9):
        when_sent(me + d < count, doc_copy(d))
    for c in range(KV_HEADS):
        send_own(V, c)
        relay_own(V, c)
    loads[3].wait()

    def turn(n, _):
        for u in range(4):
            at = pl.multiple_of((4 * n + u) * HEAD, HEAD)
            q_t[4 * n + u] = q_buf[:, pl.ds(at, HEAD)].T
        return 0

    lax.fori_loop(0, HEADS // 4, turn, 0)
    for d in range(1, 9):
        @pl.when(d > me)
        def _():
            wk[d] = jnp.zeros((KV_HEADS, ROWS, HEAD), jnp.bfloat16)
            wv[d, :, 0:HEAD] = jnp.zeros((KV_HEADS, HEAD, ROWS), jnp.bfloat16)

    doc_row = docs[...].astype(jnp.float32)
    columns = jnp.transpose(jnp.broadcast_to(doc_row, (ROWS, ROWS)))
    local = jnp.sum((columns < doc_row).astype(jnp.float32), axis=0, keepdims=True)
    first = doc_row[:, 0:1]
    powers = jnp.transpose(jnp.broadcast_to(inverse[...], (HEAD, HEAD)))[0:HEAD // 2]
    powers = jnp.concatenate([powers, powers], axis=1)
    tokens = lax.broadcasted_iota(jnp.int32, (1, ROWS), 1).astype(jnp.float32)
    loads[2].wait()
    for d in range(1, 9):
        @pl.when(d <= me)
        def _():
            doc_copy(d).wait_recv()
    behind = jnp.zeros((1, ROWS), jnp.float32)
    for d in range(1, 9):
        same = (doc_win[d - 1].astype(jnp.float32) == first) & (d <= me)
        behind = behind + jnp.where(same, 1.0, 0.0)
    behind = jnp.sum(behind, axis=1, keepdims=True)
    start = jnp.where(doc_row == first, -behind, local)
    start_out[...] = jnp.broadcast_to(start, (8, ROWS))
    angles = powers * (tokens - start)
    cosine[...] = jnp.cos(angles)
    sine[...] = jnp.sin(angles)

    def rotated(matrix):
        wide = matrix.astype(jnp.float32)
        a, b = wide[0:HEAD // 2], wide[HEAD // 2:]
        co, si = cosine[...], sine[...]
        return jnp.concatenate([a * co - b * si, b * co + a * si], axis=0)

    for c in range(KV_HEADS):
        wk[0, c] = rotated(k_buf[:, c * HEAD:(c + 1) * HEAD].T).T.astype(jnp.bfloat16)
    query = lax.broadcasted_iota(jnp.int32, (ROWS, ROWS), 1).astype(jnp.float32)
    key = lax.broadcasted_iota(jnp.int32, (ROWS, ROWS), 0).astype(jnp.float32)
    bias[0] = jnp.where((key >= start) & (key <= query), 0.0, MASKED)
    for c in range(KV_HEADS):
        send_own(K, c)
    for d in range(1, ITEMS):
        at = key - float(ROWS * d)
        bias[d] = jnp.where((at >= start) & (at <= query), 0.0, MASKED)

    def step_one(c, _):
        stage_event(0, c)

        def turned(n, _):
            for u in range(4):
                h = c * GROUP + 4 * n + u
                q_t[h] = rotated(q_t[h]).astype(jnp.bfloat16)
            return 0

        lax.fori_loop(0, GROUP // 4, turned, 0)
        return 0

    relay_keys(0)
    lax.fori_loop(0, KV_HEADS, step_one, 0)
    qt_copy = pltpu.make_async_copy(q_t, qt_hbm, qt_sem)
    qt_copy.start()
    bad_out[...] = jnp.zeros((8, ROWS), jnp.float32)

    def weigh(items, at, size):
        for u in range(size):
            h = at + u
            for n, d in enumerate(items):
                scores = lax.dot_general(wk[d, h // GROUP], q_t[h], (((1,), (0,)), ((), ())),
                                         preferred_element_type=jnp.float32)
                probs[u * len(items) + n] = jnp.exp2(scores * SCALE + bias[d]).astype(jnp.bfloat16)

    def gather(items, at, size, begin, end):
        for u in range(size):
            h = at + u
            total = None
            for n, d in enumerate(items):
                part = lax.dot_general(wv[d, h // GROUP], probs[u * len(items) + n], (((1,), (0,)), ((), ())),
                                       preferred_element_type=jnp.float32)
                total = part if total is None else total + part
            if not begin:
                total = acc[h] + total
            if end:
                bottom = total[HEAD:HEAD + 1]
                lane = h * HEAD if isinstance(h, int) else pl.multiple_of(h * HEAD, HEAD)
                q_buf[:, pl.ds(lane, HEAD)] = (total[0:HEAD] * (1.0 / bottom)).astype(jnp.bfloat16).T
                fine = (bottom >= LOW) & (bottom <= HIGH)
                bad_out[0:1] = jnp.maximum(bad_out[0:1], jnp.where(fine, 0.0, 1.0))
            else:
                acc[h] = total

    def out_copy(i):
        wide = AT_ONCE * HEAD
        lanes = pl.ds(i * wide if isinstance(i, int) else pl.multiple_of(i * wide, wide), wide)
        return pltpu.make_async_copy(q_buf.at[:, lanes], out_hbm.at[:, lanes], out_sem.at[i])

    def group(items, size, stage, before):
        begin, end = before is None, stage == len(GROUPS)
        per = GROUP // size
        stage_event(stage, 0)
        if before is not None:
            gather(before[0], HEADS - before[1], before[1], before[2], False)
        weigh(items, 0, size)

        def inner(i):
            if end:
                @pl.when(i >= 2)
                def _():
                    out_copy(i - 2).start()
            gather(items, size * (i - 1), size, begin, end)
            weigh(items, size * i, size)

        for j in range(1, per):
            inner(j)

        def outer(c, _):
            stage_event(stage, c)
            lax.fori_loop(0, per, lambda j, _: (inner(per * c + j), 0)[1], 0)
            return 0

        lax.fori_loop(1, KV_HEADS, outer, 0)
        return items, size, begin

    def kept(refs, out, sems, d):
        return pltpu.make_async_copy(refs.at[d], out.at[d], sems.at[d])

    def keep(*items):
        for d in items:
            kept(wk, wk_hbm, wk_sem, d).start()
            kept(wv, wv_hbm, wv_sem, d).start()

    before = None
    for n, items in enumerate(GROUPS):
        relay_keys(n + 1)
        before = group(items, SIZES[n], n + 1, before)
        keep(*items)
    out_copy(6).start()
    gather(GROUPS[-1], HEADS - AT_ONCE, AT_ONCE, False, True)
    out_copy(7).start()

    for d in range(1, 9):
        @pl.when(me + d < count)
        def _():
            doc_copy(d).wait_send()

    def drain(c, _):
        for (d, kind) in ROUTE:
            for way in ways(d, kind):
                @pl.when(way[3] & (way[1] <= me))
                def _():
                    copy_of(kind)(d, d, c, up).wait_send()
        drain_relays(c)
        return 0

    lax.fori_loop(0, KV_HEADS, drain, 0)
    for d in range(ITEMS):
        kept(wk, wk_hbm, wk_sem, d).wait()
        kept(wv, wv_hbm, wv_sem, d).wait()
    qt_copy.wait()
    for i in range(HEADS // AT_ONCE):
        out_copy(i).wait()


def finish(found, start, bad, qt_hbm, wk_hbm, wv_hbm, out, o_buf, q_buf, k_buf, v_buf, sems, in_sems, out_sems):
    pieces = 8
    tall = ROWS // pieces

    def taken(i):
        return pltpu.make_async_copy(found.at[pl.ds(i * tall, tall)], o_buf.at[pl.ds(i * tall, tall)], in_sems.at[i])

    def given(i):
        return pltpu.make_async_copy(o_buf.at[pl.ds(i * tall, tall)], out.at[pl.ds(i * tall, tall)], out_sems.at[i])

    for i in range(pieces):
        taken(i).start()
    fine = jnp.max(bad[...]) < 0.5

    @pl.when(fine)
    def _():
        for i in range(pieces):
            taken(i).wait()
            given(i).start()

    @pl.when(jnp.logical_not(fine))
    def _():
        for i in range(pieces):
            taken(i).wait()
        query = lax.broadcasted_iota(jnp.int32, (ROWS, ROWS), 1).astype(jnp.float32)
        key = lax.broadcasted_iota(jnp.int32, (ROWS, ROWS), 0).astype(jnp.float32)
        begin = start[0:1]

        def of_head(h, _):
            copies = [
                pltpu.make_async_copy(qt_hbm.at[h], q_buf, sems.at[0]),
                pltpu.make_async_copy(wk_hbm.at[:, h // GROUP], k_buf, sems.at[1]),
                pltpu.make_async_copy(wv_hbm.at[:, h // GROUP], v_buf, sems.at[2]),
            ]
            for copy in copies:
                copy.start()
            for copy in copies:
                copy.wait()

            def scores(d):
                at = key - (d * ROWS).astype(jnp.float32)
                product = lax.dot_general(k_buf[d], q_buf[...], (((1,), (0,)), ((), ())),
                                          preferred_element_type=jnp.float32)
                return jnp.where((at >= begin) & (at <= query), product * SCALE, MASKED)

            def highest(d, top):
                return jnp.maximum(top, jnp.max(scores(d), axis=0, keepdims=True))

            top = lax.fori_loop(0, ITEMS, highest, jnp.full((1, ROWS), MASKED, jnp.float32))

            def summed(d, carry):
                bottom, total = carry
                weights = jnp.exp2(scores(d) - top)
                bottom = bottom + jnp.sum(weights, axis=0, keepdims=True)
                part = lax.dot_general(v_buf[d, 0:HEAD], weights.astype(jnp.bfloat16), (((1,), (0,)), ((), ())),
                                       preferred_element_type=jnp.float32)
                return bottom, total + part

            bottom, total = lax.fori_loop(
                0, ITEMS, summed, (jnp.zeros((1, ROWS), jnp.float32), jnp.zeros((HEAD, ROWS), jnp.float32)))
            o_buf[:, pl.ds(pl.multiple_of(h * HEAD, HEAD), HEAD)] = (total / bottom).astype(jnp.bfloat16).T
            return 0

        lax.fori_loop(0, HEADS, of_head, 0)
        for i in range(pieces):
            given(i).start()

    for i in range(pieces):
        given(i).wait()


def shards(documents, queries, key_projection_rows, value_projection_rows):
    bf, f32 = jnp.bfloat16, jnp.float32
    powers = np.float32(1000000.0) ** (-2.0 * np.arange(HEAD // 2, dtype=np.float32) / HEAD)
    inverse = jnp.asarray(np.tile(powers, 2)[None, :], f32)
    vmem, whole = pl.BlockSpec(memory_space=VMEM), pl.BlockSpec(memory_space=pl.ANY)
    dma = pltpu.SemaphoreType.DMA
    flops = 4 * HEADS * ROWS * ITEMS * ROWS * HEAD
    per_item = (ITEMS, KV_HEADS)
    found, q_t, wk, wv, start, bad = pl.pallas_call(
        attend,
        out_shape=[
            jax.ShapeDtypeStruct((ROWS, HEADS * HEAD), bf),
            jax.ShapeDtypeStruct((HEADS, HEAD, ROWS), bf),
            jax.ShapeDtypeStruct((ITEMS, KV_HEADS, ROWS, HEAD), bf),
            jax.ShapeDtypeStruct((ITEMS, KV_HEADS, VALUE_ROWS, ROWS), bf),
            jax.ShapeDtypeStruct((8, ROWS), f32),
            jax.ShapeDtypeStruct((8, ROWS), f32),
        ],
        in_specs=[whole, vmem, whole, whole, whole],
        out_specs=[whole] * 4 + [vmem] * 2,
        scratch_shapes=[
            VMEM((1, ROWS), jnp.int32),
            VMEM((ROWS, KV_HEADS * HEAD), bf),
            VMEM((ROWS, KV_HEADS * HEAD), bf),
            VMEM((ROWS, HEADS * HEAD), bf),
            VMEM((HEADS, HEAD, ROWS), bf),
            VMEM((ITEMS, KV_HEADS, ROWS, HEAD), bf),
            VMEM((ITEMS, KV_HEADS, VALUE_ROWS, ROWS), bf),
            VMEM((ITEMS, ROWS, ROWS), f32),
            VMEM((HEADS, VALUE_ROWS, ROWS), f32),
            VMEM((AT_ONCE * MOST_AT_ONCE, ROWS, ROWS), bf),
            VMEM((8, 1, ROWS), jnp.int32),
            VMEM((HEAD // 2, ROWS), f32),
            VMEM((HEAD // 2, ROWS), f32),
            dma(per_item), dma(per_item), dma(per_item), dma(per_item),
            VMEM((KV_HEADS, HEAD, ROWS), bf), VMEM((KV_HEADS, ROWS, HEAD), bf), dma((2, 3, KV_HEADS)),
            dma((8,)), dma((8,)), dma((4,)), dma((HEADS // AT_ONCE,)), dma, dma((ITEMS,)), dma((ITEMS,)),
        ],
        compiler_params=pltpu.CompilerParams(collective_id=0, has_side_effects=True, vmem_limit_bytes=67043328),
        cost_estimate=pl.CostEstimate(flops=flops, bytes_accessed=12 * 2**20, transcendentals=HEADS * ROWS * ITEMS * ROWS),
        name="attend",
    )(documents.reshape(1, ROWS), inverse, queries, key_projection_rows, value_projection_rows)
    return pl.pallas_call(
        finish,
        out_shape=jax.ShapeDtypeStruct((ROWS, HEADS * HEAD), bf),
        in_specs=[whole, vmem, vmem, whole, whole, whole],
        out_specs=whole,
        scratch_shapes=[
            VMEM((ROWS, HEADS * HEAD), bf),
            VMEM((HEAD, ROWS), bf),
            VMEM((ITEMS, ROWS, HEAD), bf),
            VMEM((ITEMS, VALUE_ROWS, ROWS), bf),
            dma((3,)), dma((8,)), dma((8,)),
        ],
        compiler_params=pltpu.CompilerParams(vmem_limit_bytes=67043328),
        cost_estimate=pl.CostEstimate(flops=2**20, bytes_accessed=2**14, transcendentals=0),
        name="finish",
    )(found, start, bad, q_t, wk, wv)


def solution(mesh):
    in_specs = (
        P(("dp", "ctx")),
        P(("dp", "ctx"), None),
        P(("dp", "ctx"), None),
        P(("dp", "ctx"), None),
    )
    out_specs = P(("dp", "ctx"), None)
    return jax.shard_map(shards, mesh=mesh, in_specs=in_specs, out_specs=out_specs, check_vma=False)
```

```python
import functools
import math
import jax
import jax.numpy as jnp
import numpy as np
from jax import lax
from jax.experimental import pallas as pl
from jax.experimental.pallas import tpu as pltpu
from jax.sharding import PartitionSpec as P

HEAD = 128
HEADS = 32
KV_HEADS = 4
GROUP = HEADS // KV_HEADS
ROWS = 256
ITEMS = 9
VALUE_ROWS = 144
AT_ONCE = 4
MOST_AT_ONCE = 3
SCALE = math.log2(math.e) / math.sqrt(HEAD)
LOW = 1e-25
HIGH = 1e37
MASKED = -1e30
MESH = pl.DeviceIdType.MESH
UP, RIGHT, LEFT, RELAY = range(4)
V, K = range(2)
SOURCES = {(UP, 4): (0, 0), (UP, 5): (1, 1), (UP, 6): (2, 2), (UP, 7): (3, 3), (UP, 8): (4, 4), (RIGHT, 1): (0, 4),
           (RIGHT, 2): (1, 5), (RIGHT, 5): (4, 8), (LEFT, 3): (4, 0), (LEFT, 6): (7, 3), (LEFT, 7): (8, 4)}
ROUTE = {(1, K, 0): RIGHT, (1, K, 1): RIGHT, (1, V, 0): RIGHT, (1, V, 1): RIGHT, (2, K, 0): RIGHT, (2, K, 1): RIGHT, (2, V, 0): RIGHT, (2, V, 1): RIGHT, (3, K, 0): LEFT, (3, K, 1): LEFT, (3, V, 0): LEFT, (3, V, 1): LEFT, (4, K, 0): UP, (4, K, 1): UP, (4, V, 0): UP, (4, V, 1): UP, (5, K, 0): UP, (5, K, 1): UP, (5, V, 0): RIGHT, (5, V, 1): UP, (6, K, 0): UP, (6, K, 1): UP, (6, V, 0): LEFT, (6, V, 1): LEFT, (7, K, 0): UP, (7, K, 1): UP, (7, V, 0): LEFT, (7, V, 1): LEFT, (8, K, 0): RELAY, (8, K, 1): RELAY, (8, V, 0): RELAY, (8, V, 1): RELAY}
ARRIVE = {(1, K): (2, 3), (1, V): (1, 0), (2, K): (4, 11), (2, V): (5, 15), (3, K): (3, 13), (3, V): (2, 4), (4, K): (1, 10), (4, V): (0, 1), (5, K): (3, 9), (5, V): (3, 2), (6, K): (5, 7), (6, V): (5, 5), (7, K): (4, 6), (7, V): (4, 8), (8, K): (4, 12), (8, V): (2, 14)}
LEAVE = {(1, K, 0, 1): 1, (1, K, 1, 1): 1, (1, V, 0, 1): 0, (1, V, 1, 1): 0, (2, K, 0, 0): 2, (2, K, 0, 1): 3, (2, K, 1, 0): 2, (2, K, 1, 1): 3, (2, V, 0, 0): 3, (2, V, 0, 1): 4, (2, V, 1, 0): 3, (2, V, 1, 1): 4, (3, K, 0, 0): 1, (3, K, 1, 0): 1, (3, V, 0, 0): 0, (3, V, 1, 0): 0, (5, K, 0, 0): 2, (5, K, 1, 0): 2, (5, V, 0, 0): 0, (5, V, 0, 1): 2, (5, V, 1, 0): 1, (6, K, 0, 0): 4, (6, K, 1, 0): 4, (6, V, 0, 0): 4, (6, V, 0, 1): 2, (6, V, 1, 0): 4, (6, V, 1, 1): 2, (7, K, 0, 0): 3, (7, K, 1, 0): 3, (7, V, 0, 0): 2, (7, V, 0, 1): 0, (7, V, 1, 0): 2, (7, V, 1, 1): 0}
RELAYED = {V: (0, 0), K: (3, 1)}
RELAY_KEYS_AT = 1
GROUPS = ((0,), (1, 4), (3, 5), (8,), (2, 6, 7))
SIZES = (8, 4, 4, 8, 4)
VMEM = pltpu.VMEM


def attend(doc_hbm, inverse, q_hbm, k_hbm, v_hbm, out_hbm, qt_hbm, wk_hbm, wv_hbm, start_out, bad_out,
           docs, k_buf, v_buf, q_buf, q_t, wk, wv, bias, acc, probs, doc_win, cosine, sine,
           rk, rv, sk, sv, relay_v, relay_k, relay_sems, doc_send, doc_recv, in_sem, out_sem, qt_sem, wk_sem, wv_sem):
    count = lax.axis_size("ctx")
    me = lax.axis_index("ctx")
    x = lax.rem(me, 4)
    row = me - x
    right = row + lax.rem(x + 1, 4)
    left = row + lax.rem(x + 3, 4)
    up = lax.rem(me + 4, count)

    plane = me - lax.rem(me, 16)
    y = lax.rem(me // 4, 4)
    down = plane + 4 * lax.rem(y + 3, 4) + x
    above = plane + 4 * lax.rem(y + 1, 4) + x
    ahead = lax.rem(me + 8, count)
    relay = ahead - lax.rem(ahead, 16) + 4 * lax.rem(lax.rem(ahead // 4, 4) + 1, 4) + x

    barrier = pltpu.get_barrier_semaphore()

    def greet(other):
        pl.semaphore_signal(barrier, inc=1, device_id={"ctx": other}, device_id_type=MESH)

    for d in range(1, 9):
        @pl.when(d <= me)
        def _():
            greet(lax.rem(me + count - d, count))
    greet(left)
    greet(right)

    @pl.when(down >= 8)
    def _():
        greet(lax.rem(down + count - 8, count))

    @pl.when(me >= 8)
    def _():
        greet(above)

    loads = [pltpu.make_async_copy(a, b, in_sem.at[n])
             for n, (a, b) in enumerate([(v_hbm, v_buf), (doc_hbm, docs), (k_hbm, k_buf), (q_hbm, q_buf)])]
    for load in loads:
        load.start()

    def value_copy(src, dst, c, target):
        return pltpu.make_async_remote_copy(
            wv.at[src, c, pl.ds(0, HEAD)], wv.at[dst, c, pl.ds(0, HEAD)], sv.at[dst, c], rv.at[dst, c],
            device_id={"ctx": target}, device_id_type=MESH)

    def key_copy(src, dst, c, target):
        return pltpu.make_async_remote_copy(
            wk.at[src, c], wk.at[dst, c], sk.at[dst, c], rk.at[dst, c],
            device_id={"ctx": target}, device_id_type=MESH)

    def doc_copy(d):
        return pltpu.make_async_remote_copy(
            docs, doc_win.at[d - 1], doc_send.at[d - 1], doc_recv.at[d - 1],
            device_id={"ctx": lax.rem(me + d, count)}, device_id_type=MESH)

    def when_sent(condition, copy):
        @pl.when(condition)
        def _():
            copy.start()

    def relay_copy(kind, c):
        buf = relay_v if kind == V else relay_k
        mine = wv.at[0, c, pl.ds(0, HEAD)] if kind == V else wk.at[0, c]
        return pltpu.make_async_remote_copy(
            mine, buf.at[c], relay_sems.at[kind, 0, c], relay_sems.at[kind, 1, c],
            device_id={"ctx": relay}, device_id_type=MESH)

    def relayed_copy(kind, c):
        if kind == V:
            return pltpu.make_async_remote_copy(
                relay_v.at[c], wv.at[8, c, pl.ds(0, HEAD)], relay_sems.at[kind, 2, c], rv.at[8, c],
                device_id={"ctx": down}, device_id_type=MESH)
        return pltpu.make_async_remote_copy(
            relay_k.at[c], wk.at[8, c], relay_sems.at[kind, 2, c], rk.at[8, c],
            device_id={"ctx": down}, device_id_type=MESH)

    def relay_own(kind, c):
        if kind in RELAYED:
            when_sent(me + 8 < count, relay_copy(kind, c))

    def relay_keys(stage):
        if K in RELAYED and stage == RELAY_KEYS_AT:
            for c in range(KV_HEADS):
                relay_own(K, c)

    def relay_event(stage, late, c):
        for kind in RELAYED:
            if RELAYED[kind] == (stage, late):
                @pl.when(down >= 8)
                def _():
                    relay_copy(kind, c).wait_recv()
                    relayed_copy(kind, c).start()

    def drain_relays(c):
        for kind in RELAYED:
            @pl.when(me + 8 < count)
            def _():
                relay_copy(kind, c).wait_send()

            @pl.when(down >= 8)
            def _():
                relayed_copy(kind, c).wait_send()

    def copy_of(kind):
        return value_copy if kind == V else key_copy

    def ways(d, kind, half):
        link = ROUTE[d, kind, half]
        if link == RELAY:
            return []
        plain, edge = SOURCES[link, d]
        if link == UP:
            return [(0, plain, up, me + 4 < count)]
        special = x == 3 if link == RIGHT else x == 0
        target = right if link == RIGHT else left
        return [(0, plain, target, jnp.logical_not(special)), (1, edge, target, special)]

    def send(way, d, kind, half, c):
        _, src, target, there = way
        if ROUTE[d, kind, 1 - half] != ROUTE[d, kind, half]:
            if isinstance(c, int):
                if c // 2 != half:
                    return
            else:
                there = there & (c // 2 == half)
        elif half:
            return
        when_sent(there & (src <= me), copy_of(kind)(src, d, c, target))

    def send_own(kind, c):
        for d in (4, 1, 3):
            for way in ways(d, kind, 0):
                if way[1] == 0:
                    send(way, d, kind, 0, c)

    def stage_event(stage, c):
        first, after = [], {}
        for (d, kind, half) in ROUTE:
            for way in ways(d, kind, half):
                if way[1] != 0 and LEAVE[d, kind, half, way[0]] == stage:
                    if ARRIVE[way[1], kind][0] < stage:
                        first.append((way, d, kind, half))
                    else:
                        after.setdefault((way[1], kind), []).append((way, d, kind, half))
        for entry in first:
            send(*entry, c)
        relay_event(stage, 0, c)
        for d, kind in sorted((e for e in ARRIVE if ARRIVE[e][0] == stage), key=lambda e: ARRIVE[e][1]):
            @pl.when(d <= me)
            def _():
                copy_of(kind)(d, d, c, up).wait_recv()
            for entry in after.get((d, kind), []):
                send(*entry, c)
        relay_event(stage, 1, c)

    wv[:, :, HEAD:, :] = jnp.ones((ITEMS, KV_HEADS, VALUE_ROWS - HEAD, ROWS), jnp.bfloat16)
    loads[0].wait()
    for c in range(KV_HEADS):
        wv[0, c, 0:HEAD] = v_buf[:, c * HEAD:(c + 1) * HEAD].T
    loads[1].wait()
    pl.semaphore_wait(barrier, 2 + jnp.minimum(8, count - 1 - me) + jnp.where(me + 8 < count, 1, 0)
                      + jnp.where(down >= 8, 1, 0))
    for d in range(1, 9):
        when_sent(me + d < count, doc_copy(d))
    for c in range(KV_HEADS):
        send_own(V, c)
        relay_own(V, c)
    loads[3].wait()

    def turn(n, _):
        for u in range(4):
            at = pl.multiple_of((4 * n + u) * HEAD, HEAD)
            q_t[4 * n + u] = q_buf[:, pl.ds(at, HEAD)].T
        return 0

    lax.fori_loop(0, HEADS // 4, turn, 0)
    for d in range(1, 9):
        @pl.when(d > me)
        def _():
            wk[d] = jnp.zeros((KV_HEADS, ROWS, HEAD), jnp.bfloat16)
            wv[d, :, 0:HEAD] = jnp.zeros((KV_HEADS, HEAD, ROWS), jnp.bfloat16)

    doc_row = docs[...].astype(jnp.float32)
    columns = jnp.transpose(jnp.broadcast_to(doc_row, (ROWS, ROWS)))
    local = jnp.sum((columns < doc_row).astype(jnp.float32), axis=0, keepdims=True)
    first = doc_row[:, 0:1]
    powers = jnp.transpose(jnp.broadcast_to(inverse[...], (HEAD, HEAD)))[0:HEAD // 2]
    powers = jnp.concatenate([powers, powers], axis=1)
    tokens = lax.broadcasted_iota(jnp.int32, (1, ROWS), 1).astype(jnp.float32)
    loads[2].wait()
    for d in range(1, 9):
        @pl.when(d <= me)
        def _():
            doc_copy(d).wait_recv()
    behind = jnp.zeros((1, ROWS), jnp.float32)
    for d in range(1, 9):
        same = (doc_win[d - 1].astype(jnp.float32) == first) & (d <= me)
        behind = behind + jnp.where(same, 1.0, 0.0)
    behind = jnp.sum(behind, axis=1, keepdims=True)
    start = jnp.where(doc_row == first, -behind, local)
    start_out[...] = jnp.broadcast_to(start, (8, ROWS))
    angles = powers * (tokens - start)
    cosine[...] = jnp.cos(angles)
    sine[...] = jnp.sin(angles)

    def rotated(matrix):
        wide = matrix.astype(jnp.float32)
        a, b = wide[0:HEAD // 2], wide[HEAD // 2:]
        co, si = cosine[...], sine[...]
        return jnp.concatenate([a * co - b * si, b * co + a * si], axis=0)

    for c in range(KV_HEADS):
        wk[0, c] = rotated(k_buf[:, c * HEAD:(c + 1) * HEAD].T).T.astype(jnp.bfloat16)
    query = lax.broadcasted_iota(jnp.int32, (ROWS, ROWS), 1).astype(jnp.float32)
    key = lax.broadcasted_iota(jnp.int32, (ROWS, ROWS), 0).astype(jnp.float32)
    bias[0] = jnp.where((key >= start) & (key <= query), 0.0, MASKED)
    for c in range(KV_HEADS):
        send_own(K, c)
    for d in range(1, ITEMS):
        at = key - float(ROWS * d)
        bias[d] = jnp.where((at >= start) & (at <= query), 0.0, MASKED)

    def step_one(c, _):
        stage_event(0, c)

        def turned(n, _):
            for u in range(4):
                h = c * GROUP + 4 * n + u
                q_t[h] = rotated(q_t[h]).astype(jnp.bfloat16)
            return 0

        lax.fori_loop(0, GROUP // 4, turned, 0)
        return 0

    relay_keys(0)
    lax.fori_loop(0, KV_HEADS, step_one, 0)
    qt_copy = pltpu.make_async_copy(q_t, qt_hbm, qt_sem)
    qt_copy.start()
    bad_out[...] = jnp.zeros((8, ROWS), jnp.float32)

    def weigh(items, at, size):
        for u in range(size):
            h = at + u
            for n, d in enumerate(items):
                scores = lax.dot_general(wk[d, h // GROUP], q_t[h], (((1,), (0,)), ((), ())),
                                         preferred_element_type=jnp.float32)
                probs[u * len(items) + n] = jnp.exp2(scores * SCALE + bias[d]).astype(jnp.bfloat16)

    def gather(items, at, size, begin, end):
        for u in range(size):
            h = at + u
            total = None
            for n, d in enumerate(items):
                part = lax.dot_general(wv[d, h // GROUP], probs[u * len(items) + n], (((1,), (0,)), ((), ())),
                                       preferred_element_type=jnp.float32)
                total = part if total is None else total + part
            if not begin:
                total = acc[h] + total
            if end:
                bottom = total[HEAD:HEAD + 1]
                lane = h * HEAD if isinstance(h, int) else pl.multiple_of(h * HEAD, HEAD)
                q_buf[:, pl.ds(lane, HEAD)] = (total[0:HEAD] * (1.0 / bottom)).astype(jnp.bfloat16).T
                fine = (bottom >= LOW) & (bottom <= HIGH)
                bad_out[0:1] = jnp.maximum(bad_out[0:1], jnp.where(fine, 0.0, 1.0))
            else:
                acc[h] = total

    def out_copy(i):
        wide = AT_ONCE * HEAD
        lanes = pl.ds(i * wide if isinstance(i, int) else pl.multiple_of(i * wide, wide), wide)
        return pltpu.make_async_copy(q_buf.at[:, lanes], out_hbm.at[:, lanes], out_sem.at[i])

    def group(items, size, stage, before):
        begin, end = before is None, stage == len(GROUPS)
        per = GROUP // size
        stage_event(stage, 0)
        if before is not None:
            gather(before[0], HEADS - before[1], before[1], before[2], False)
        weigh(items, 0, size)

        def inner(i):
            if end:
                @pl.when(i >= 2)
                def _():
                    out_copy(i - 2).start()
            gather(items, size * (i - 1), size, begin, end)
            weigh(items, size * i, size)

        for j in range(1, per):
            inner(j)

        def outer(c, _):
            stage_event(stage, c)
            lax.fori_loop(0, per, lambda j, _: (inner(per * c + j), 0)[1], 0)
            return 0

        lax.fori_loop(1, KV_HEADS, outer, 0)
        return items, size, begin

    def kept(refs, out, sems, d):
        return pltpu.make_async_copy(refs.at[d], out.at[d], sems.at[d])

    def keep(*items):
        for d in items:
            kept(wk, wk_hbm, wk_sem, d).start()
            kept(wv, wv_hbm, wv_sem, d).start()

    before = None
    for n, items in enumerate(GROUPS):
        relay_keys(n + 1)
        before = group(items, SIZES[n], n + 1, before)
        keep(*items)
    out_copy(6).start()
    gather(GROUPS[-1], HEADS - AT_ONCE, AT_ONCE, False, True)
    out_copy(7).start()

    for d in range(1, 9):
        @pl.when(me + d < count)
        def _():
            doc_copy(d).wait_send()

    def drain(c, _):
        for (d, kind, half) in ROUTE:
            same = ROUTE[d, kind, 1 - half] == ROUTE[d, kind, half]
            for way in ways(d, kind, half) if not (same and half) else []:
                @pl.when(way[3] & (way[1] <= me) & ((c // 2 == half) | same))
                def _():
                    copy_of(kind)(d, d, c, up).wait_send()
        drain_relays(c)
        return 0

    lax.fori_loop(0, KV_HEADS, drain, 0)
    for d in range(ITEMS):
        kept(wk, wk_hbm, wk_sem, d).wait()
        kept(wv, wv_hbm, wv_sem, d).wait()
    qt_copy.wait()
    for i in range(HEADS // AT_ONCE):
        out_copy(i).wait()


def finish(found, start_hbm, bad_hbm, qt_hbm, wk_hbm, wv_hbm, out, o_buf, start, bad, q_buf, k_buf, v_buf, sems, in_sems, out_sems):
    pieces = 8
    tall = ROWS // pieces

    def taken(i):
        return pltpu.make_async_copy(found.at[pl.ds(i * tall, tall)], o_buf.at[pl.ds(i * tall, tall)], in_sems.at[i])

    def given(i):
        return pltpu.make_async_copy(o_buf.at[pl.ds(i * tall, tall)], out.at[pl.ds(i * tall, tall)], out_sems.at[i])

    small = [pltpu.make_async_copy(bad_hbm, bad, sems.at[3]), pltpu.make_async_copy(start_hbm, start, sems.at[4])]
    for copy in small:
        copy.start()
    for i in range(pieces):
        taken(i).start()
    for copy in small:
        copy.wait()
    fine = jnp.max(bad[...]) < 0.5

    @pl.when(fine)
    def _():
        for i in range(pieces):
            taken(i).wait()
            given(i).start()

    @pl.when(jnp.logical_not(fine))
    def _():
        for i in range(pieces):
            taken(i).wait()
        query = lax.broadcasted_iota(jnp.int32, (ROWS, ROWS), 1).astype(jnp.float32)
        key = lax.broadcasted_iota(jnp.int32, (ROWS, ROWS), 0).astype(jnp.float32)
        begin = start[0:1]

        def of_head(h, _):
            copies = [
                pltpu.make_async_copy(qt_hbm.at[h], q_buf, sems.at[0]),
                pltpu.make_async_copy(wk_hbm.at[:, h // GROUP], k_buf, sems.at[1]),
                pltpu.make_async_copy(wv_hbm.at[:, h // GROUP], v_buf, sems.at[2]),
            ]
            for copy in copies:
                copy.start()
            for copy in copies:
                copy.wait()

            def scores(d):
                at = key - (d * ROWS).astype(jnp.float32)
                product = lax.dot_general(k_buf[d], q_buf[...], (((1,), (0,)), ((), ())),
                                          preferred_element_type=jnp.float32)
                return jnp.where((at >= begin) & (at <= query), product * SCALE, MASKED)

            def highest(d, top):
                return jnp.maximum(top, jnp.max(scores(d), axis=0, keepdims=True))

            top = lax.fori_loop(0, ITEMS, highest, jnp.full((1, ROWS), MASKED, jnp.float32))

            def summed(d, carry):
                bottom, total = carry
                weights = jnp.exp2(scores(d) - top)
                bottom = bottom + jnp.sum(weights, axis=0, keepdims=True)
                part = lax.dot_general(v_buf[d, 0:HEAD], weights.astype(jnp.bfloat16), (((1,), (0,)), ((), ())),
                                       preferred_element_type=jnp.float32)
                return bottom, total + part

            bottom, total = lax.fori_loop(
                0, ITEMS, summed, (jnp.zeros((1, ROWS), jnp.float32), jnp.zeros((HEAD, ROWS), jnp.float32)))
            o_buf[:, pl.ds(pl.multiple_of(h * HEAD, HEAD), HEAD)] = (total / bottom).astype(jnp.bfloat16).T
            return 0

        lax.fori_loop(0, HEADS, of_head, 0)
        for i in range(pieces):
            given(i).start()

    for i in range(pieces):
        given(i).wait()


def shards(documents, queries, key_projection_rows, value_projection_rows):
    bf, f32 = jnp.bfloat16, jnp.float32
    powers = np.float32(1000000.0) ** (-2.0 * np.arange(HEAD // 2, dtype=np.float32) / HEAD)
    inverse = jnp.asarray(np.tile(powers, 2)[None, :], f32)
    vmem, whole = pl.BlockSpec(memory_space=VMEM), pl.BlockSpec(memory_space=pl.ANY)
    dma = pltpu.SemaphoreType.DMA
    flops = 4 * HEADS * ROWS * ITEMS * ROWS * HEAD
    per_item = (ITEMS, KV_HEADS)
    found, q_t, wk, wv, start, bad = pl.pallas_call(
        attend,
        out_shape=[
            jax.ShapeDtypeStruct((ROWS, HEADS * HEAD), bf),
            jax.ShapeDtypeStruct((HEADS, HEAD, ROWS), bf),
            jax.ShapeDtypeStruct((ITEMS, KV_HEADS, ROWS, HEAD), bf),
            jax.ShapeDtypeStruct((ITEMS, KV_HEADS, VALUE_ROWS, ROWS), bf),
            jax.ShapeDtypeStruct((8, ROWS), f32),
            jax.ShapeDtypeStruct((8, ROWS), f32),
        ],
        in_specs=[whole, vmem, whole, whole, whole],
        out_specs=[whole] * 4 + [vmem] * 2,
        scratch_shapes=[
            VMEM((1, ROWS), jnp.int32),
            VMEM((ROWS, KV_HEADS * HEAD), bf),
            VMEM((ROWS, KV_HEADS * HEAD), bf),
            VMEM((ROWS, HEADS * HEAD), bf),
            VMEM((HEADS, HEAD, ROWS), bf),
            VMEM((ITEMS, KV_HEADS, ROWS, HEAD), bf),
            VMEM((ITEMS, KV_HEADS, VALUE_ROWS, ROWS), bf),
            VMEM((ITEMS, ROWS, ROWS), f32),
            VMEM((HEADS, VALUE_ROWS, ROWS), f32),
            VMEM((AT_ONCE * MOST_AT_ONCE, ROWS, ROWS), bf),
            VMEM((8, 1, ROWS), jnp.int32),
            VMEM((HEAD // 2, ROWS), f32),
            VMEM((HEAD // 2, ROWS), f32),
            dma(per_item), dma(per_item), dma(per_item), dma(per_item),
            VMEM((KV_HEADS, HEAD, ROWS), bf), VMEM((KV_HEADS, ROWS, HEAD), bf), dma((2, 3, KV_HEADS)),
            dma((8,)), dma((8,)), dma((4,)), dma((HEADS // AT_ONCE,)), dma, dma((ITEMS,)), dma((ITEMS,)),
        ],
        compiler_params=pltpu.CompilerParams(collective_id=0, has_side_effects=True, vmem_limit_bytes=67043328),
        cost_estimate=pl.CostEstimate(flops=flops, bytes_accessed=12 * 2**20, transcendentals=HEADS * ROWS * ITEMS * ROWS),
        name="attend",
    )(documents.reshape(1, ROWS), inverse, queries, key_projection_rows, value_projection_rows)
    return pl.pallas_call(
        finish,
        out_shape=jax.ShapeDtypeStruct((ROWS, HEADS * HEAD), bf),
        in_specs=[whole] * 6,
        out_specs=whole,
        scratch_shapes=[
            VMEM((ROWS, HEADS * HEAD), bf),
            VMEM((8, ROWS), f32),
            VMEM((8, ROWS), f32),
            VMEM((HEAD, ROWS), bf),
            VMEM((ITEMS, ROWS, HEAD), bf),
            VMEM((ITEMS, VALUE_ROWS, ROWS), bf),
            dma((5,)), dma((8,)), dma((8,)),
        ],
        compiler_params=pltpu.CompilerParams(vmem_limit_bytes=67043328),
        cost_estimate=pl.CostEstimate(flops=2**20, bytes_accessed=2**14, transcendentals=0),
        name="finish",
    )(found, start, bad, q_t, wk, wv)


def solution(mesh):
    in_specs = (
        P(("dp", "ctx")),
        P(("dp", "ctx"), None),
        P(("dp", "ctx"), None),
        P(("dp", "ctx"), None),
    )
    out_specs = P(("dp", "ctx"), None)
    return jax.shard_map(shards, mesh=mesh, in_specs=in_specs, out_specs=out_specs, check_vma=False)
```

```python
import functools
import math
import jax
import jax.numpy as jnp
import numpy as np
from jax import lax
from jax.experimental import pallas as pl
from jax.experimental.pallas import tpu as pltpu
from jax.sharding import PartitionSpec as P

HEAD = 128
HEADS = 32
KV_HEADS = 4
GROUP = HEADS // KV_HEADS
ROWS = 256
ITEMS = 9
VALUE_ROWS = 144
AT_ONCE = 4
MOST_AT_ONCE = 3
SCALE = math.log2(math.e) / math.sqrt(HEAD)
LOW = 1e-25
HIGH = 1e37
MASKED = -1e30
MESH = pl.DeviceIdType.MESH
UP, RIGHT, LEFT, RELAY = range(4)
V, K = range(2)
SOURCES = {(UP, 4): (0, 0), (UP, 5): (1, 1), (UP, 6): (2, 2), (UP, 7): (3, 3), (UP, 8): (4, 4), (RIGHT, 1): (0, 4),
           (RIGHT, 2): (1, 5), (RIGHT, 5): (4, 8), (LEFT, 3): (4, 0), (LEFT, 6): (7, 3), (LEFT, 7): (8, 4)}
ROUTE = {(1, K, 0): RIGHT, (1, K, 1): RIGHT, (1, V, 0): RIGHT, (1, V, 1): RIGHT, (2, K, 0): RIGHT, (2, K, 1): RIGHT, (2, V, 0): RIGHT, (2, V, 1): RIGHT, (3, K, 0): LEFT, (3, K, 1): LEFT, (3, V, 0): LEFT, (3, V, 1): LEFT, (4, K, 0): UP, (4, K, 1): UP, (4, V, 0): UP, (4, V, 1): UP, (5, K, 0): UP, (5, K, 1): UP, (5, V, 0): RIGHT, (5, V, 1): UP, (6, K, 0): UP, (6, K, 1): UP, (6, V, 0): LEFT, (6, V, 1): LEFT, (7, K, 0): UP, (7, K, 1): UP, (7, V, 0): LEFT, (7, V, 1): LEFT, (8, K, 0): RELAY, (8, K, 1): RELAY, (8, V, 0): RELAY, (8, V, 1): RELAY}
ARRIVE = {(1, K): (2, 11), (1, V): (1, 6), (2, K): (4, 12), (2, V): (5, 4), (3, K): (3, 8), (3, V): (2, 9), (4, K): (1, 14), (4, V): (0, 3), (5, K): (3, 7), (5, V): (4, 13), (6, K): (6, 1), (6, V): (6, 2), (7, K): (4, 15), (7, V): (4, 10), (8, K): (4, 0), (8, V): (2, 5)}
LEAVE = {(1, K, 0, 1): 1, (1, K, 1, 1): 1, (1, V, 0, 1): 0, (1, V, 1, 1): 0, (2, K, 0, 0): 2, (2, K, 0, 1): 3, (2, K, 1, 0): 2, (2, K, 1, 1): 3, (2, V, 0, 0): 1, (2, V, 0, 1): 4, (2, V, 1, 0): 1, (2, V, 1, 1): 4, (3, K, 0, 0): 1, (3, K, 1, 0): 1, (3, V, 0, 0): 0, (3, V, 1, 0): 0, (5, K, 0, 0): 2, (5, K, 1, 0): 2, (5, V, 0, 0): 1, (5, V, 0, 1): 2, (5, V, 1, 0): 1, (6, K, 0, 0): 4, (6, K, 1, 0): 4, (6, V, 0, 0): 4, (6, V, 0, 1): 2, (6, V, 1, 0): 4, (6, V, 1, 1): 2, (7, K, 0, 0): 3, (7, K, 1, 0): 3, (7, V, 0, 0): 2, (7, V, 0, 1): 0, (7, V, 1, 0): 2, (7, V, 1, 1): 0}
RELAYED = {V: (0, 1), K: (3, 1)}
RELAY_KEYS_AT = 1
GROUPS = ((0,), (4,), (3, 1), (5, 8, 7), (2,), (6,))
SIZES = (8, 8, 4, 4, 8, 8)
VMEM = pltpu.VMEM


def attend(doc_hbm, inverse_hbm, q_hbm, k_hbm, v_hbm, out_hbm, qt_hbm, wk_hbm, wv_hbm, start_hbm, bad_hbm,
           inverse, start_out, bad_out, docs, k_buf, v_buf, q_buf, q_t, wk, wv, bias, acc, probs, doc_win, cosine, sine,
           rk, rv, sk, sv, relay_v, relay_k, relay_sems, doc_send, doc_recv, in_sem, out_sem, qt_sem, wk_sem, wv_sem, small_sem):
    count = lax.axis_size("ctx")
    me = lax.axis_index("ctx")
    x = lax.rem(me, 4)
    row = me - x
    right = row + lax.rem(x + 1, 4)
    left = row + lax.rem(x + 3, 4)
    up = lax.rem(me + 4, count)

    plane = me - lax.rem(me, 16)
    y = lax.rem(me // 4, 4)
    down = plane + 4 * lax.rem(y + 3, 4) + x
    above = plane + 4 * lax.rem(y + 1, 4) + x
    ahead = lax.rem(me + 8, count)
    relay = ahead - lax.rem(ahead, 16) + 4 * lax.rem(lax.rem(ahead // 4, 4) + 1, 4) + x

    barrier = pltpu.get_barrier_semaphore()

    def greet(other):
        pl.semaphore_signal(barrier, inc=1, device_id={"ctx": other}, device_id_type=MESH)

    for d in range(1, 9):
        @pl.when(d <= me)
        def _():
            greet(lax.rem(me + count - d, count))
    greet(left)
    greet(right)

    @pl.when(down >= 8)
    def _():
        greet(lax.rem(down + count - 8, count))

    @pl.when(me >= 8)
    def _():
        greet(above)

    loads = [pltpu.make_async_copy(a, b, in_sem.at[n])
             for n, (a, b) in enumerate([(v_hbm, v_buf), (doc_hbm, docs), (k_hbm, k_buf), (q_hbm, q_buf),
                                    (inverse_hbm, inverse)])]
    for load in loads:
        load.start()

    def value_copy(src, dst, c, target):
        return pltpu.make_async_remote_copy(
            wv.at[src, c, pl.ds(0, HEAD)], wv.at[dst, c, pl.ds(0, HEAD)], sv.at[dst, c], rv.at[dst, c],
            device_id={"ctx": target}, device_id_type=MESH)

    def key_copy(src, dst, c, target):
        return pltpu.make_async_remote_copy(
            wk.at[src, c], wk.at[dst, c], sk.at[dst, c], rk.at[dst, c],
            device_id={"ctx": target}, device_id_type=MESH)

    def doc_copy(d):
        return pltpu.make_async_remote_copy(
            docs, doc_win.at[d - 1], doc_send.at[d - 1], doc_recv.at[d - 1],
            device_id={"ctx": lax.rem(me + d, count)}, device_id_type=MESH)

    def when_sent(condition, copy):
        @pl.when(condition)
        def _():
            copy.start()

    def relay_copy(kind, c):
        buf = relay_v if kind == V else relay_k
        mine = wv.at[0, c, pl.ds(0, HEAD)] if kind == V else wk.at[0, c]
        return pltpu.make_async_remote_copy(
            mine, buf.at[c], relay_sems.at[kind, 0, c], relay_sems.at[kind, 1, c],
            device_id={"ctx": relay}, device_id_type=MESH)

    def relayed_copy(kind, c):
        if kind == V:
            return pltpu.make_async_remote_copy(
                relay_v.at[c], wv.at[8, c, pl.ds(0, HEAD)], relay_sems.at[kind, 2, c], rv.at[8, c],
                device_id={"ctx": down}, device_id_type=MESH)
        return pltpu.make_async_remote_copy(
            relay_k.at[c], wk.at[8, c], relay_sems.at[kind, 2, c], rk.at[8, c],
            device_id={"ctx": down}, device_id_type=MESH)

    def relay_own(kind, c):
        if kind in RELAYED:
            when_sent(me + 8 < count, relay_copy(kind, c))

    def relay_keys(stage):
        if K in RELAYED and stage == RELAY_KEYS_AT:
            for c in range(KV_HEADS):
                relay_own(K, c)

    def relay_event(stage, late, c):
        for kind in RELAYED:
            if RELAYED[kind] == (stage, late):
                @pl.when(down >= 8)
                def _():
                    relay_copy(kind, c).wait_recv()
                    relayed_copy(kind, c).start()

    def drain_relays(c):
        for kind in RELAYED:
            @pl.when(me + 8 < count)
            def _():
                relay_copy(kind, c).wait_send()

            @pl.when(down >= 8)
            def _():
                relayed_copy(kind, c).wait_send()

    def copy_of(kind):
        return value_copy if kind == V else key_copy

    def ways(d, kind, half):
        link = ROUTE[d, kind, half]
        if link == RELAY:
            return []
        plain, edge = SOURCES[link, d]
        if link == UP:
            return [(0, plain, up, me + 4 < count)]
        special = x == 3 if link == RIGHT else x == 0
        target = right if link == RIGHT else left
        return [(0, plain, target, jnp.logical_not(special)), (1, edge, target, special)]

    def send(way, d, kind, half, c):
        _, src, target, there = way
        if ROUTE[d, kind, 1 - half] != ROUTE[d, kind, half]:
            if isinstance(c, int):
                if c // 2 != half:
                    return
            else:
                there = there & (c // 2 == half)
        elif half:
            return
        when_sent(there & (src <= me), copy_of(kind)(src, d, c, target))

    def send_own(kind, c):
        for d in (4, 1, 3):
            for way in ways(d, kind, 0):
                if way[1] == 0:
                    send(way, d, kind, 0, c)

    def stage_event(stage, c):
        first, after = [], {}
        for (d, kind, half) in ROUTE:
            for way in ways(d, kind, half):
                if way[1] != 0 and LEAVE[d, kind, half, way[0]] == stage:
                    if ARRIVE[way[1], kind][0] < stage:
                        first.append((way, d, kind, half))
                    else:
                        after.setdefault((way[1], kind), []).append((way, d, kind, half))
        for entry in first:
            send(*entry, c)
        relay_event(stage, 0, c)
        for d, kind in sorted((e for e in ARRIVE if ARRIVE[e][0] == stage), key=lambda e: ARRIVE[e][1]):
            @pl.when(d <= me)
            def _():
                copy_of(kind)(d, d, c, up).wait_recv()
            for entry in after.get((d, kind), []):
                send(*entry, c)
        relay_event(stage, 1, c)

    wv[:, :, HEAD:, :] = jnp.ones((ITEMS, KV_HEADS, VALUE_ROWS - HEAD, ROWS), jnp.bfloat16)
    loads[0].wait()
    for c in range(KV_HEADS):
        wv[0, c, 0:HEAD] = v_buf[:, c * HEAD:(c + 1) * HEAD].T
    loads[1].wait()
    pl.semaphore_wait(barrier, 2 + jnp.minimum(8, count - 1 - me) + jnp.where(me + 8 < count, 1, 0)
                      + jnp.where(down >= 8, 1, 0))
    for d in range(1, 9):
        when_sent(me + d < count, doc_copy(d))
    for c in range(KV_HEADS):
        send_own(V, c)
        relay_own(V, c)
    loads[3].wait()

    def turn(n, _):
        for u in range(4):
            at = pl.multiple_of((4 * n + u) * HEAD, HEAD)
            q_t[4 * n + u] = q_buf[:, pl.ds(at, HEAD)].T
        return 0

    lax.fori_loop(0, HEADS // 4, turn, 0)
    for d in range(1, 9):
        @pl.when(d > me)
        def _():
            wk[d] = jnp.zeros((KV_HEADS, ROWS, HEAD), jnp.bfloat16)
            wv[d, :, 0:HEAD] = jnp.zeros((KV_HEADS, HEAD, ROWS), jnp.bfloat16)

    doc_row = docs[...].astype(jnp.float32)
    columns = jnp.transpose(jnp.broadcast_to(doc_row, (ROWS, ROWS)))
    local = jnp.sum((columns < doc_row).astype(jnp.float32), axis=0, keepdims=True)
    first = doc_row[:, 0:1]
    loads[4].wait()
    powers = jnp.transpose(jnp.broadcast_to(inverse[...], (HEAD, HEAD)))[0:HEAD // 2]
    powers = jnp.concatenate([powers, powers], axis=1)
    tokens = lax.broadcasted_iota(jnp.int32, (1, ROWS), 1).astype(jnp.float32)
    loads[2].wait()
    for d in range(1, 9):
        @pl.when(d <= me)
        def _():
            doc_copy(d).wait_recv()
    behind = jnp.zeros((1, ROWS), jnp.float32)
    for d in range(1, 9):
        same = (doc_win[d - 1].astype(jnp.float32) == first) & (d <= me)
        behind = behind + jnp.where(same, 1.0, 0.0)
    behind = jnp.sum(behind, axis=1, keepdims=True)
    start = jnp.where(doc_row == first, -behind, local)
    start_out[...] = jnp.broadcast_to(start, (8, ROWS))
    angles = powers * (tokens - start)
    cosine[...] = jnp.cos(angles)
    sine[...] = jnp.sin(angles)

    def rotated(matrix):
        wide = matrix.astype(jnp.float32)
        a, b = wide[0:HEAD // 2], wide[HEAD // 2:]
        co, si = cosine[...], sine[...]
        return jnp.concatenate([a * co - b * si, b * co + a * si], axis=0)

    for c in range(KV_HEADS):
        wk[0, c] = rotated(k_buf[:, c * HEAD:(c + 1) * HEAD].T).T.astype(jnp.bfloat16)
    query = lax.broadcasted_iota(jnp.int32, (ROWS, ROWS), 1).astype(jnp.float32)
    key = lax.broadcasted_iota(jnp.int32, (ROWS, ROWS), 0).astype(jnp.float32)
    bias[0] = jnp.where((key >= start) & (key <= query), 0.0, MASKED)
    for c in range(KV_HEADS):
        send_own(K, c)
    for d in range(1, ITEMS):
        at = key - float(ROWS * d)
        bias[d] = jnp.where((at >= start) & (at <= query), 0.0, MASKED)

    def step_one(c, _):
        stage_event(0, c)

        def turned(n, _):
            for u in range(4):
                h = c * GROUP + 4 * n + u
                q_t[h] = rotated(q_t[h]).astype(jnp.bfloat16)
            return 0

        lax.fori_loop(0, GROUP // 4, turned, 0)
        return 0

    relay_keys(0)
    lax.fori_loop(0, KV_HEADS, step_one, 0)
    qt_copy = pltpu.make_async_copy(q_t, qt_hbm, qt_sem)
    qt_copy.start()
    start_copy = pltpu.make_async_copy(start_out, start_hbm, small_sem.at[0])
    start_copy.start()
    bad_out[...] = jnp.zeros((8, ROWS), jnp.float32)

    def weigh(items, at, size):
        for u in range(size):
            h = at + u
            for n, d in enumerate(items):
                scores = lax.dot_general(wk[d, h // GROUP], q_t[h], (((1,), (0,)), ((), ())),
                                         preferred_element_type=jnp.float32)
                probs[u * len(items) + n] = jnp.exp2(scores * SCALE + bias[d]).astype(jnp.bfloat16)

    def gather(items, at, size, begin, end):
        for u in range(size):
            h = at + u
            total = None
            for n, d in enumerate(items):
                part = lax.dot_general(wv[d, h // GROUP], probs[u * len(items) + n], (((1,), (0,)), ((), ())),
                                       preferred_element_type=jnp.float32)
                total = part if total is None else total + part
            if not begin:
                total = acc[h] + total
            if end:
                bottom = total[HEAD:HEAD + 1]
                lane = h * HEAD if isinstance(h, int) else pl.multiple_of(h * HEAD, HEAD)
                q_buf[:, pl.ds(lane, HEAD)] = (total[0:HEAD] * (1.0 / bottom)).astype(jnp.bfloat16).T
                fine = (bottom >= LOW) & (bottom <= HIGH)
                bad_out[0:1] = jnp.maximum(bad_out[0:1], jnp.where(fine, 0.0, 1.0))
            else:
                acc[h] = total

    def out_copy(i):
        wide = SIZES[-1] * HEAD
        lanes = pl.ds(i * wide if isinstance(i, int) else pl.multiple_of(i * wide, wide), wide)
        return pltpu.make_async_copy(q_buf.at[:, lanes], out_hbm.at[:, lanes], out_sem.at[i])

    def group(items, size, stage, before):
        begin, end = before is None, stage == len(GROUPS)
        per = GROUP // size
        stage_event(stage, 0)
        if before is not None:
            gather(before[0], HEADS - before[1], before[1], before[2], False)
        weigh(items, 0, size)

        def inner(i):
            if end:
                @pl.when(i >= 2)
                def _():
                    out_copy(i - 2).start()
            gather(items, size * (i - 1), size, begin, end)
            weigh(items, size * i, size)

        for j in range(1, per):
            inner(j)

        def outer(c, _):
            stage_event(stage, c)
            lax.fori_loop(0, per, lambda j, _: (inner(per * c + j), 0)[1], 0)
            return 0

        lax.fori_loop(1, KV_HEADS, outer, 0)
        return items, size, begin

    def kept(refs, out, sems, d):
        return pltpu.make_async_copy(refs.at[d], out.at[d], sems.at[d])

    def keep(*items):
        for d in items:
            kept(wk, wk_hbm, wk_sem, d).start()
            kept(wv, wv_hbm, wv_sem, d).start()

    before = None
    for n, items in enumerate(GROUPS):
        relay_keys(n + 1)
        before = group(items, SIZES[n], n + 1, before)
        keep(*items)
    batches = HEADS // SIZES[-1]
    out_copy(batches - 2).start()
    gather(GROUPS[-1], HEADS - SIZES[-1], SIZES[-1], False, True)
    out_copy(batches - 1).start()
    bad_copy = pltpu.make_async_copy(bad_out, bad_hbm, small_sem.at[1])
    bad_copy.start()

    for d in range(1, 9):
        @pl.when(me + d < count)
        def _():
            doc_copy(d).wait_send()

    def drain(c, _):
        for (d, kind, half) in ROUTE:
            same = ROUTE[d, kind, 1 - half] == ROUTE[d, kind, half]
            for way in ways(d, kind, half) if not (same and half) else []:
                @pl.when(way[3] & (way[1] <= me) & ((c // 2 == half) | same))
                def _():
                    copy_of(kind)(d, d, c, up).wait_send()
        drain_relays(c)
        return 0

    lax.fori_loop(0, KV_HEADS, drain, 0)
    for d in range(ITEMS):
        kept(wk, wk_hbm, wk_sem, d).wait()
        kept(wv, wv_hbm, wv_sem, d).wait()
    qt_copy.wait()
    start_copy.wait()
    bad_copy.wait()
    for i in range(batches):
        out_copy(i).wait()


def finish(found, start_hbm, bad_hbm, qt_hbm, wk_hbm, wv_hbm, out, o_buf, start, bad, q_buf, k_buf, v_buf, sems, in_sems, out_sems):
    pieces = 8
    tall = ROWS // pieces

    def taken(i):
        return pltpu.make_async_copy(found.at[pl.ds(i * tall, tall)], o_buf.at[pl.ds(i * tall, tall)], in_sems.at[i])

    def given(i):
        return pltpu.make_async_copy(o_buf.at[pl.ds(i * tall, tall)], out.at[pl.ds(i * tall, tall)], out_sems.at[i])

    small = [pltpu.make_async_copy(bad_hbm, bad, sems.at[3]), pltpu.make_async_copy(start_hbm, start, sems.at[4])]
    for copy in small:
        copy.start()
    for i in range(pieces):
        taken(i).start()
    for copy in small:
        copy.wait()
    fine = jnp.max(bad[...]) < 0.5

    @pl.when(fine)
    def _():
        for i in range(pieces):
            taken(i).wait()
            given(i).start()

    @pl.when(jnp.logical_not(fine))
    def _():
        for i in range(pieces):
            taken(i).wait()
        query = lax.broadcasted_iota(jnp.int32, (ROWS, ROWS), 1).astype(jnp.float32)
        key = lax.broadcasted_iota(jnp.int32, (ROWS, ROWS), 0).astype(jnp.float32)
        begin = start[0:1]

        def of_head(h, _):
            copies = [
                pltpu.make_async_copy(qt_hbm.at[h], q_buf, sems.at[0]),
                pltpu.make_async_copy(wk_hbm.at[:, h // GROUP], k_buf, sems.at[1]),
                pltpu.make_async_copy(wv_hbm.at[:, h // GROUP], v_buf, sems.at[2]),
            ]
            for copy in copies:
                copy.start()
            for copy in copies:
                copy.wait()

            def scores(d):
                at = key - (d * ROWS).astype(jnp.float32)
                product = lax.dot_general(k_buf[d], q_buf[...], (((1,), (0,)), ((), ())),
                                          preferred_element_type=jnp.float32)
                return jnp.where((at >= begin) & (at <= query), product * SCALE, MASKED)

            def highest(d, top):
                return jnp.maximum(top, jnp.max(scores(d), axis=0, keepdims=True))

            top = lax.fori_loop(0, ITEMS, highest, jnp.full((1, ROWS), MASKED, jnp.float32))

            def summed(d, carry):
                bottom, total = carry
                weights = jnp.exp2(scores(d) - top)
                bottom = bottom + jnp.sum(weights, axis=0, keepdims=True)
                part = lax.dot_general(v_buf[d, 0:HEAD], weights.astype(jnp.bfloat16), (((1,), (0,)), ((), ())),
                                       preferred_element_type=jnp.float32)
                return bottom, total + part

            bottom, total = lax.fori_loop(
                0, ITEMS, summed, (jnp.zeros((1, ROWS), jnp.float32), jnp.zeros((HEAD, ROWS), jnp.float32)))
            o_buf[:, pl.ds(pl.multiple_of(h * HEAD, HEAD), HEAD)] = (total / bottom).astype(jnp.bfloat16).T
            return 0

        lax.fori_loop(0, HEADS, of_head, 0)
        for i in range(pieces):
            given(i).start()

    for i in range(pieces):
        given(i).wait()


def shards(documents, queries, key_projection_rows, value_projection_rows):
    bf, f32 = jnp.bfloat16, jnp.float32
    powers = np.float32(1000000.0) ** (-2.0 * np.arange(HEAD // 2, dtype=np.float32) / HEAD)
    inverse = jnp.asarray(np.tile(powers, 2)[None, :], f32)
    whole = pl.BlockSpec(memory_space=pl.ANY)
    dma = pltpu.SemaphoreType.DMA
    flops = 4 * HEADS * ROWS * ITEMS * ROWS * HEAD
    per_item = (ITEMS, KV_HEADS)
    found, q_t, wk, wv, start, bad = pl.pallas_call(
        attend,
        out_shape=[
            jax.ShapeDtypeStruct((ROWS, HEADS * HEAD), bf),
            jax.ShapeDtypeStruct((HEADS, HEAD, ROWS), bf),
            jax.ShapeDtypeStruct((ITEMS, KV_HEADS, ROWS, HEAD), bf),
            jax.ShapeDtypeStruct((ITEMS, KV_HEADS, VALUE_ROWS, ROWS), bf),
            jax.ShapeDtypeStruct((8, ROWS), f32),
            jax.ShapeDtypeStruct((8, ROWS), f32),
        ],
        in_specs=[whole] * 5,
        out_specs=[whole] * 6,
        scratch_shapes=[
            VMEM((1, HEAD), f32),
            VMEM((8, ROWS), f32),
            VMEM((8, ROWS), f32),
            VMEM((1, ROWS), jnp.int32),
            VMEM((ROWS, KV_HEADS * HEAD), bf),
            VMEM((ROWS, KV_HEADS * HEAD), bf),
            VMEM((ROWS, HEADS * HEAD), bf),
            VMEM((HEADS, HEAD, ROWS), bf),
            VMEM((ITEMS, KV_HEADS, ROWS, HEAD), bf),
            VMEM((ITEMS, KV_HEADS, VALUE_ROWS, ROWS), bf),
            VMEM((ITEMS, ROWS, ROWS), f32),
            VMEM((HEADS, VALUE_ROWS, ROWS), f32),
            VMEM((AT_ONCE * MOST_AT_ONCE, ROWS, ROWS), bf),
            VMEM((8, 1, ROWS), jnp.int32),
            VMEM((HEAD // 2, ROWS), f32),
            VMEM((HEAD // 2, ROWS), f32),
            dma(per_item), dma(per_item), dma(per_item), dma(per_item),
            VMEM((KV_HEADS, HEAD, ROWS), bf), VMEM((KV_HEADS, ROWS, HEAD), bf), dma((2, 3, KV_HEADS)),
            dma((8,)), dma((8,)), dma((5,)), dma((HEADS // AT_ONCE,)), dma, dma((ITEMS,)), dma((ITEMS,)), dma((2,)),
        ],
        compiler_params=pltpu.CompilerParams(collective_id=0, has_side_effects=True, vmem_limit_bytes=67043328),
        cost_estimate=pl.CostEstimate(flops=flops, bytes_accessed=12 * 2**20, transcendentals=HEADS * ROWS * ITEMS * ROWS),
        name="attend",
    )(documents.reshape(1, ROWS), inverse, queries, key_projection_rows, value_projection_rows)
    return pl.pallas_call(
        finish,
        out_shape=jax.ShapeDtypeStruct((ROWS, HEADS * HEAD), bf),
        in_specs=[whole] * 6,
        out_specs=whole,
        scratch_shapes=[
            VMEM((ROWS, HEADS * HEAD), bf),
            VMEM((8, ROWS), f32),
            VMEM((8, ROWS), f32),
            VMEM((HEAD, ROWS), bf),
            VMEM((ITEMS, ROWS, HEAD), bf),
            VMEM((ITEMS, VALUE_ROWS, ROWS), bf),
            dma((5,)), dma((8,)), dma((8,)),
        ],
        compiler_params=pltpu.CompilerParams(vmem_limit_bytes=67043328),
        cost_estimate=pl.CostEstimate(flops=2**20, bytes_accessed=2**14, transcendentals=0),
        name="finish",
    )(found, start, bad, q_t, wk, wv)


def solution(mesh):
    in_specs = (
        P(("dp", "ctx")),
        P(("dp", "ctx"), None),
        P(("dp", "ctx"), None),
        P(("dp", "ctx"), None),
    )
    out_specs = P(("dp", "ctx"), None)
    return jax.shard_map(shards, mesh=mesh, in_specs=in_specs, out_specs=out_specs, check_vma=False)
```

```python
import functools
import math
import jax
import jax.numpy as jnp
import numpy as np
from jax import lax
from jax.experimental import pallas as pl
from jax.experimental.pallas import tpu as pltpu
from jax.sharding import PartitionSpec as P

HEAD = 128
HEADS = 32
KV_HEADS = 4
GROUP = HEADS // KV_HEADS
ROWS = 256
ITEMS = 9
VALUE_ROWS = 144
AT_ONCE = 4
MOST_AT_ONCE = 3
SCALE = math.log2(math.e) / math.sqrt(HEAD)
LOW = 1e-25
HIGH = 1e37
MASKED = -1e30
MESH = pl.DeviceIdType.MESH
UP, RIGHT, LEFT = range(3)
V, K = range(2)
SENDS = (
    (1, 3, 0, 1, 0, 2, -1),
    (1, 4, 4, 1, 0, 2, 0),
    (1, 3, 0, 1, 1, 2, -1),
    (1, 4, 4, 1, 1, 2, 1),
    (1, 3, 1, 2, 0, 0, 1),
    (1, 3, 1, 2, 0, 1, 2),
    (1, 4, 5, 2, 0, 2, 4),
    (1, 3, 1, 2, 1, 2, 2),
    (1, 4, 5, 2, 1, 2, 3),
    (2, 1, 0, 3, 0, 2, -1),
    (2, 7, 4, 3, 0, 2, 0),
    (2, 1, 0, 3, 1, 2, -1),
    (2, 7, 4, 3, 1, 2, 1),
    (0, 0, 0, 4, 0, 2, -1),
    (0, 0, 0, 4, 1, 2, -1),
    (0, 0, 1, 5, 0, 1, 1),
    (1, 3, 4, 5, 0, 0, 1),
    (1, 4, 8, 5, 0, 0, 2),
    (0, 0, 1, 5, 1, 2, 2),
    (2, 1, 3, 6, 0, 2, 2),
    (2, 7, 7, 6, 0, 2, 4),
    (0, 0, 2, 6, 1, 2, 4),
    (2, 1, 4, 7, 0, 0, 0),
    (2, 1, 4, 7, 0, 1, 1),
    (2, 7, 8, 7, 0, 2, 2),
    (0, 0, 3, 7, 1, 2, 3),
)
ARRIVE = {(1, K): (2, 11), (1, V): (1, 6), (2, K): (4, 12), (2, V): (5, 4), (3, K): (3, 8), (3, V): (2, 9), (4, K): (1, 14), (4, V): (0, 3), (5, K): (3, 7), (5, V): (4, 13), (6, K): (6, 1), (6, V): (6, 2), (7, K): (4, 15), (7, V): (4, 10), (8, K): (4, 0), (8, V): (2, 5)}
RELAYED = {V: (0, 1), K: (3, 1)}
RELAY_KEYS_AT = 1
GROUPS = ((0,), (4,), (3, 1), (5, 8, 7), (2,), (6,))
SIZES = (8, 8, 4, 4, 8, 8)
VMEM = pltpu.VMEM


def attend(doc_hbm, inverse_hbm, q_hbm, k_hbm, v_hbm, out_hbm, qt_hbm, wk_hbm, wv_hbm, start_hbm, bad_hbm,
           inverse, start_out, bad_out, docs, k_buf, v_buf, q_buf, q_t, wk, wv, bias, acc, probs, doc_win, cosine, sine,
           rk, rv, sk, sv, relay_v, relay_k, relay_sems, doc_send, doc_recv, in_sem, out_sem, qt_sem, wk_sem, wv_sem, small_sem):
    count = lax.axis_size("ctx")
    me = lax.axis_index("ctx")
    x = lax.rem(me, 4)
    row = me - x
    right = row + lax.rem(x + 1, 4)
    left = row + lax.rem(x + 3, 4)
    up = lax.rem(me + 4, count)

    plane = me - lax.rem(me, 16)
    y = lax.rem(me // 4, 4)
    down = plane + 4 * lax.rem(y + 3, 4) + x
    above = plane + 4 * lax.rem(y + 1, 4) + x
    ahead = lax.rem(me + 8, count)
    relay = ahead - lax.rem(ahead, 16) + 4 * lax.rem(lax.rem(ahead // 4, 4) + 1, 4) + x

    barrier = pltpu.get_barrier_semaphore()

    def greet(other):
        pl.semaphore_signal(barrier, inc=1, device_id={"ctx": other}, device_id_type=MESH)

    for d in range(1, 9):
        @pl.when(d <= me)
        def _():
            greet(lax.rem(me + count - d, count))
    greet(left)
    greet(right)

    @pl.when(down >= 8)
    def _():
        greet(lax.rem(down + count - 8, count))

    @pl.when(me >= 8)
    def _():
        greet(above)

    loads = [pltpu.make_async_copy(a, b, in_sem.at[n])
             for n, (a, b) in enumerate([(v_hbm, v_buf), (doc_hbm, docs), (k_hbm, k_buf), (q_hbm, q_buf),
                                    (inverse_hbm, inverse)])]
    for load in loads:
        load.start()

    def value_copy(src, dst, c, target, link=0, half=2):
        return pltpu.make_async_remote_copy(
            wv.at[src, c, pl.ds(0, HEAD)], wv.at[dst, c, pl.ds(0, HEAD)], sv.at[link, dst, half], rv.at[dst, c],
            device_id={"ctx": target}, device_id_type=MESH)

    def key_copy(src, dst, c, target, link=0, half=2):
        return pltpu.make_async_remote_copy(
            wk.at[src, c], wk.at[dst, c], sk.at[link, dst, half], rk.at[dst, c],
            device_id={"ctx": target}, device_id_type=MESH)

    def doc_copy(d):
        return pltpu.make_async_remote_copy(
            docs, doc_win.at[d - 1], doc_send.at[d - 1], doc_recv.at[d - 1],
            device_id={"ctx": lax.rem(me + d, count)}, device_id_type=MESH)

    def when_sent(condition, copy):
        @pl.when(condition)
        def _():
            copy.start()

    def relay_copy(kind, c):
        buf = relay_v if kind == V else relay_k
        mine = wv.at[0, c, pl.ds(0, HEAD)] if kind == V else wk.at[0, c]
        return pltpu.make_async_remote_copy(
            mine, buf.at[c], relay_sems.at[kind, 0, 0], relay_sems.at[kind, 1, c],
            device_id={"ctx": relay}, device_id_type=MESH)

    def relayed_copy(kind, c):
        if kind == V:
            return pltpu.make_async_remote_copy(
                relay_v.at[c], wv.at[8, c, pl.ds(0, HEAD)], relay_sems.at[kind, 2, 0], rv.at[8, c],
                device_id={"ctx": down}, device_id_type=MESH)
        return pltpu.make_async_remote_copy(
            relay_k.at[c], wk.at[8, c], relay_sems.at[kind, 2, 0], rk.at[8, c],
            device_id={"ctx": down}, device_id_type=MESH)

    def relay_own(kind, c):
        if kind in RELAYED:
            when_sent(me + 8 < count, relay_copy(kind, c))

    def relay_keys(stage):
        if K in RELAYED and stage == RELAY_KEYS_AT:
            for c in range(KV_HEADS):
                relay_own(K, c)

    def relay_event(stage, late, c):
        for kind in RELAYED:
            if RELAYED[kind] == (stage, late):
                @pl.when(down >= 8)
                def _():
                    relay_copy(kind, c).wait_recv()
                    relayed_copy(kind, c).start()

    def drain_relays():
        for kind in RELAYED:
            @pl.when(me + 8 < count)
            def _():
                sent(kind, 8, relay_sems.at[kind, 0, 0])

            @pl.when(down >= 8)
            def _():
                sent(kind, 8, relay_sems.at[kind, 2, 0])

    def copy_of(kind):
        return value_copy if kind == V else key_copy

    targets = (up, right, left)
    classes = (me >= 0, x == 0, x != 0, x < 3, x == 3, x == 1, x >= 2, x >= 1)

    def open_to(entry):
        link, who, src = entry[:3]
        there = classes[who] & (src <= me)
        return there & (me + 4 < count) if link == UP else there

    def goes(entry, c):
        half = entry[5]
        return open_to(entry) if half == 2 else open_to(entry) & (c // 2 == half)

    def sent(kind, d, sem, heads=pl.ds(0, KV_HEADS)):
        ref = wv.at[d, heads, pl.ds(0, HEAD)] if kind == V else wk.at[d, heads]
        pltpu.make_async_remote_copy(ref, ref, sem, sem, device_id={"ctx": up}, device_id_type=MESH).wait_send()

    def send(entry, c):
        link, _, src, d, kind, half, _ = entry
        if isinstance(c, int) and half != 2 and c // 2 != half:
            return
        when_sent(goes(entry, c), copy_of(kind)(src, d, c, targets[link], link, half))

    def send_own(kind, c):
        for entry in SENDS:
            if entry[6] < 0 and entry[4] == kind:
                send(entry, c)

    def stage_event(stage, c):
        first, after = [], {}
        for entry in SENDS:
            _, _, src, _, kind, _, at = entry
            if at == stage:
                if ARRIVE[src, kind][0] < stage:
                    first.append(entry)
                else:
                    after.setdefault((src, kind), []).append(entry)
        for entry in first:
            send(entry, c)
        relay_event(stage, 0, c)
        for d, kind in sorted((e for e in ARRIVE if ARRIVE[e][0] == stage), key=lambda e: ARRIVE[e][1]):
            @pl.when(d <= me)
            def _():
                copy_of(kind)(d, d, c, up).wait_recv()
            for entry in after.get((d, kind), []):
                send(entry, c)
        relay_event(stage, 1, c)

    wv[:, :, HEAD:, :] = jnp.ones((ITEMS, KV_HEADS, VALUE_ROWS - HEAD, ROWS), jnp.bfloat16)
    loads[0].wait()
    for c in range(KV_HEADS):
        wv[0, c, 0:HEAD] = v_buf[:, c * HEAD:(c + 1) * HEAD].T
    loads[1].wait()
    pl.semaphore_wait(barrier, 2 + jnp.minimum(8, count - 1 - me) + jnp.where(me + 8 < count, 1, 0)
                      + jnp.where(down >= 8, 1, 0))
    for d in range(1, 9):
        when_sent(me + d < count, doc_copy(d))
    for c in range(KV_HEADS):
        send_own(V, c)
        relay_own(V, c)
    loads[3].wait()

    def turn(n, _):
        for u in range(4):
            at = pl.multiple_of((4 * n + u) * HEAD, HEAD)
            q_t[4 * n + u] = q_buf[:, pl.ds(at, HEAD)].T
        return 0

    lax.fori_loop(0, HEADS // 4, turn, 0)
    for d in range(1, 9):
        @pl.when(d > me)
        def _():
            wk[d] = jnp.zeros((KV_HEADS, ROWS, HEAD), jnp.bfloat16)
            wv[d, :, 0:HEAD] = jnp.zeros((KV_HEADS, HEAD, ROWS), jnp.bfloat16)

    doc_row = docs[...].astype(jnp.float32)
    columns = jnp.transpose(jnp.broadcast_to(doc_row, (ROWS, ROWS)))
    local = jnp.sum((columns < doc_row).astype(jnp.float32), axis=0, keepdims=True)
    first = doc_row[:, 0:1]
    loads[4].wait()
    powers = jnp.transpose(jnp.broadcast_to(inverse[...], (HEAD, HEAD)))[0:HEAD // 2]
    powers = jnp.concatenate([powers, powers], axis=1)
    tokens = lax.broadcasted_iota(jnp.int32, (1, ROWS), 1).astype(jnp.float32)
    loads[2].wait()
    for d in range(1, 9):
        @pl.when(d <= me)
        def _():
            doc_copy(d).wait_recv()
    behind = jnp.zeros((1, ROWS), jnp.float32)
    for d in range(1, 9):
        same = (doc_win[d - 1].astype(jnp.float32) == first) & (d <= me)
        behind = behind + jnp.where(same, 1.0, 0.0)
    behind = jnp.sum(behind, axis=1, keepdims=True)
    start = jnp.where(doc_row == first, -behind, local)
    start_out[...] = jnp.broadcast_to(start, (8, ROWS))
    angles = powers * (tokens - start)
    cosine[...] = jnp.cos(angles)
    sine[...] = jnp.sin(angles)

    def rotated(matrix):
        wide = matrix.astype(jnp.float32)
        a, b = wide[0:HEAD // 2], wide[HEAD // 2:]
        co, si = cosine[...], sine[...]
        return jnp.concatenate([a * co - b * si, b * co + a * si], axis=0)

    for c in range(KV_HEADS):
        wk[0, c] = rotated(k_buf[:, c * HEAD:(c + 1) * HEAD].T).T.astype(jnp.bfloat16)
    query = lax.broadcasted_iota(jnp.int32, (ROWS, ROWS), 1).astype(jnp.float32)
    key = lax.broadcasted_iota(jnp.int32, (ROWS, ROWS), 0).astype(jnp.float32)
    bias[0] = jnp.where((key >= start) & (key <= query), 0.0, MASKED)
    for c in range(KV_HEADS):
        send_own(K, c)
    for d in range(1, ITEMS):
        at = key - float(ROWS * d)
        bias[d] = jnp.where((at >= start) & (at <= query), 0.0, MASKED)

    def step_one(c, _):
        stage_event(0, c)

        def turned(n, _):
            for u in range(4):
                h = c * GROUP + 4 * n + u
                q_t[h] = rotated(q_t[h]).astype(jnp.bfloat16)
            return 0

        lax.fori_loop(0, GROUP // 4, turned, 0)
        return 0

    relay_keys(0)
    lax.fori_loop(0, KV_HEADS, step_one, 0)
    qt_copy = pltpu.make_async_copy(q_t, qt_hbm, qt_sem)
    qt_copy.start()
    start_copy = pltpu.make_async_copy(start_out, start_hbm, small_sem.at[0])
    start_copy.start()
    bad_out[...] = jnp.zeros((8, ROWS), jnp.float32)

    def weigh(items, at, size):
        for u in range(size):
            h = at + u
            for n, d in enumerate(items):
                scores = lax.dot_general(wk[d, h // GROUP], q_t[h], (((1,), (0,)), ((), ())),
                                         preferred_element_type=jnp.float32)
                probs[u * len(items) + n] = jnp.exp2(scores * SCALE + bias[d]).astype(jnp.bfloat16)

    def gather(items, at, size, begin, end):
        for u in range(size):
            h = at + u
            total = None
            for n, d in enumerate(items):
                part = lax.dot_general(wv[d, h // GROUP], probs[u * len(items) + n], (((1,), (0,)), ((), ())),
                                       preferred_element_type=jnp.float32)
                total = part if total is None else total + part
            if not begin:
                total = acc[h] + total
            if end:
                bottom = total[HEAD:HEAD + 1]
                lane = h * HEAD if isinstance(h, int) else pl.multiple_of(h * HEAD, HEAD)
                q_buf[:, pl.ds(lane, HEAD)] = (total[0:HEAD] * (1.0 / bottom)).astype(jnp.bfloat16).T
                fine = (bottom >= LOW) & (bottom <= HIGH)
                bad_out[0:1] = jnp.maximum(bad_out[0:1], jnp.where(fine, 0.0, 1.0))
            else:
                acc[h] = total

    def out_copy(i):
        wide = SIZES[-1] * HEAD
        lanes = pl.ds(i * wide if isinstance(i, int) else pl.multiple_of(i * wide, wide), wide)
        return pltpu.make_async_copy(q_buf.at[:, lanes], out_hbm.at[:, lanes], out_sem.at[i])

    def group(items, size, stage, before):
        begin, end = before is None, stage == len(GROUPS)
        per = GROUP // size
        stage_event(stage, 0)
        if before is not None:
            gather(before[0], HEADS - before[1], before[1], before[2], False)
        weigh(items, 0, size)

        def inner(i):
            if end:
                @pl.when(i >= 2)
                def _():
                    out_copy(i - 2).start()
            gather(items, size * (i - 1), size, begin, end)
            weigh(items, size * i, size)

        for j in range(1, per):
            inner(j)

        def outer(c, _):
            stage_event(stage, c)
            lax.fori_loop(0, per, lambda j, _: (inner(per * c + j), 0)[1], 0)
            return 0

        lax.fori_loop(1, KV_HEADS, outer, 0)
        return items, size, begin

    def kept(refs, out, sems, d):
        return pltpu.make_async_copy(refs.at[d], out.at[d], sems.at[d])

    def keep(*items):
        for d in items:
            kept(wk, wk_hbm, wk_sem, d).start()
            kept(wv, wv_hbm, wv_sem, d).start()

    before = None
    for n, items in enumerate(GROUPS):
        relay_keys(n + 1)
        before = group(items, SIZES[n], n + 1, before)
        keep(*items)
    batches = HEADS // SIZES[-1]
    out_copy(batches - 2).start()
    gather(GROUPS[-1], HEADS - SIZES[-1], SIZES[-1], False, True)
    out_copy(batches - 1).start()
    bad_copy = pltpu.make_async_copy(bad_out, bad_hbm, small_sem.at[1])
    bad_copy.start()

    for d in range(1, 9):
        @pl.when(me + d < count)
        def _():
            doc_copy(d).wait_send()

    for entry in SENDS:
        @pl.when(open_to(entry))
        def _():
            link, _, _, d, kind, half, _ = entry
            sent(kind, d, (sv if kind == V else sk).at[link, d, half],
                 pl.ds(0, KV_HEADS) if half == 2 else pl.ds(2 * half, 2))
    drain_relays()
    for d in range(ITEMS):
        kept(wk, wk_hbm, wk_sem, d).wait()
        kept(wv, wv_hbm, wv_sem, d).wait()
    qt_copy.wait()
    start_copy.wait()
    bad_copy.wait()
    for i in range(batches):
        out_copy(i).wait()


def finish(found, start_hbm, bad_hbm, qt_hbm, wk_hbm, wv_hbm, out, o_buf, start, bad, q_buf, k_buf, v_buf, sems, in_sems, out_sems):
    pieces = 8
    tall = ROWS // pieces

    def taken(i):
        return pltpu.make_async_copy(found.at[pl.ds(i * tall, tall)], o_buf.at[pl.ds(i * tall, tall)], in_sems.at[i])

    def given(i):
        return pltpu.make_async_copy(o_buf.at[pl.ds(i * tall, tall)], out.at[pl.ds(i * tall, tall)], out_sems.at[i])

    small = [pltpu.make_async_copy(bad_hbm, bad, sems.at[3]), pltpu.make_async_copy(start_hbm, start, sems.at[4])]
    for copy in small:
        copy.start()
    for i in range(pieces):
        taken(i).start()
    for copy in small:
        copy.wait()
    fine = jnp.max(bad[...]) < 0.5

    @pl.when(fine)
    def _():
        for i in range(pieces):
            taken(i).wait()
            given(i).start()

    @pl.when(jnp.logical_not(fine))
    def _():
        for i in range(pieces):
            taken(i).wait()
        query = lax.broadcasted_iota(jnp.int32, (ROWS, ROWS), 1).astype(jnp.float32)
        key = lax.broadcasted_iota(jnp.int32, (ROWS, ROWS), 0).astype(jnp.float32)
        begin = start[0:1]

        def of_head(h, _):
            copies = [
                pltpu.make_async_copy(qt_hbm.at[h], q_buf, sems.at[0]),
                pltpu.make_async_copy(wk_hbm.at[:, h // GROUP], k_buf, sems.at[1]),
                pltpu.make_async_copy(wv_hbm.at[:, h // GROUP], v_buf, sems.at[2]),
            ]
            for copy in copies:
                copy.start()
            for copy in copies:
                copy.wait()

            def scores(d):
                at = key - (d * ROWS).astype(jnp.float32)
                product = lax.dot_general(k_buf[d], q_buf[...], (((1,), (0,)), ((), ())),
                                          preferred_element_type=jnp.float32)
                return jnp.where((at >= begin) & (at <= query), product * SCALE, MASKED)

            def highest(d, top):
                return jnp.maximum(top, jnp.max(scores(d), axis=0, keepdims=True))

            top = lax.fori_loop(0, ITEMS, highest, jnp.full((1, ROWS), MASKED, jnp.float32))

            def summed(d, carry):
                bottom, total = carry
                weights = jnp.exp2(scores(d) - top)
                bottom = bottom + jnp.sum(weights, axis=0, keepdims=True)
                part = lax.dot_general(v_buf[d, 0:HEAD], weights.astype(jnp.bfloat16), (((1,), (0,)), ((), ())),
                                       preferred_element_type=jnp.float32)
                return bottom, total + part

            bottom, total = lax.fori_loop(
                0, ITEMS, summed, (jnp.zeros((1, ROWS), jnp.float32), jnp.zeros((HEAD, ROWS), jnp.float32)))
            o_buf[:, pl.ds(pl.multiple_of(h * HEAD, HEAD), HEAD)] = (total / bottom).astype(jnp.bfloat16).T
            return 0

        lax.fori_loop(0, HEADS, of_head, 0)
        for i in range(pieces):
            given(i).start()

    for i in range(pieces):
        given(i).wait()


def shards(documents, queries, key_projection_rows, value_projection_rows):
    bf, f32 = jnp.bfloat16, jnp.float32
    powers = np.float32(1000000.0) ** (-2.0 * np.arange(HEAD // 2, dtype=np.float32) / HEAD)
    inverse = jnp.asarray(np.tile(powers, 2)[None, :], f32)
    whole = pl.BlockSpec(memory_space=pl.ANY)
    dma = pltpu.SemaphoreType.DMA
    flops = 4 * HEADS * ROWS * ITEMS * ROWS * HEAD
    per_item = (ITEMS, KV_HEADS)
    found, q_t, wk, wv, start, bad = pl.pallas_call(
        attend,
        out_shape=[
            jax.ShapeDtypeStruct((ROWS, HEADS * HEAD), bf),
            jax.ShapeDtypeStruct((HEADS, HEAD, ROWS), bf),
            jax.ShapeDtypeStruct((ITEMS, KV_HEADS, ROWS, HEAD), bf),
            jax.ShapeDtypeStruct((ITEMS, KV_HEADS, VALUE_ROWS, ROWS), bf),
            jax.ShapeDtypeStruct((8, ROWS), f32),
            jax.ShapeDtypeStruct((8, ROWS), f32),
        ],
        in_specs=[whole] * 5,
        out_specs=[whole] * 6,
        scratch_shapes=[
            VMEM((1, HEAD), f32),
            VMEM((8, ROWS), f32),
            VMEM((8, ROWS), f32),
            VMEM((1, ROWS), jnp.int32),
            VMEM((ROWS, KV_HEADS * HEAD), bf),
            VMEM((ROWS, KV_HEADS * HEAD), bf),
            VMEM((ROWS, HEADS * HEAD), bf),
            VMEM((HEADS, HEAD, ROWS), bf),
            VMEM((ITEMS, KV_HEADS, ROWS, HEAD), bf),
            VMEM((ITEMS, KV_HEADS, VALUE_ROWS, ROWS), bf),
            VMEM((ITEMS, ROWS, ROWS), f32),
            VMEM((HEADS, VALUE_ROWS, ROWS), f32),
            VMEM((AT_ONCE * MOST_AT_ONCE, ROWS, ROWS), bf),
            VMEM((8, 1, ROWS), jnp.int32),
            VMEM((HEAD // 2, ROWS), f32),
            VMEM((HEAD // 2, ROWS), f32),
            dma(per_item), dma(per_item), dma((3, ITEMS, 3)), dma((3, ITEMS, 3)),
            VMEM((KV_HEADS, HEAD, ROWS), bf), VMEM((KV_HEADS, ROWS, HEAD), bf), dma((2, 3, KV_HEADS)),
            dma((8,)), dma((8,)), dma((5,)), dma((HEADS // AT_ONCE,)), dma, dma((ITEMS,)), dma((ITEMS,)), dma((2,)),
        ],
        compiler_params=pltpu.CompilerParams(collective_id=0, has_side_effects=True, vmem_limit_bytes=67043328),
        cost_estimate=pl.CostEstimate(flops=flops, bytes_accessed=12 * 2**20, transcendentals=HEADS * ROWS * ITEMS * ROWS),
        name="attend",
    )(documents.reshape(1, ROWS), inverse, queries, key_projection_rows, value_projection_rows)
    return pl.pallas_call(
        finish,
        out_shape=jax.ShapeDtypeStruct((ROWS, HEADS * HEAD), bf),
        in_specs=[whole] * 6,
        out_specs=whole,
        scratch_shapes=[
            VMEM((ROWS, HEADS * HEAD), bf),
            VMEM((8, ROWS), f32),
            VMEM((8, ROWS), f32),
            VMEM((HEAD, ROWS), bf),
            VMEM((ITEMS, ROWS, HEAD), bf),
            VMEM((ITEMS, VALUE_ROWS, ROWS), bf),
            dma((5,)), dma((8,)), dma((8,)),
        ],
        compiler_params=pltpu.CompilerParams(vmem_limit_bytes=67043328),
        cost_estimate=pl.CostEstimate(flops=2**20, bytes_accessed=2**14, transcendentals=0),
        name="finish",
    )(found, start, bad, q_t, wk, wv)


def solution(mesh):
    in_specs = (
        P(("dp", "ctx")),
        P(("dp", "ctx"), None),
        P(("dp", "ctx"), None),
        P(("dp", "ctx"), None),
    )
    out_specs = P(("dp", "ctx"), None)
    return jax.shard_map(shards, mesh=mesh, in_specs=in_specs, out_specs=out_specs, check_vma=False)
```

```python
import functools
import math
import jax
import jax.numpy as jnp
import numpy as np
from jax import lax
from jax.experimental import pallas as pl
from jax.experimental.pallas import tpu as pltpu
from jax.sharding import PartitionSpec as P

HEAD = 128
HEADS = 32
KV_HEADS = 4
GROUP = HEADS // KV_HEADS
ROWS = 256
ITEMS = 9
VALUE_ROWS = 144
AT_ONCE = 4
MOST_AT_ONCE = 3
SCALE = math.log2(math.e) / math.sqrt(HEAD)
LOW = 1e-25
HIGH = 1e37
MASKED = -1e30
MESH = pl.DeviceIdType.MESH
UP, RIGHT, LEFT = range(3)
V, K = range(2)
SENDS = (
    (1, 3, 0, 1, 0, 2, -1),
    (1, 4, 4, 1, 0, 2, 0),
    (1, 3, 0, 1, 1, 2, -1),
    (1, 4, 4, 1, 1, 2, 1),
    (1, 3, 1, 2, 0, 2, 1),
    (1, 4, 5, 2, 0, 2, 4),
    (1, 3, 1, 2, 1, 2, 2),
    (1, 4, 5, 2, 1, 2, 3),
    (2, 1, 0, 3, 0, 2, -1),
    (2, 7, 4, 3, 0, 2, 0),
    (2, 1, 0, 3, 1, 2, -1),
    (2, 7, 4, 3, 1, 2, 1),
    (0, 0, 0, 4, 0, 2, -1),
    (0, 0, 0, 4, 1, 2, -1),
    (0, 0, 1, 5, 0, 1, 1),
    (1, 3, 4, 5, 0, 0, 1),
    (1, 4, 8, 5, 0, 0, 2),
    (0, 0, 1, 5, 1, 2, 2),
    (2, 1, 3, 6, 0, 2, 2),
    (2, 7, 7, 6, 0, 2, 4),
    (0, 0, 2, 6, 1, 2, 4),
    (2, 1, 4, 7, 0, 2, 0),
    (2, 7, 8, 7, 0, 2, 2),
    (0, 0, 3, 7, 1, 2, 3),
)
ARRIVE = {(1, K): (2, 11), (1, V): (1, 6), (2, K): (4, 12), (2, V): (5, 4), (3, K): (3, 8), (3, V): (2, 9), (4, K): (1, 14), (4, V): (0, 3), (5, K): (3, 7), (5, V): (4, 13), (6, K): (6, 1), (6, V): (6, 2), (7, K): (4, 15), (7, V): (4, 10), (8, K): (4, 0), (8, V): (2, 5)}
RELAYED = {V: (0, 1), K: (3, 1)}
RELAY_KEYS_AT = 1
GROUPS = ((0,), (4,), (3, 1), (5, 8, 7), (2,), (6,))
SIZES = (8, 8, 4, 4, 8, 8)
VMEM = pltpu.VMEM


def attend(doc_hbm, inverse_hbm, q_hbm, k_hbm, v_hbm, out_hbm, qt_hbm, wk_hbm, wv_hbm, start_hbm, bad_hbm,
           inverse, start_out, bad_out, docs, k_buf, v_buf, q_buf, q_t, wk, wv, bias, acc, probs, doc_win, cosine, sine,
           rk, rv, sk, sv, relay_v, relay_k, relay_sems, doc_send, doc_recv, in_sem, out_sem, qt_sem, wk_sem, wv_sem, small_sem):
    count = lax.axis_size("ctx")
    me = lax.axis_index("ctx")
    x = lax.rem(me, 4)
    row = me - x
    right = row + lax.rem(x + 1, 4)
    left = row + lax.rem(x + 3, 4)
    up = lax.rem(me + 4, count)

    plane = me - lax.rem(me, 16)
    y = lax.rem(me // 4, 4)
    down = plane + 4 * lax.rem(y + 3, 4) + x
    above = plane + 4 * lax.rem(y + 1, 4) + x
    ahead = lax.rem(me + 8, count)
    relay = ahead - lax.rem(ahead, 16) + 4 * lax.rem(lax.rem(ahead // 4, 4) + 1, 4) + x

    barrier = pltpu.get_barrier_semaphore()

    def greet(other):
        pl.semaphore_signal(barrier, inc=1, device_id={"ctx": other}, device_id_type=MESH)

    for d in range(1, 9):
        @pl.when(d <= me)
        def _():
            greet(lax.rem(me + count - d, count))
    greet(left)
    greet(right)

    @pl.when(down >= 8)
    def _():
        greet(lax.rem(down + count - 8, count))

    @pl.when(me >= 8)
    def _():
        greet(above)

    loads = [pltpu.make_async_copy(a, b, in_sem.at[n])
             for n, (a, b) in enumerate([(v_hbm, v_buf), (doc_hbm, docs), (k_hbm, k_buf), (q_hbm, q_buf),
                                    (inverse_hbm, inverse)])]
    for load in loads:
        load.start()

    def value_copy(src, dst, c, target, link=0, half=2):
        return pltpu.make_async_remote_copy(
            wv.at[src, c, pl.ds(0, HEAD)], wv.at[dst, c, pl.ds(0, HEAD)], sv.at[link, dst, half], rv.at[dst, c],
            device_id={"ctx": target}, device_id_type=MESH)

    def key_copy(src, dst, c, target, link=0, half=2):
        return pltpu.make_async_remote_copy(
            wk.at[src, c], wk.at[dst, c], sk.at[link, dst, half], rk.at[dst, c],
            device_id={"ctx": target}, device_id_type=MESH)

    def doc_copy(d):
        return pltpu.make_async_remote_copy(
            docs, doc_win.at[d - 1], doc_send.at[d - 1], doc_recv.at[d - 1],
            device_id={"ctx": lax.rem(me + d, count)}, device_id_type=MESH)

    def when_sent(condition, copy):
        @pl.when(condition)
        def _():
            copy.start()

    def relay_copy(kind, c):
        buf = relay_v if kind == V else relay_k
        mine = wv.at[0, c, pl.ds(0, HEAD)] if kind == V else wk.at[0, c]
        return pltpu.make_async_remote_copy(
            mine, buf.at[c], relay_sems.at[kind, 0, 0], relay_sems.at[kind, 1, c],
            device_id={"ctx": relay}, device_id_type=MESH)

    def relayed_copy(kind, c):
        if kind == V:
            return pltpu.make_async_remote_copy(
                relay_v.at[c], wv.at[8, c, pl.ds(0, HEAD)], relay_sems.at[kind, 2, 0], rv.at[8, c],
                device_id={"ctx": down}, device_id_type=MESH)
        return pltpu.make_async_remote_copy(
            relay_k.at[c], wk.at[8, c], relay_sems.at[kind, 2, 0], rk.at[8, c],
            device_id={"ctx": down}, device_id_type=MESH)

    def relay_own(kind, c):
        if kind in RELAYED:
            when_sent(me + 8 < count, relay_copy(kind, c))

    def relay_keys(stage):
        if K in RELAYED and stage == RELAY_KEYS_AT:
            for c in range(KV_HEADS):
                relay_own(K, c)

    def relay_event(stage, late, c):
        for kind in RELAYED:
            if RELAYED[kind] == (stage, late):
                @pl.when(down >= 8)
                def _():
                    relay_copy(kind, c).wait_recv()
                    relayed_copy(kind, c).start()

    def drain_relays():
        for kind in RELAYED:
            @pl.when(me + 8 < count)
            def _():
                sent(kind, 8, relay_sems.at[kind, 0, 0])

            @pl.when(down >= 8)
            def _():
                sent(kind, 8, relay_sems.at[kind, 2, 0])

    def copy_of(kind):
        return value_copy if kind == V else key_copy

    targets = (up, right, left)
    classes = (me >= 0, x == 0, x != 0, x < 3, x == 3, x == 1, x >= 2, x >= 1)

    def open_to(entry):
        link, who, src = entry[:3]
        there = classes[who] & (src <= me)
        return there & (me + 4 < count) if link == UP else there

    def goes(entry, c):
        half = entry[5]
        return open_to(entry) if half == 2 else open_to(entry) & (c // 2 == half)

    def sent(kind, d, sem, heads=pl.ds(0, KV_HEADS)):
        ref = wv.at[d, heads, pl.ds(0, HEAD)] if kind == V else wk.at[d, heads]
        pltpu.make_async_remote_copy(ref, ref, sem, sem, device_id={"ctx": up}, device_id_type=MESH).wait_send()

    def send(entry, c):
        link, _, src, d, kind, half, _ = entry
        if isinstance(c, int) and half != 2 and c // 2 != half:
            return
        when_sent(goes(entry, c), copy_of(kind)(src, d, c, targets[link], link, half))

    def send_own(kind, c):
        for entry in SENDS:
            if entry[6] < 0 and entry[4] == kind:
                send(entry, c)

    def stage_event(stage, c):
        first, after = [], {}
        for entry in SENDS:
            _, _, src, _, kind, _, at = entry
            if at == stage:
                if ARRIVE[src, kind][0] < stage:
                    first.append(entry)
                else:
                    after.setdefault((src, kind), []).append(entry)
        for entry in first:
            send(entry, c)
        relay_event(stage, 0, c)
        for d, kind in sorted((e for e in ARRIVE if ARRIVE[e][0] == stage), key=lambda e: ARRIVE[e][1]):
            @pl.when(d <= me)
            def _():
                copy_of(kind)(d, d, c, up).wait_recv()
            for entry in after.get((d, kind), []):
                send(entry, c)
        relay_event(stage, 1, c)

    wv[:, :, HEAD:, :] = jnp.ones((ITEMS, KV_HEADS, VALUE_ROWS - HEAD, ROWS), jnp.bfloat16)
    loads[0].wait()
    for c in range(KV_HEADS):
        wv[0, c, 0:HEAD] = v_buf[:, c * HEAD:(c + 1) * HEAD].T
    loads[1].wait()
    pl.semaphore_wait(barrier, 2 + jnp.minimum(8, count - 1 - me) + jnp.where(me + 8 < count, 1, 0)
                      + jnp.where(down >= 8, 1, 0))
    for d in range(1, 9):
        when_sent(me + d < count, doc_copy(d))
    for c in range(KV_HEADS):
        send_own(V, c)
        relay_own(V, c)
    loads[3].wait()

    def turn(n, _):
        for u in range(4):
            at = pl.multiple_of((4 * n + u) * HEAD, HEAD)
            q_t[4 * n + u] = q_buf[:, pl.ds(at, HEAD)].T
        return 0

    lax.fori_loop(0, HEADS // 4, turn, 0)
    for d in range(1, 9):
        @pl.when(d > me)
        def _():
            wk[d] = jnp.zeros((KV_HEADS, ROWS, HEAD), jnp.bfloat16)
            wv[d, :, 0:HEAD] = jnp.zeros((KV_HEADS, HEAD, ROWS), jnp.bfloat16)

    doc_row = docs[...].astype(jnp.float32)
    columns = jnp.transpose(jnp.broadcast_to(doc_row, (ROWS, ROWS)))
    local = jnp.sum((columns < doc_row).astype(jnp.float32), axis=0, keepdims=True)
    first = doc_row[:, 0:1]
    loads[4].wait()
    powers = jnp.transpose(jnp.broadcast_to(inverse[...], (HEAD, HEAD)))[0:HEAD // 2]
    powers = jnp.concatenate([powers, powers], axis=1)
    tokens = lax.broadcasted_iota(jnp.int32, (1, ROWS), 1).astype(jnp.float32)
    loads[2].wait()
    for d in range(1, 9):
        @pl.when(d <= me)
        def _():
            doc_copy(d).wait_recv()
    behind = jnp.zeros((1, ROWS), jnp.float32)
    for d in range(1, 9):
        same = (doc_win[d - 1].astype(jnp.float32) == first) & (d <= me)
        behind = behind + jnp.where(same, 1.0, 0.0)
    behind = jnp.sum(behind, axis=1, keepdims=True)
    start = jnp.where(doc_row == first, -behind, local)
    start_out[...] = jnp.broadcast_to(start, (8, ROWS))
    angles = powers * (tokens - start)
    cosine[...] = jnp.cos(angles)
    sine[...] = jnp.sin(angles)

    def rotated(matrix):
        wide = matrix.astype(jnp.float32)
        a, b = wide[0:HEAD // 2], wide[HEAD // 2:]
        co, si = cosine[...], sine[...]
        return jnp.concatenate([a * co - b * si, b * co + a * si], axis=0)

    for c in range(KV_HEADS):
        wk[0, c] = rotated(k_buf[:, c * HEAD:(c + 1) * HEAD].T).T.astype(jnp.bfloat16)
    query = lax.broadcasted_iota(jnp.int32, (ROWS, ROWS), 1).astype(jnp.float32)
    key = lax.broadcasted_iota(jnp.int32, (ROWS, ROWS), 0).astype(jnp.float32)
    bias[0] = jnp.where((key >= start) & (key <= query), 0.0, MASKED)
    for c in range(KV_HEADS):
        send_own(K, c)
    for d in range(1, ITEMS):
        at = key - float(ROWS * d)
        bias[d] = jnp.where((at >= start) & (at <= query), 0.0, MASKED)

    def step_one(c, _):
        stage_event(0, c)

        def turned(n, _):
            for u in range(4):
                h = c * GROUP + 4 * n + u
                q_t[h] = rotated(q_t[h]).astype(jnp.bfloat16)
            return 0

        lax.fori_loop(0, GROUP // 4, turned, 0)
        return 0

    relay_keys(0)
    lax.fori_loop(0, KV_HEADS, step_one, 0)
    qt_copy = pltpu.make_async_copy(q_t, qt_hbm, qt_sem)
    qt_copy.start()
    start_copy = pltpu.make_async_copy(start_out, start_hbm, small_sem.at[0])
    start_copy.start()
    bad_out[...] = jnp.zeros((8, ROWS), jnp.float32)

    def weigh(items, at, size):
        for u in range(size):
            h = at + u
            for n, d in enumerate(items):
                scores = lax.dot_general(wk[d, h // GROUP], q_t[h], (((1,), (0,)), ((), ())),
                                         preferred_element_type=jnp.float32)
                probs[u * len(items) + n] = jnp.exp2(scores * SCALE + bias[d]).astype(jnp.bfloat16)

    def gather(items, at, size, begin, end):
        for u in range(size):
            h = at + u
            total = None
            for n, d in enumerate(items):
                part = lax.dot_general(wv[d, h // GROUP], probs[u * len(items) + n], (((1,), (0,)), ((), ())),
                                       preferred_element_type=jnp.float32)
                total = part if total is None else total + part
            if not begin:
                total = acc[h] + total
            if end:
                bottom = total[HEAD:HEAD + 1]
                lane = h * HEAD if isinstance(h, int) else pl.multiple_of(h * HEAD, HEAD)
                q_buf[:, pl.ds(lane, HEAD)] = (total[0:HEAD] * (1.0 / bottom)).astype(jnp.bfloat16).T
                fine = (bottom >= LOW) & (bottom <= HIGH)
                bad_out[0:1] = jnp.maximum(bad_out[0:1], jnp.where(fine, 0.0, 1.0))
            else:
                acc[h] = total

    def out_copy(i):
        wide = SIZES[-1] * HEAD
        lanes = pl.ds(i * wide if isinstance(i, int) else pl.multiple_of(i * wide, wide), wide)
        return pltpu.make_async_copy(q_buf.at[:, lanes], out_hbm.at[:, lanes], out_sem.at[i])

    def group(items, size, stage, before):
        begin, end = before is None, stage == len(GROUPS)
        per = GROUP // size
        stage_event(stage, 0)
        if before is not None:
            gather(before[0], HEADS - before[1], before[1], before[2], False)
        weigh(items, 0, size)

        def inner(i):
            if end:
                @pl.when(i >= 2)
                def _():
                    out_copy(i - 2).start()
            gather(items, size * (i - 1), size, begin, end)
            weigh(items, size * i, size)

        for j in range(1, per):
            inner(j)

        def outer(c, _):
            stage_event(stage, c)
            lax.fori_loop(0, per, lambda j, _: (inner(per * c + j), 0)[1], 0)
            return 0

        lax.fori_loop(1, KV_HEADS, outer, 0)
        return items, size, begin

    def kept(refs, out, sems, d):
        return pltpu.make_async_copy(refs.at[d], out.at[d], sems.at[d])

    def keep(*items):
        for d in items:
            kept(wk, wk_hbm, wk_sem, d).start()
            kept(wv, wv_hbm, wv_sem, d).start()

    before = None
    for n, items in enumerate(GROUPS):
        relay_keys(n + 1)
        before = group(items, SIZES[n], n + 1, before)
        keep(*items)
    batches = HEADS // SIZES[-1]
    out_copy(batches - 2).start()
    gather(GROUPS[-1], HEADS - SIZES[-1], SIZES[-1], False, True)
    out_copy(batches - 1).start()
    bad_copy = pltpu.make_async_copy(bad_out, bad_hbm, small_sem.at[1])
    bad_copy.start()

    for d in range(1, 9):
        @pl.when(me + d < count)
        def _():
            doc_copy(d).wait_send()

    for entry in SENDS:
        @pl.when(open_to(entry))
        def _():
            link, _, _, d, kind, half, _ = entry
            sent(kind, d, (sv if kind == V else sk).at[link, d, half],
                 pl.ds(0, KV_HEADS) if half == 2 else pl.ds(2 * half, 2))
    drain_relays()
    for d in range(ITEMS):
        kept(wk, wk_hbm, wk_sem, d).wait()
        kept(wv, wv_hbm, wv_sem, d).wait()
    qt_copy.wait()
    start_copy.wait()
    bad_copy.wait()
    for i in range(batches):
        out_copy(i).wait()


def finish(found, start_hbm, bad_hbm, qt_hbm, wk_hbm, wv_hbm, out, o_buf, start, bad, q_buf, k_buf, v_buf, sems, in_sems, out_sems):
    pieces = 8
    tall = ROWS // pieces

    def taken(i):
        return pltpu.make_async_copy(found.at[pl.ds(i * tall, tall)], o_buf.at[pl.ds(i * tall, tall)], in_sems.at[i])

    def given(i):
        return pltpu.make_async_copy(o_buf.at[pl.ds(i * tall, tall)], out.at[pl.ds(i * tall, tall)], out_sems.at[i])

    small = [pltpu.make_async_copy(bad_hbm, bad, sems.at[3]), pltpu.make_async_copy(start_hbm, start, sems.at[4])]
    for copy in small:
        copy.start()
    for i in range(pieces):
        taken(i).start()
    for copy in small:
        copy.wait()
    fine = jnp.max(bad[...]) < 0.5

    @pl.when(fine)
    def _():
        for i in range(pieces):
            taken(i).wait()
            given(i).start()

    @pl.when(jnp.logical_not(fine))
    def _():
        for i in range(pieces):
            taken(i).wait()
        query = lax.broadcasted_iota(jnp.int32, (ROWS, ROWS), 1).astype(jnp.float32)
        key = lax.broadcasted_iota(jnp.int32, (ROWS, ROWS), 0).astype(jnp.float32)
        begin = start[0:1]

        def of_head(h, _):
            copies = [
                pltpu.make_async_copy(qt_hbm.at[h], q_buf, sems.at[0]),
                pltpu.make_async_copy(wk_hbm.at[:, h // GROUP], k_buf, sems.at[1]),
                pltpu.make_async_copy(wv_hbm.at[:, h // GROUP], v_buf, sems.at[2]),
            ]
            for copy in copies:
                copy.start()
            for copy in copies:
                copy.wait()

            def scores(d):
                at = key - (d * ROWS).astype(jnp.float32)
                product = lax.dot_general(k_buf[d], q_buf[...], (((1,), (0,)), ((), ())),
                                          preferred_element_type=jnp.float32)
                return jnp.where((at >= begin) & (at <= query), product * SCALE, MASKED)

            def highest(d, top):
                return jnp.maximum(top, jnp.max(scores(d), axis=0, keepdims=True))

            top = lax.fori_loop(0, ITEMS, highest, jnp.full((1, ROWS), MASKED, jnp.float32))

            def summed(d, carry):
                bottom, total = carry
                weights = jnp.exp2(scores(d) - top)
                bottom = bottom + jnp.sum(weights, axis=0, keepdims=True)
                part = lax.dot_general(v_buf[d, 0:HEAD], weights.astype(jnp.bfloat16), (((1,), (0,)), ((), ())),
                                       preferred_element_type=jnp.float32)
                return bottom, total + part

            bottom, total = lax.fori_loop(
                0, ITEMS, summed, (jnp.zeros((1, ROWS), jnp.float32), jnp.zeros((HEAD, ROWS), jnp.float32)))
            o_buf[:, pl.ds(pl.multiple_of(h * HEAD, HEAD), HEAD)] = (total / bottom).astype(jnp.bfloat16).T
            return 0

        lax.fori_loop(0, HEADS, of_head, 0)
        for i in range(pieces):
            given(i).start()

    for i in range(pieces):
        given(i).wait()


def shards(documents, queries, key_projection_rows, value_projection_rows):
    bf, f32 = jnp.bfloat16, jnp.float32
    powers = np.float32(1000000.0) ** (-2.0 * np.arange(HEAD // 2, dtype=np.float32) / HEAD)
    inverse = jnp.asarray(np.tile(powers, 2)[None, :], f32)
    whole = pl.BlockSpec(memory_space=pl.ANY)
    dma = pltpu.SemaphoreType.DMA
    flops = 4 * HEADS * ROWS * ITEMS * ROWS * HEAD
    per_item = (ITEMS, KV_HEADS)
    found, q_t, wk, wv, start, bad = pl.pallas_call(
        attend,
        out_shape=[
            jax.ShapeDtypeStruct((ROWS, HEADS * HEAD), bf),
            jax.ShapeDtypeStruct((HEADS, HEAD, ROWS), bf),
            jax.ShapeDtypeStruct((ITEMS, KV_HEADS, ROWS, HEAD), bf),
            jax.ShapeDtypeStruct((ITEMS, KV_HEADS, VALUE_ROWS, ROWS), bf),
            jax.ShapeDtypeStruct((8, ROWS), f32),
            jax.ShapeDtypeStruct((8, ROWS), f32),
        ],
        in_specs=[whole] * 5,
        out_specs=[whole] * 6,
        scratch_shapes=[
            VMEM((1, HEAD), f32),
            VMEM((8, ROWS), f32),
            VMEM((8, ROWS), f32),
            VMEM((1, ROWS), jnp.int32),
            VMEM((ROWS, KV_HEADS * HEAD), bf),
            VMEM((ROWS, KV_HEADS * HEAD), bf),
            VMEM((ROWS, HEADS * HEAD), bf),
            VMEM((HEADS, HEAD, ROWS), bf),
            VMEM((ITEMS, KV_HEADS, ROWS, HEAD), bf),
            VMEM((ITEMS, KV_HEADS, VALUE_ROWS, ROWS), bf),
            VMEM((ITEMS, ROWS, ROWS), f32),
            VMEM((HEADS, VALUE_ROWS, ROWS), f32),
            VMEM((AT_ONCE * MOST_AT_ONCE, ROWS, ROWS), bf),
            VMEM((8, 1, ROWS), jnp.int32),
            VMEM((HEAD // 2, ROWS), f32),
            VMEM((HEAD // 2, ROWS), f32),
            dma(per_item), dma(per_item), dma((3, ITEMS, 3)), dma((3, ITEMS, 3)),
            VMEM((KV_HEADS, HEAD, ROWS), bf), VMEM((KV_HEADS, ROWS, HEAD), bf), dma((2, 3, KV_HEADS)),
            dma((8,)), dma((8,)), dma((5,)), dma((HEADS // AT_ONCE,)), dma, dma((ITEMS,)), dma((ITEMS,)), dma((2,)),
        ],
        compiler_params=pltpu.CompilerParams(collective_id=0, has_side_effects=True, vmem_limit_bytes=67043328),
        cost_estimate=pl.CostEstimate(flops=flops, bytes_accessed=12 * 2**20, transcendentals=HEADS * ROWS * ITEMS * ROWS),
        name="attend",
    )(documents.reshape(1, ROWS), inverse, queries, key_projection_rows, value_projection_rows)
    return pl.pallas_call(
        finish,
        out_shape=jax.ShapeDtypeStruct((ROWS, HEADS * HEAD), bf),
        in_specs=[whole] * 6,
        out_specs=whole,
        scratch_shapes=[
            VMEM((ROWS, HEADS * HEAD), bf),
            VMEM((8, ROWS), f32),
            VMEM((8, ROWS), f32),
            VMEM((HEAD, ROWS), bf),
            VMEM((ITEMS, ROWS, HEAD), bf),
            VMEM((ITEMS, VALUE_ROWS, ROWS), bf),
            dma((5,)), dma((8,)), dma((8,)),
        ],
        compiler_params=pltpu.CompilerParams(vmem_limit_bytes=67043328),
        cost_estimate=pl.CostEstimate(flops=2**20, bytes_accessed=2**14, transcendentals=0),
        name="finish",
    )(found, start, bad, q_t, wk, wv)


def solution(mesh):
    in_specs = (
        P(("dp", "ctx")),
        P(("dp", "ctx"), None),
        P(("dp", "ctx"), None),
        P(("dp", "ctx"), None),
    )
    out_specs = P(("dp", "ctx"), None)
    return jax.shard_map(shards, mesh=mesh, in_specs=in_specs, out_specs=out_specs, check_vma=False)
```

```python
import functools
import math
import jax
import jax.numpy as jnp
import numpy as np
from jax import lax
from jax.experimental import pallas as pl
from jax.experimental.pallas import tpu as pltpu
from jax.sharding import PartitionSpec as P

HEAD = 128
HEADS = 32
KV_HEADS = 4
GROUP = HEADS // KV_HEADS
ROWS = 256
ITEMS = 9
VALUE_ROWS = 144
AT_ONCE = 4
MOST_AT_ONCE = 3
SCALE = math.log2(math.e) / math.sqrt(HEAD)
LOW = 1e-25
HIGH = 1e37
MASKED = -1e30
MESH = pl.DeviceIdType.MESH
UP, RIGHT, LEFT, RELAY = range(4)
V, K = range(2)
SOURCES = {(UP, 4): (0, 0), (UP, 5): (1, 1), (UP, 6): (2, 2), (UP, 7): (3, 3), (UP, 8): (4, 4), (RIGHT, 1): (0, 4),
           (RIGHT, 2): (1, 5), (RIGHT, 5): (4, 8), (LEFT, 3): (4, 0), (LEFT, 6): (7, 3), (LEFT, 7): (8, 4)}
ROUTE = {(1, K, 0): RIGHT, (1, K, 1): RIGHT, (1, V, 0): RIGHT, (1, V, 1): RIGHT, (2, K, 0): RIGHT, (2, K, 1): RIGHT, (2, V, 0): RIGHT, (2, V, 1): RIGHT, (3, K, 0): LEFT, (3, K, 1): LEFT, (3, V, 0): LEFT, (3, V, 1): LEFT, (4, K, 0): UP, (4, K, 1): UP, (4, V, 0): UP, (4, V, 1): UP, (5, K, 0): UP, (5, K, 1): UP, (5, V, 0): RIGHT, (5, V, 1): UP, (6, K, 0): UP, (6, K, 1): UP, (6, V, 0): LEFT, (6, V, 1): LEFT, (7, K, 0): UP, (7, K, 1): UP, (7, V, 0): LEFT, (7, V, 1): LEFT, (8, K, 0): RELAY, (8, K, 1): RELAY, (8, V, 0): RELAY, (8, V, 1): RELAY}
ARRIVE = {(1, K): (2, 11), (1, V): (1, 6), (2, K): (4, 12), (2, V): (5, 4), (3, K): (3, 8), (3, V): (2, 9), (4, K): (1, 14), (4, V): (0, 3), (5, K): (3, 7), (5, V): (4, 13), (6, K): (6, 1), (6, V): (6, 2), (7, K): (4, 15), (7, V): (4, 10), (8, K): (4, 0), (8, V): (2, 5)}
LEAVE = {(1, K, 0, 1): 1, (1, K, 1, 1): 1, (1, V, 0, 1): 0, (1, V, 1, 1): 0, (2, K, 0, 0): 2, (2, K, 0, 1): 3, (2, K, 1, 0): 2, (2, K, 1, 1): 3, (2, V, 0, 0): 1, (2, V, 0, 1): 4, (2, V, 1, 0): 1, (2, V, 1, 1): 4, (3, K, 0, 0): 1, (3, K, 1, 0): 1, (3, V, 0, 0): 0, (3, V, 1, 0): 0, (5, K, 0, 0): 2, (5, K, 1, 0): 2, (5, V, 0, 0): 1, (5, V, 0, 1): 2, (5, V, 1, 0): 1, (6, K, 0, 0): 4, (6, K, 1, 0): 4, (6, V, 0, 0): 4, (6, V, 0, 1): 2, (6, V, 1, 0): 4, (6, V, 1, 1): 2, (7, K, 0, 0): 3, (7, K, 1, 0): 3, (7, V, 0, 0): 2, (7, V, 0, 1): 0, (7, V, 1, 0): 2, (7, V, 1, 1): 0}
RELAYED = {V: (0, 1), K: (3, 1)}
RELAY_KEYS_AT = 1
GROUPS = ((0,), (4,), (3, 1), (5, 8, 7), (2,), (6,))
SIZES = (8, 8, 4, 4, 8, 8)
VMEM = pltpu.VMEM


def attend(doc_hbm, inverse_hbm, q_hbm, k_hbm, v_hbm, out_hbm, qt_hbm, wk_hbm, wv_hbm, start_hbm, bad_hbm,
           inverse, start_out, bad_out, docs, k_buf, v_buf, q_buf, q_t, wk, wv, bias, acc, probs, doc_win, cosine, sine,
           rk, rv, sk, sv, relay_v, relay_k, relay_sems, doc_send, doc_recv, in_sem, out_sem, qt_sem, wk_sem, wv_sem, small_sem):
    count = lax.axis_size("ctx")
    me = lax.axis_index("ctx")
    x = lax.rem(me, 4)
    row = me - x
    right = row + lax.rem(x + 1, 4)
    left = row + lax.rem(x + 3, 4)
    up = lax.rem(me + 4, count)

    plane = me - lax.rem(me, 16)
    y = lax.rem(me // 4, 4)
    down = plane + 4 * lax.rem(y + 3, 4) + x
    above = plane + 4 * lax.rem(y + 1, 4) + x
    ahead = lax.rem(me + 8, count)
    relay = ahead - lax.rem(ahead, 16) + 4 * lax.rem(lax.rem(ahead // 4, 4) + 1, 4) + x

    barrier = pltpu.get_barrier_semaphore()

    def greet(other):
        pl.semaphore_signal(barrier, inc=1, device_id={"ctx": other}, device_id_type=MESH)

    for d in range(1, 9):
        @pl.when(d <= me)
        def _():
            greet(lax.rem(me + count - d, count))
    greet(left)
    greet(right)

    @pl.when(down >= 8)
    def _():
        greet(lax.rem(down + count - 8, count))

    @pl.when(me >= 8)
    def _():
        greet(above)

    loads = [pltpu.make_async_copy(a, b, in_sem.at[n])
             for n, (a, b) in enumerate([(v_hbm, v_buf), (doc_hbm, docs), (k_hbm, k_buf), (q_hbm, q_buf),
                                    (inverse_hbm, inverse)])]
    for load in loads:
        load.start()

    def value_copy(src, dst, c, target):
        return pltpu.make_async_remote_copy(
            wv.at[src, c, pl.ds(0, HEAD)], wv.at[dst, c, pl.ds(0, HEAD)], sv.at[dst, c], rv.at[dst, c],
            device_id={"ctx": target}, device_id_type=MESH)

    def key_copy(src, dst, c, target):
        return pltpu.make_async_remote_copy(
            wk.at[src, c], wk.at[dst, c], sk.at[dst, c], rk.at[dst, c],
            device_id={"ctx": target}, device_id_type=MESH)

    def doc_copy(d):
        return pltpu.make_async_remote_copy(
            docs, doc_win.at[d - 1], doc_send.at[d - 1], doc_recv.at[d - 1],
            device_id={"ctx": lax.rem(me + d, count)}, device_id_type=MESH)

    def when_sent(condition, copy):
        @pl.when(condition)
        def _():
            copy.start()

    def relay_copy(kind, c):
        buf = relay_v if kind == V else relay_k
        mine = wv.at[0, c, pl.ds(0, HEAD)] if kind == V else wk.at[0, c]
        return pltpu.make_async_remote_copy(
            mine, buf.at[c], relay_sems.at[kind, 0, c], relay_sems.at[kind, 1, c],
            device_id={"ctx": relay}, device_id_type=MESH)

    def relayed_copy(kind, c):
        if kind == V:
            return pltpu.make_async_remote_copy(
                relay_v.at[c], wv.at[8, c, pl.ds(0, HEAD)], relay_sems.at[kind, 2, c], rv.at[8, c],
                device_id={"ctx": down}, device_id_type=MESH)
        return pltpu.make_async_remote_copy(
            relay_k.at[c], wk.at[8, c], relay_sems.at[kind, 2, c], rk.at[8, c],
            device_id={"ctx": down}, device_id_type=MESH)

    def relay_own(kind, c):
        if kind in RELAYED:
            when_sent(me + 8 < count, relay_copy(kind, c))

    def relay_keys(stage):
        if K in RELAYED and stage == RELAY_KEYS_AT:
            for c in range(KV_HEADS):
                relay_own(K, c)

    def relay_event(stage, late, c):
        for kind in RELAYED:
            if RELAYED[kind] == (stage, late):
                @pl.when(down >= 8)
                def _():
                    relay_copy(kind, c).wait_recv()
                    relayed_copy(kind, c).start()

    def drain_relays(c):
        for kind in RELAYED:
            @pl.when(me + 8 < count)
            def _():
                relay_copy(kind, c).wait_send()

            @pl.when(down >= 8)
            def _():
                relayed_copy(kind, c).wait_send()

    def copy_of(kind):
        return value_copy if kind == V else key_copy

    def ways(d, kind, half):
        link = ROUTE[d, kind, half]
        if link == RELAY:
            return []
        plain, edge = SOURCES[link, d]
        if link == UP:
            return [(0, plain, up, me + 4 < count)]
        special = x == 3 if link == RIGHT else x == 0
        target = right if link == RIGHT else left
        return [(0, plain, target, jnp.logical_not(special)), (1, edge, target, special)]

    def send(way, d, kind, half, c):
        _, src, target, there = way
        if ROUTE[d, kind, 1 - half] != ROUTE[d, kind, half]:
            if isinstance(c, int):
                if c // 2 != half:
                    return
            else:
                there = there & (c // 2 == half)
        elif half:
            return
        when_sent(there & (src <= me), copy_of(kind)(src, d, c, target))

    def send_own(kind, c):
        for d in (4, 1, 3):
            for way in ways(d, kind, 0):
                if way[1] == 0:
                    send(way, d, kind, 0, c)

    def stage_event(stage, c):
        first, after = [], {}
        for (d, kind, half) in ROUTE:
            for way in ways(d, kind, half):
                if way[1] != 0 and LEAVE[d, kind, half, way[0]] == stage:
                    if ARRIVE[way[1], kind][0] < stage:
                        first.append((way, d, kind, half))
                    else:
                        after.setdefault((way[1], kind), []).append((way, d, kind, half))
        first.sort(key=lambda e: ROUTE[e[1:]] != UP)
        for entry in first:
            send(*entry, c)
        relay_event(stage, 0, c)
        for d, kind in sorted((e for e in ARRIVE if ARRIVE[e][0] == stage), key=lambda e: ARRIVE[e][1]):
            @pl.when(d <= me)
            def _():
                copy_of(kind)(d, d, c, up).wait_recv()
            for entry in sorted(after.get((d, kind), []), key=lambda e: ROUTE[e[1:]] != UP):
                send(*entry, c)
        relay_event(stage, 1, c)

    wv[:, :, HEAD:, :] = jnp.ones((ITEMS, KV_HEADS, VALUE_ROWS - HEAD, ROWS), jnp.bfloat16)
    loads[0].wait()
    for c in range(KV_HEADS):
        wv[0, c, 0:HEAD] = v_buf[:, c * HEAD:(c + 1) * HEAD].T
    loads[1].wait()
    pl.semaphore_wait(barrier, 2 + jnp.minimum(8, count - 1 - me) + jnp.where(me + 8 < count, 1, 0)
                      + jnp.where(down >= 8, 1, 0))
    for d in range(1, 9):
        when_sent(me + d < count, doc_copy(d))
    for c in range(KV_HEADS):
        send_own(V, c)
        relay_own(V, c)
    loads[3].wait()

    def turn(n, _):
        for u in range(4):
            at = pl.multiple_of((4 * n + u) * HEAD, HEAD)
            q_t[4 * n + u] = q_buf[:, pl.ds(at, HEAD)].T
        return 0

    lax.fori_loop(0, HEADS // 4, turn, 0)
    for d in range(1, 9):
        @pl.when(d > me)
        def _():
            wk[d] = jnp.zeros((KV_HEADS, ROWS, HEAD), jnp.bfloat16)
            wv[d, :, 0:HEAD] = jnp.zeros((KV_HEADS, HEAD, ROWS), jnp.bfloat16)

    doc_row = docs[...].astype(jnp.float32)
    columns = jnp.transpose(jnp.broadcast_to(doc_row, (ROWS, ROWS)))
    local = jnp.sum((columns < doc_row).astype(jnp.float32), axis=0, keepdims=True)
    first = doc_row[:, 0:1]
    loads[4].wait()
    powers = jnp.transpose(jnp.broadcast_to(inverse[...], (HEAD, HEAD)))[0:HEAD // 2]
    powers = jnp.concatenate([powers, powers], axis=1)
    tokens = lax.broadcasted_iota(jnp.int32, (1, ROWS), 1).astype(jnp.float32)
    loads[2].wait()
    for d in range(1, 9):
        @pl.when(d <= me)
        def _():
            doc_copy(d).wait_recv()
    behind = jnp.zeros((1, ROWS), jnp.float32)
    for d in range(1, 9):
        same = (doc_win[d - 1].astype(jnp.float32) == first) & (d <= me)
        behind = behind + jnp.where(same, 1.0, 0.0)
    behind = jnp.sum(behind, axis=1, keepdims=True)
    start = jnp.where(doc_row == first, -behind, local)
    start_out[...] = jnp.broadcast_to(start, (8, ROWS))
    angles = powers * (tokens - start)
    cosine[...] = jnp.cos(angles)
    sine[...] = jnp.sin(angles)

    def rotated(matrix):
        wide = matrix.astype(jnp.float32)
        a, b = wide[0:HEAD // 2], wide[HEAD // 2:]
        co, si = cosine[...], sine[...]
        return jnp.concatenate([a * co - b * si, b * co + a * si], axis=0)

    for c in range(KV_HEADS):
        wk[0, c] = rotated(k_buf[:, c * HEAD:(c + 1) * HEAD].T).T.astype(jnp.bfloat16)
    query = lax.broadcasted_iota(jnp.int32, (ROWS, ROWS), 1).astype(jnp.float32)
    key = lax.broadcasted_iota(jnp.int32, (ROWS, ROWS), 0).astype(jnp.float32)
    bias[0] = jnp.where((key >= start) & (key <= query), 0.0, MASKED)
    for c in range(KV_HEADS):
        send_own(K, c)
    for d in range(1, ITEMS):
        at = key - float(ROWS * d)
        bias[d] = jnp.where((at >= start) & (at <= query), 0.0, MASKED)

    def step_one(c, _):
        stage_event(0, c)

        def turned(n, _):
            for u in range(4):
                h = c * GROUP + 4 * n + u
                q_t[h] = rotated(q_t[h]).astype(jnp.bfloat16)
            return 0

        lax.fori_loop(0, GROUP // 4, turned, 0)
        return 0

    relay_keys(0)
    lax.fori_loop(0, KV_HEADS, step_one, 0)
    qt_copy = pltpu.make_async_copy(q_t, qt_hbm, qt_sem)
    qt_copy.start()
    start_copy = pltpu.make_async_copy(start_out, start_hbm, small_sem.at[0])
    start_copy.start()
    bad_out[...] = jnp.zeros((8, ROWS), jnp.float32)

    def weigh(items, at, size):
        for u in range(size):
            h = at + u
            for n, d in enumerate(items):
                scores = lax.dot_general(wk[d, h // GROUP], q_t[h], (((1,), (0,)), ((), ())),
                                         preferred_element_type=jnp.float32)
                probs[u * len(items) + n] = jnp.exp2(scores * SCALE + bias[d]).astype(jnp.bfloat16)

    def gather(items, at, size, begin, end):
        for u in range(size):
            h = at + u
            total = None
            for n, d in enumerate(items):
                part = lax.dot_general(wv[d, h // GROUP], probs[u * len(items) + n], (((1,), (0,)), ((), ())),
                                       preferred_element_type=jnp.float32)
                total = part if total is None else total + part
            if not begin:
                total = acc[h] + total
            if end:
                bottom = total[HEAD:HEAD + 1]
                lane = h * HEAD if isinstance(h, int) else pl.multiple_of(h * HEAD, HEAD)
                q_buf[:, pl.ds(lane, HEAD)] = (total[0:HEAD] * (1.0 / bottom)).astype(jnp.bfloat16).T
                fine = (bottom >= LOW) & (bottom <= HIGH)
                bad_out[0:1] = jnp.maximum(bad_out[0:1], jnp.where(fine, 0.0, 1.0))
            else:
                acc[h] = total

    def out_copy(i):
        wide = SIZES[-1] * HEAD
        lanes = pl.ds(i * wide if isinstance(i, int) else pl.multiple_of(i * wide, wide), wide)
        return pltpu.make_async_copy(q_buf.at[:, lanes], out_hbm.at[:, lanes], out_sem.at[i])

    def group(items, size, stage, before):
        begin, end = before is None, stage == len(GROUPS)
        per = GROUP // size
        stage_event(stage, 0)
        if before is not None:
            gather(before[0], HEADS - before[1], before[1], before[2], False)
        weigh(items, 0, size)

        def inner(i):
            if end:
                @pl.when(i >= 2)
                def _():
                    out_copy(i - 2).start()
            gather(items, size * (i - 1), size, begin, end)
            weigh(items, size * i, size)

        for j in range(1, per):
            inner(j)

        def outer(c, _):
            stage_event(stage, c)
            lax.fori_loop(0, per, lambda j, _: (inner(per * c + j), 0)[1], 0)
            return 0

        lax.fori_loop(1, KV_HEADS, outer, 0)
        return items, size, begin

    def kept(refs, out, sems, d):
        return pltpu.make_async_copy(refs.at[d], out.at[d], sems.at[d])

    def keep(*items):
        for d in items:
            kept(wk, wk_hbm, wk_sem, d).start()
            kept(wv, wv_hbm, wv_sem, d).start()

    before = None
    for n, items in enumerate(GROUPS):
        relay_keys(n + 1)
        before = group(items, SIZES[n], n + 1, before)
        keep(*items)
    batches = HEADS // SIZES[-1]
    out_copy(batches - 2).start()
    gather(GROUPS[-1], HEADS - SIZES[-1], SIZES[-1], False, True)
    out_copy(batches - 1).start()
    bad_copy = pltpu.make_async_copy(bad_out, bad_hbm, small_sem.at[1])
    bad_copy.start()

    for d in range(1, 9):
        @pl.when(me + d < count)
        def _():
            doc_copy(d).wait_send()

    def drain(c, _):
        for (d, kind, half) in ROUTE:
            same = ROUTE[d, kind, 1 - half] == ROUTE[d, kind, half]
            for way in ways(d, kind, half) if not (same and half) else []:
                @pl.when(way[3] & (way[1] <= me) & ((c // 2 == half) | same))
                def _():
                    copy_of(kind)(d, d, c, up).wait_send()
        drain_relays(c)
        return 0

    lax.fori_loop(0, KV_HEADS, drain, 0)
    for d in range(ITEMS):
        kept(wk, wk_hbm, wk_sem, d).wait()
        kept(wv, wv_hbm, wv_sem, d).wait()
    qt_copy.wait()
    start_copy.wait()
    bad_copy.wait()
    for i in range(batches):
        out_copy(i).wait()


def finish(found, start_hbm, bad_hbm, qt_hbm, wk_hbm, wv_hbm, out, o_buf, start, bad, q_buf, k_buf, v_buf, sems, in_sems, out_sems):
    pieces = 8
    tall = ROWS // pieces

    def taken(i):
        return pltpu.make_async_copy(found.at[pl.ds(i * tall, tall)], o_buf.at[pl.ds(i * tall, tall)], in_sems.at[i])

    def given(i):
        return pltpu.make_async_copy(o_buf.at[pl.ds(i * tall, tall)], out.at[pl.ds(i * tall, tall)], out_sems.at[i])

    small = [pltpu.make_async_copy(bad_hbm, bad, sems.at[3]), pltpu.make_async_copy(start_hbm, start, sems.at[4])]
    for copy in small:
        copy.start()
    for i in range(pieces):
        taken(i).start()
    for copy in small:
        copy.wait()
    fine = jnp.max(bad[...]) < 0.5

    @pl.when(fine)
    def _():
        for i in range(pieces):
            taken(i).wait()
            given(i).start()

    @pl.when(jnp.logical_not(fine))
    def _():
        for i in range(pieces):
            taken(i).wait()
        query = lax.broadcasted_iota(jnp.int32, (ROWS, ROWS), 1).astype(jnp.float32)
        key = lax.broadcasted_iota(jnp.int32, (ROWS, ROWS), 0).astype(jnp.float32)
        begin = start[0:1]

        def of_head(h, _):
            copies = [
                pltpu.make_async_copy(qt_hbm.at[h], q_buf, sems.at[0]),
                pltpu.make_async_copy(wk_hbm.at[:, h // GROUP], k_buf, sems.at[1]),
                pltpu.make_async_copy(wv_hbm.at[:, h // GROUP], v_buf, sems.at[2]),
            ]
            for copy in copies:
                copy.start()
            for copy in copies:
                copy.wait()

            def scores(d):
                at = key - (d * ROWS).astype(jnp.float32)
                product = lax.dot_general(k_buf[d], q_buf[...], (((1,), (0,)), ((), ())),
                                          preferred_element_type=jnp.float32)
                return jnp.where((at >= begin) & (at <= query), product * SCALE, MASKED)

            def highest(d, top):
                return jnp.maximum(top, jnp.max(scores(d), axis=0, keepdims=True))

            top = lax.fori_loop(0, ITEMS, highest, jnp.full((1, ROWS), MASKED, jnp.float32))

            def summed(d, carry):
                bottom, total = carry
                weights = jnp.exp2(scores(d) - top)
                bottom = bottom + jnp.sum(weights, axis=0, keepdims=True)
                part = lax.dot_general(v_buf[d, 0:HEAD], weights.astype(jnp.bfloat16), (((1,), (0,)), ((), ())),
                                       preferred_element_type=jnp.float32)
                return bottom, total + part

            bottom, total = lax.fori_loop(
                0, ITEMS, summed, (jnp.zeros((1, ROWS), jnp.float32), jnp.zeros((HEAD, ROWS), jnp.float32)))
            o_buf[:, pl.ds(pl.multiple_of(h * HEAD, HEAD), HEAD)] = (total / bottom).astype(jnp.bfloat16).T
            return 0

        lax.fori_loop(0, HEADS, of_head, 0)
        for i in range(pieces):
            given(i).start()

    for i in range(pieces):
        given(i).wait()


def shards(documents, queries, key_projection_rows, value_projection_rows):
    bf, f32 = jnp.bfloat16, jnp.float32
    powers = np.float32(1000000.0) ** (-2.0 * np.arange(HEAD // 2, dtype=np.float32) / HEAD)
    inverse = jnp.asarray(np.tile(powers, 2)[None, :], f32)
    whole = pl.BlockSpec(memory_space=pl.ANY)
    dma = pltpu.SemaphoreType.DMA
    flops = 4 * HEADS * ROWS * ITEMS * ROWS * HEAD
    per_item = (ITEMS, KV_HEADS)
    found, q_t, wk, wv, start, bad = pl.pallas_call(
        attend,
        out_shape=[
            jax.ShapeDtypeStruct((ROWS, HEADS * HEAD), bf),
            jax.ShapeDtypeStruct((HEADS, HEAD, ROWS), bf),
            jax.ShapeDtypeStruct((ITEMS, KV_HEADS, ROWS, HEAD), bf),
            jax.ShapeDtypeStruct((ITEMS, KV_HEADS, VALUE_ROWS, ROWS), bf),
            jax.ShapeDtypeStruct((8, ROWS), f32),
            jax.ShapeDtypeStruct((8, ROWS), f32),
        ],
        in_specs=[whole] * 5,
        out_specs=[whole] * 6,
        scratch_shapes=[
            VMEM((1, HEAD), f32),
            VMEM((8, ROWS), f32),
            VMEM((8, ROWS), f32),
            VMEM((1, ROWS), jnp.int32),
            VMEM((ROWS, KV_HEADS * HEAD), bf),
            VMEM((ROWS, KV_HEADS * HEAD), bf),
            VMEM((ROWS, HEADS * HEAD), bf),
            VMEM((HEADS, HEAD, ROWS), bf),
            VMEM((ITEMS, KV_HEADS, ROWS, HEAD), bf),
            VMEM((ITEMS, KV_HEADS, VALUE_ROWS, ROWS), bf),
            VMEM((ITEMS, ROWS, ROWS), f32),
            VMEM((HEADS, VALUE_ROWS, ROWS), f32),
            VMEM((AT_ONCE * MOST_AT_ONCE, ROWS, ROWS), bf),
            VMEM((8, 1, ROWS), jnp.int32),
            VMEM((HEAD // 2, ROWS), f32),
            VMEM((HEAD // 2, ROWS), f32),
            dma(per_item), dma(per_item), dma(per_item), dma(per_item),
            VMEM((KV_HEADS, HEAD, ROWS), bf), VMEM((KV_HEADS, ROWS, HEAD), bf), dma((2, 3, KV_HEADS)),
            dma((8,)), dma((8,)), dma((5,)), dma((HEADS // AT_ONCE,)), dma, dma((ITEMS,)), dma((ITEMS,)), dma((2,)),
        ],
        compiler_params=pltpu.CompilerParams(collective_id=0, has_side_effects=True, vmem_limit_bytes=67043328),
        cost_estimate=pl.CostEstimate(flops=flops, bytes_accessed=12 * 2**20, transcendentals=HEADS * ROWS * ITEMS * ROWS),
        name="attend",
    )(documents.reshape(1, ROWS), inverse, queries, key_projection_rows, value_projection_rows)
    return pl.pallas_call(
        finish,
        out_shape=jax.ShapeDtypeStruct((ROWS, HEADS * HEAD), bf),
        in_specs=[whole] * 6,
        out_specs=whole,
        scratch_shapes=[
            VMEM((ROWS, HEADS * HEAD), bf),
            VMEM((8, ROWS), f32),
            VMEM((8, ROWS), f32),
            VMEM((HEAD, ROWS), bf),
            VMEM((ITEMS, ROWS, HEAD), bf),
            VMEM((ITEMS, VALUE_ROWS, ROWS), bf),
            dma((5,)), dma((8,)), dma((8,)),
        ],
        compiler_params=pltpu.CompilerParams(vmem_limit_bytes=67043328),
        cost_estimate=pl.CostEstimate(flops=2**20, bytes_accessed=2**14, transcendentals=0),
        name="finish",
    )(found, start, bad, q_t, wk, wv)


def solution(mesh):
    in_specs = (
        P(("dp", "ctx")),
        P(("dp", "ctx"), None),
        P(("dp", "ctx"), None),
        P(("dp", "ctx"), None),
    )
    out_specs = P(("dp", "ctx"), None)
    return jax.shard_map(shards, mesh=mesh, in_specs=in_specs, out_specs=out_specs, check_vma=False)
```
